32 devices in a mesh: star: 2 (over x), blk: 16 (over z, y, core).
Axes of the slice: x: 2, y: 2, z: 4, core: 2. Of those that a mesh axis runs over, the one named last changes fastest.
Arguments:
- lapse_field: float32 [256, 16, 256], P(('star', 'blk')), may hold values from 0.3 to 1
- conformal: float32 [256, 16, 256], P(('star', 'blk')), may hold values from 0.5 to 1.5
- mean_curv: float32 [256, 16, 256], P(('star', 'blk')), may hold values from -3 to 3
- conformal_metric: float32 [6, 256, 16, 256], P(None, ('star', 'blk')), may hold values from -0.3 to 1.6, as said below
- traceless_curv: float32 [6, 256, 16, 256], P(None, ('star', 'blk')), may hold values from -2 to 2
- shift_vector: float32 [3, 256, 16, 256], P(None, ('star', 'blk')), may hold values from -3 to 3
- density: float32 [2, 256, 16, 256], P('star', 'blk'), may hold values from 0.2 to 2
- momentum: float32 [2, 3, 256, 16, 256], P('star', None, 'blk'), may hold values from -3 to 3
- energy: float32 [2, 256, 16, 256], P('star', 'blk'), may hold values from 0.2 to 2
- velocity: float32 [2, 3, 256, 16, 256], P('star', None, 'blk'), may hold values from -0.5 to 0.5
- pressure: float32 [2, 256, 16, 256], P('star', 'blk'), may hold values from 0.05 to 0.5
Outputs:
- bssn_rhs: float32 [15, 256, 16, 256], P(None, ('star', 'blk'))
- hydro_rhs: float32 [2, 5, 256, 16, 256], P('star', None, 'blk')
The draws below stay inside these ranges and needn't reach their ends.
Inputs may be any that keep to these rules, and one draw needn't show every extreme that they name: `conformal_metric`: in every cell the symmetric matrix with rows (xx, xy, xz), (xy, yy, yz), (xz, yz, zz) has diagonal entries from 0.8 to 1.6 and off-diagonal entries from -0.3 to 0.3, and each diagonal entry exceeds the sum of the magnitudes of the other entries of its row.
All inputs are finite; a program needn't handle non-finite values.
Results may differ from the reference program's by a relative error of at most 0.0003.
Values sent between devices are 32-bit elements; how exact they have to be, the bound alone decides.
No kernel may reach another device: no remote copies, remote signals or barrier semaphores. Data moves between devices by JAX's collectives and lax.ppermute only.
A program may use at most 128 MiB of HBM per device.

```python
import math
from functools import reduce
import jax
import jax.numpy as jnp
from jax import lax

CX = 8
CY = 16
CZ = 256
STARS = 2
NX = 256
FX = 256
N_BLK = 16


def draw_conformal_metric(key, part):
    diag_key, off_key = jax.random.split(jax.random.fold_in(key, 11))
    cell_shape = (3, NX, CY, CZ)
    diagonal = jax.random.uniform(diag_key, cell_shape, jnp.float32, 0.8, 1.4)
    offdiag = jax.random.uniform(off_key, cell_shape, jnp.float32, -0.2, 0.2)
    return jnp.stack([diagonal[0], offdiag[0], offdiag[1], diagonal[1], offdiag[2], diagonal[2]], 0)


def steps_of(own_key, dims, pieces, smallest, high):
    def one(axis_at, blocks):
        steps = jax.random.uniform(jax.random.fold_in(jax.random.fold_in(own_key, 6), axis_at), (blocks,), jnp.float32, smallest / len(pieces), high / len(pieces))
        return jnp.repeat(jnp.exp(steps), dims[axis_at] // blocks).reshape((-1,) + (1,) * (len(dims) - axis_at - 1))

    level = one(*pieces[0])
    for cut in pieces[1:]:
        level = level * one(*cut)
    return level


def noise(rng, extent, spread, limit, shards=(), held_as=jnp.bfloat16):
    result = jax.random.normal(rng, extent, jnp.float32) * spread
    if len(shards) > 0:
        result = steps_of(rng, extent, shards, -0.22, 0.18) * result
    return jnp.clip(result, min=-limit, max=limit).astype(held_as)


def setup_inputs(seed: int = 0) -> dict:
    arg_keys = jax.random.split(jax.random.key(seed), 12)
    return {
        "lapse_field": jnp.clip(0.3 + 0.7 * jax.random.uniform(arg_keys[0], (NX, CY, CZ), jnp.float32) ** steps_of(arg_keys[0], (NX, CY, CZ), ((0, 32),), -0.2, 0.2), 0.3, 1.0),
        "conformal": jnp.clip(0.5 + 1.0 * jax.random.uniform(arg_keys[1], (NX, CY, CZ), jnp.float32) ** steps_of(arg_keys[1], (NX, CY, CZ), ((0, 32),), -0.2, 0.2), 0.5, 1.5),
        "mean_curv": noise(arg_keys[2], (NX, CY, CZ), 0.5, 3.0, ((0, 32),), jnp.float32),
        "conformal_metric": draw_conformal_metric(jax.random.fold_in(arg_keys[11], 71), 0),
        "traceless_curv": noise(arg_keys[4], (6, NX, CY, CZ), 0.3, 2.0, ((1, 32),), jnp.float32),
        "shift_vector": noise(arg_keys[5], (3, NX, CY, CZ), 0.5, 3.0, ((1, 32),), jnp.float32),
        "density": jnp.clip(jnp.exp(math.log(2.0) - 2.3025851 * jax.random.uniform(arg_keys[6], (STARS, FX, CY, CZ), jnp.float32) ** steps_of(arg_keys[6], (STARS, FX, CY, CZ), ((0, 2), (1, 16)), -0.2, 0.2)), 0.2, 2.0),
        "momentum": noise(arg_keys[7], (STARS, 3, FX, CY, CZ), 0.5, 3.0, ((0, 2), (2, 16)), jnp.float32),
        "energy": jnp.clip(jnp.exp(math.log(2.0) - 2.3025851 * jax.random.uniform(arg_keys[8], (STARS, FX, CY, CZ), jnp.float32) ** steps_of(arg_keys[8], (STARS, FX, CY, CZ), ((0, 2), (1, 16)), -0.2, 0.2)), 0.2, 2.0),
        "velocity": jnp.clip(jax.random.uniform(arg_keys[9], (STARS, 3, FX, CY, CZ), jnp.float32, -0.5, 0.5) * steps_of(arg_keys[9], (STARS, 3, FX, CY, CZ), ((0, 2), (2, 16)), -0.4, 0.0), -0.5, 0.5),
        "pressure": jnp.clip(jnp.exp(math.log(0.5) - 2.3025851 * jax.random.uniform(arg_keys[10], (STARS, FX, CY, CZ), jnp.float32) ** steps_of(arg_keys[10], (STARS, FX, CY, CZ), ((0, 2), (1, 16)), -0.2, 0.2)), 0.05, 0.5),
    }


pair_index = ((0, 1, 2), (1, 3, 4), (2, 4, 5))
sym_pairs = ((0, 0), (0, 1), (0, 2), (1, 1), (1, 2), (2, 2))
weno_eps = 1e-6


def accumulate(terms):
    return reduce(lambda x, y: x + y, terms)


def xfirst(values):
    return (values[..., 0:-4, :, :] - 8.0 * values[..., 1:-3, :, :] + 8.0 * values[..., 3:-1, :, :] - values[..., 4:, :, :]) / 12.0


def xsecond(values):
    return (-values[..., 0:-4, :, :] + 16.0 * values[..., 1:-3, :, :] - 30.0 * values[..., 2:-2, :, :] + 16.0 * values[..., 3:-1, :, :] - values[..., 4:, :, :]) / 12.0


def rfirst(values, direction):
    return (jnp.roll(values, 2, direction) - 8.0 * jnp.roll(values, 1, direction) + 8.0 * jnp.roll(values, -1, direction) - jnp.roll(values, -2, direction)) / 12.0


def rsecond(values, direction):
    return (-jnp.roll(values, 2, direction) + 16.0 * jnp.roll(values, 1, direction) - 30.0 * values + 16.0 * jnp.roll(values, -1, direction) - jnp.roll(values, -2, direction)) / 12.0


def bssn_rates(padded, sources):
    core_cells = padded[:, 2:-2]
    gradients = (xfirst(padded), rfirst(core_cells, -2), rfirst(core_cells, -1))
    lapse_core = core_cells[0]
    conf_core = core_cells[1]
    mean_core = core_cells[2]
    shift_core = core_cells[15:18]
    advected = shift_core[0] * gradients[0][:15] + shift_core[1] * gradients[1][:15] + shift_core[2] * gradients[2][:15]

    def metric_at(i, j):
        return core_cells[3 + pair_index[i][j]]

    def curv_at(i, j):
        return core_cells[9 + pair_index[i][j]]

    def dshift(k, i):
        return gradients[k][15 + i]

    div_shift = dshift(0, 0) + dshift(1, 1) + dshift(2, 2)
    a, b, c, d, e, f = [core_cells[3 + n] for n in range(6)]
    cofactor = (d * f - e * e, c * e - b * f, b * e - c * d, a * f - c * c, b * c - a * e, a * d - b * b)
    determ = a * cofactor[0] + b * cofactor[1] + c * cofactor[2]
    inverse = [entry / determ for entry in cofactor]

    def inverse_at(i, j):
        return inverse[pair_index[i][j]]

    lapse_pad = padded[0]
    hessian = (xsecond(lapse_pad), xfirst(rfirst(lapse_pad, -2)), xfirst(rfirst(lapse_pad, -1)),
               rsecond(lapse_core, -2), rfirst(rfirst(lapse_core, -1), -2), rsecond(lapse_core, -1))

    def hess_at(i, j):
        return hessian[pair_index[i][j]]

    trace_hess = accumulate([inverse_at(i, j) * hess_at(i, j) for i in range(3) for j in range(3)])
    mixed_curv = [[accumulate([curv_at(i, l) * inverse_at(l, j) for l in range(3)]) for j in range(3)] for i in range(3)]
    square_trace = accumulate([mixed_curv[i][j] * mixed_curv[j][i] for i in range(3) for j in range(3)])
    lapse_rate = advected[0] - 2.0 * lapse_core * mean_core
    conf_rate = advected[1] + (2.0 / 3.0) * conf_core * (lapse_core * mean_core - div_shift)
    mean_rate = advected[2] - conf_core * trace_hess + lapse_core * (square_trace + mean_core * mean_core / 3.0) + 4.0 * math.pi * lapse_core * sources[0]
    metric_rates = []
    curv_rates = []
    for p, (i, j) in enumerate(sym_pairs):
        moved_metric = accumulate([metric_at(i, k) * dshift(j, k) + metric_at(j, k) * dshift(i, k) for k in range(3)])
        metric_rates.append(advected[3 + p] - 2.0 * lapse_core * curv_at(i, j) + moved_metric - (2.0 / 3.0) * metric_at(i, j) * div_shift)
        moved_curv = accumulate([curv_at(i, k) * dshift(j, k) + curv_at(j, k) * dshift(i, k) for k in range(3)])
        product = accumulate([mixed_curv[i][k] * curv_at(k, j) for k in range(3)])
        curv_rates.append(advected[9 + p] + lapse_core * (mean_core * curv_at(i, j) - 2.0 * product) + moved_curv
                          - (2.0 / 3.0) * curv_at(i, j) * div_shift - conf_core * (hess_at(i, j) - trace_hess * metric_at(i, j) / 3.0))
    return jnp.stack([lapse_rate, conf_rate, mean_rate] + metric_rates + curv_rates, 0)


def restrict(fine_cells):
    leading = fine_cells.shape[:-3]
    extent_x, extent_y, extent_z = fine_cells.shape[-3:]
    blocks = fine_cells.reshape(leading + (extent_x // 2, 2, extent_y // 2, 2, extent_z // 2, 2))
    return jnp.sum(blocks, axis=(-5, -3, -1)) * 0.125


def refine_axis(coarse, axis_index):
    cell_count = coarse.shape[axis_index] - 2
    center = lax.slice_in_dim(coarse, 1, cell_count + 1, axis=axis_index)
    lower_side = lax.slice_in_dim(coarse, 0, cell_count, axis=axis_index)
    upper_side = lax.slice_in_dim(coarse, 2, cell_count + 2, axis=axis_index)
    even_cells = 0.75 * center + 0.25 * lower_side
    odd_cells = 0.75 * center + 0.25 * upper_side
    stacked = jnp.stack([even_cells, odd_cells], axis_index + 1)
    new_shape = coarse.shape[:axis_index] + (2 * cell_count,) + coarse.shape[axis_index + 1:]
    return stacked.reshape(new_shape)


def prolong(window):
    return refine_axis(refine_axis(refine_axis(window, 1), 2), 3)


def split_fluxes(conserved, velocity, pressure, fine_metric):
    lapse_fine = fine_metric[0]
    shift_fine = fine_metric[1]
    conf_fine = fine_metric[2]
    transport = lapse_fine * velocity[0] - shift_fine
    weight = lapse_fine * conf_fine ** -1.5 * pressure
    flux_terms = jnp.stack([conserved[0] * transport, conserved[1] * transport + weight, conserved[2] * transport,
                            conserved[3] * transport, conserved[4] * transport + weight * velocity[0]], 0)
    max_speed = lapse_fine + jnp.abs(shift_fine)
    return jnp.concatenate([0.5 * (flux_terms + max_speed * conserved), 0.5 * (flux_terms - max_speed * conserved)], 0)


def weno_value(left_two, left_one, middle, right_one, right_two):
    guess_one = (2.0 * left_two - 7.0 * left_one + 11.0 * middle) / 6.0
    guess_two = (-left_one + 5.0 * middle + 2.0 * right_one) / 6.0
    guess_three = (2.0 * middle + 5.0 * right_one - right_two) / 6.0
    smooth_one = 13.0 / 12.0 * (left_two - 2.0 * left_one + middle) ** 2 + 0.25 * (left_two - 4.0 * left_one + 3.0 * middle) ** 2
    smooth_two = 13.0 / 12.0 * (left_one - 2.0 * middle + right_one) ** 2 + 0.25 * (left_one - right_one) ** 2
    smooth_three = 13.0 / 12.0 * (middle - 2.0 * right_one + right_two) ** 2 + 0.25 * (3.0 * middle - 4.0 * right_one + right_two) ** 2
    weight_one = 0.1 / (weno_eps + smooth_one) ** 2
    weight_two = 0.6 / (weno_eps + smooth_two) ** 2
    weight_three = 0.3 / (weno_eps + smooth_three) ** 2
    return (weight_one * guess_one + weight_two * guess_two + weight_three * guess_three) / (weight_one + weight_two + weight_three)


def weno_rates(ghosts):
    cell_count = ghosts.shape[1] - 6
    plus_part = ghosts[:5]
    minus_part = ghosts[5:]

    def taps(values, start):
        return values[:, start:start + cell_count + 1]

    face_flux = weno_value(taps(plus_part, 0), taps(plus_part, 1), taps(plus_part, 2), taps(plus_part, 3), taps(plus_part, 4)) \
        + weno_value(taps(minus_part, 5), taps(minus_part, 4), taps(minus_part, 3), taps(minus_part, 2), taps(minus_part, 1))
    return (face_flux[:, :-1] - face_flux[:, 1:]) * 2.0


def reference(lapse_field, conformal, mean_curv, conformal_metric, traceless_curv, shift_vector, density, momentum, energy, velocity, pressure):
    metric_state = jnp.concatenate([lapse_field[None], conformal[None], mean_curv[None], conformal_metric, traceless_curv, shift_vector], 0)
    source_fine = energy + density + (momentum[:, 0] * velocity[:, 0] + momentum[:, 1] * velocity[:, 1] + momentum[:, 2] * velocity[:, 2]) + 3.0 * pressure
    source_coarse = restrict(source_fine)
    joined = source_coarse.reshape(NX, CY // 2, CZ // 2)
    source_level = jnp.roll(joined, 1, axis=0)
    source_level = jnp.pad(source_level, ((0, 0), (CY // 4, CY // 4), (CZ // 4, CZ // 4)))[None]
    slab_count = NX // CX
    slab_ids = jnp.arange(slab_count, dtype=jnp.int32)

    def metric_slab(slab_index):
        row_index = (slab_index * CX + jnp.arange(-2, CX + 2, dtype=jnp.int32)) % NX
        padded = jnp.take(metric_state, row_index, axis=1)
        sources = lax.dynamic_slice_in_dim(source_level, slab_index * CX, CX, 1)
        return bssn_rates(padded, sources)

    slab_rates = lax.map(metric_slab, slab_ids)
    bssn_rhs = slab_rates.transpose(1, 0, 2, 3, 4).reshape(15, NX, CY, CZ)

    coarse_three = jnp.stack([lapse_field, shift_vector[0], conformal], 0)
    shifted = jnp.roll(coarse_three, -1, axis=1)
    extended = jnp.concatenate([shifted[:, -1:], shifted, shifted[:, :1]], 1)
    extended = extended[:, :, CY // 4 - 1:3 * CY // 4 + 1, CZ // 4 - 1:3 * CZ // 4 + 1]

    def fine_slab(slab_index):
        return prolong(lax.dynamic_slice_in_dim(extended, slab_index * CX, CX + 2, 1))

    fine_blocks = lax.map(fine_slab, slab_ids)
    fine_metric = fine_blocks.reshape(STARS, N_BLK, 3, 2 * CX, CY, CZ).transpose(0, 2, 1, 3, 4, 5).reshape(STARS, 3, FX, CY, CZ)
    conserved = jnp.concatenate([density[:, None], momentum, energy[:, None]], 1)
    split_flux = jax.vmap(split_fluxes)(conserved, velocity, pressure, fine_metric)

    def hydro_slab(slab_index):
        star_index = slab_index // N_BLK
        block_index = slab_index % N_BLK
        row_index = block_index * (2 * CX) + jnp.arange(-3, 2 * CX + 3, dtype=jnp.int32)
        inside = (row_index >= 0) & (row_index < FX)
        clipped = jnp.clip(row_index, 0, FX - 1)
        star_flux = lax.dynamic_index_in_dim(split_flux, star_index, 0, keepdims=False)
        gathered = jnp.take(star_flux, clipped, axis=1)
        ghosts = jnp.where(inside[:, None, None], gathered, jnp.zeros_like(gathered))
        return weno_rates(ghosts)

    hydro_blocks = lax.map(hydro_slab, slab_ids)
    hydro_rhs = hydro_blocks.reshape(STARS, N_BLK, 5, 2 * CX, CY, CZ).transpose(0, 2, 1, 3, 4, 5).reshape(STARS, 5, FX, CY, CZ)
    return bssn_rhs, hydro_rhs
```

```python
import functools
import math

import jax
import jax.numpy as jnp
from jax import lax
from jax.experimental import pallas as pl
from jax.experimental.pallas import tpu as pltpu
from jax.sharding import PartitionSpec as P

pair_index = ((0, 1, 2), (1, 3, 4), (2, 4, 5))
sym_pairs = ((0, 0), (0, 1), (0, 2), (1, 1), (1, 2), (2, 2))
weno_eps = 1e-06
RING = ("star", "blk")
LANES = 128
METRIC = 18
FLUID = 7
ANY = pl.BlockSpec(memory_space=pl.ANY)
F32 = jnp.float32


class Copies:
    def __init__(self, sems):
        self.sems = sems
        self.count = 0
        self.groups = {}

    def start(self, group, src, dst):
        copy = pltpu.make_async_copy(src, dst, self.sems.at[self.count])
        copy.start()
        self.count += 1
        self.groups.setdefault(group, []).append(copy)

    def wait(self, group):
        for copy in self.groups.pop(group):
            copy.wait()

    def wait_all(self):
        for group in list(self.groups):
            self.wait(group)


def metric_pieces(lapse, conf, mean, metric, curv, shift):
    singles = [(n, None, ref) for n, ref in enumerate((lapse, conf, mean))]
    return singles + [(3, 6, metric), (9, 6, curv), (15, 3, shift)]


def pack_kernel(lapse, conf, mean, metric, curv, shift, dens, mom, ener, velo, pres, up, down, sems):
    nx = lapse.shape[0]
    fx = dens.shape[1]
    copies = Copies(sems)
    for buf, first, fluid_first in ((up, nx - 2, fx - 3), (down, 0, 0)):
        for k in range(2):
            for field, count, ref in metric_pieces(lapse, conf, mean, metric, curv, shift):
                at = k * METRIC + field
                if count is None:
                    copies.start(0, ref.at[first + k], buf.at[at])
                else:
                    copies.start(0, ref.at[:, first + k], buf.at[pl.ds(at, count)])
        for k in range(3):
            at = 2 * METRIC + k * FLUID
            row = fluid_first + k
            copies.start(0, dens.at[0, row], buf.at[at])
            copies.start(0, mom.at[0, :, row], buf.at[pl.ds(at + 1, 3)])
            copies.start(0, ener.at[0, row], buf.at[at + 4])
            copies.start(0, velo.at[0, 0, row], buf.at[at + 5])
            copies.start(0, pres.at[0, row], buf.at[at + 6])
    tail = 2 * METRIC + 3 * FLUID
    for k in range(2):
        copies.start(0, velo.at[0, pl.ds(1, 2), fx - 2 + k], up.at[pl.ds(tail + 2 * k, 2)])
    copies.start(0, lapse.at[2], down.at[tail])
    copies.start(0, shift.at[0, 2], down.at[tail + 1])
    copies.start(0, conf.at[2], down.at[tail + 2])
    copies.wait_all()


def bssn_layer(state, sources, out, at, src_at, out_at):
    ny, nz = state.shape[-2:]

    def value(field, off=0):
        return state[field, at + off]

    def rolled(v, axis):
        n = (ny, nz)[axis]
        return tuple(pltpu.roll(v, s % n, axis) for s in (2, 1, -1, -2))

    def first(taps):
        m2, m1, p1, p2 = taps
        return (m2 - p2) + 8.0 * (p1 - m1)

    def second(taps, mid):
        m2, m1, p1, p2 = taps
        return 16.0 * (m1 + p1) - (m2 + p2) - 30.0 * mid

    def xtaps(field):
        return tuple(value(field, o) for o in (-2, -1, 1, 2))

    twelfth = 1.0 / 12.0
    third = 1.0 / 3.0
    lapse = value(0)
    conf = value(1)
    mean = value(2)
    shift12 = [value(15 + n) * twelfth for n in range(3)]

    def gradient(field):
        v = value(field)
        return first(xtaps(field)), first(rolled(v, 0)), first(rolled(v, 1))

    def along_shift(field):
        gx, gy, gz = gradient(field)
        return shift12[0] * gx + shift12[1] * gy + shift12[2] * gz

    dshift = [[None] * 3 for _ in range(3)]
    for n in range(3):
        for k, g in enumerate(gradient(15 + n)):
            dshift[k][n] = g * twelfth
    div_shift = dshift[0][0] + dshift[1][1] + dshift[2][2]
    div23 = (2.0 / 3.0) * div_shift

    taps_x = xtaps(0)
    taps_y = rolled(lapse, 0)
    taps_z = rolled(lapse, 1)
    lx, ly, lz = first(taps_x), first(taps_y), first(taps_z)
    out[0, out_at] = (shift12[0] * lx + shift12[1] * ly + shift12[2] * lz) - 2.0 * lapse * mean
    sq = twelfth * twelfth
    hess = (
        second(taps_x, lapse) * twelfth,
        first(rolled(lx, 0)) * sq,
        first(rolled(lx, 1)) * sq,
        second(taps_y, lapse) * twelfth,
        first(rolled(lz, 0)) * sq,
        second(taps_z, lapse) * twelfth,
    )
    out[1, out_at] = along_shift(1) + conf * ((2.0 / 3.0) * (lapse * mean) - div23)

    a, b, c, d, e, f = g = [value(3 + n) for n in range(6)]
    cof = (d * f - e * e, c * e - b * f, b * e - c * d, a * f - c * c, b * c - a * e, a * d - b * b)
    scale = 1.0 / (a * cof[0] + b * cof[1] + c * cof[2])
    inv = [entry * scale for entry in cof]
    trace = (inv[0] * hess[0] + inv[3] * hess[3] + inv[5] * hess[5]) + 2.0 * (
        inv[1] * hess[1] + inv[2] * hess[2] + inv[4] * hess[4]
    )
    trace3 = trace * third
    curv = [value(9 + n) for n in range(6)]

    def pick(six, i, j):
        return six[pair_index[i][j]]

    def total(terms):
        return functools.reduce(lambda x, y: x + y, terms)

    mixed = [
        [total([pick(curv, i, l) * pick(inv, l, j) for l in range(3)]) for j in range(3)]
        for i in range(3)
    ]
    square = (mixed[0][0] * mixed[0][0] + mixed[1][1] * mixed[1][1] + mixed[2][2] * mixed[2][2]) + 2.0 * (
        mixed[0][1] * mixed[1][0] + mixed[0][2] * mixed[2][0] + mixed[1][2] * mixed[2][1]
    )
    out[2, out_at] = (
        along_shift(2)
        - conf * trace
        + lapse * (square + mean * mean * third + (4.0 * math.pi) * sources[src_at])
    )
    lapse2 = 2.0 * lapse
    mean_lapse = lapse * mean

    def stretched(six, i, j):
        if i == j:
            return 2.0 * total([pick(six, i, k) * dshift[i][k] for k in range(3)])
        return total([pick(six, i, k) * dshift[j][k] + pick(six, j, k) * dshift[i][k] for k in range(3)])

    for p, (i, j) in enumerate(sym_pairs):
        product = total([mixed[i][k] * pick(curv, k, j) for k in range(3)])
        out[9 + p, out_at] = (
            along_shift(9 + p)
            + (mean_lapse - div23) * curv[p]
            - lapse2 * product
            + stretched(curv, i, j)
            - conf * (hess[p] - trace3 * g[p])
        )
    for p, (i, j) in enumerate(sym_pairs):
        out[3 + p, out_at] = along_shift(3 + p) - lapse2 * curv[p] + stretched(g, i, j) - div23 * g[p]


def lane_matrix(nz, weights):
    row = lax.broadcasted_iota(jnp.int32, (nz, nz), 0)
    col = lax.broadcasted_iota(jnp.int32, (nz, nz), 1)
    return weights(row, col)


def dot(x, y):
    return jnp.dot(x, y, precision=lax.Precision.HIGHEST, preferred_element_type=F32)


def restrict_planes(pairs, rows, out, out_first):
    ny, nz = out.shape[-2:]
    half = ny // 2
    quarter_y, quarter_z = ny // 4, nz // 4
    count = len(pairs)
    for n, plane in enumerate(pairs):
        for h in range(nz // LANES):
            rows[h, pl.ds(n * ny, ny), :] = plane()[:, h * LANES : (h + 1) * LANES]
    halves = [
        rows[h, pl.ds(0, count * half, stride=2), :] + rows[h, pl.ds(1, count * half, stride=2), :]
        for h in range(nz // LANES)
    ]
    matrix = lane_matrix(
        nz, lambda r, c: jnp.where(c == quarter_z + lax.shift_right_logical(r, 1), 0.125, 0.0).astype(F32)
    )
    level = dot(jnp.concatenate(halves, axis=1), matrix)
    for n in range(count):
        out[out_first + n] = jnp.zeros((ny, nz), F32)
        out[out_first + n, pl.ds(quarter_y, half), :] = level[n * half : (n + 1) * half]


def prolong_yz(planes, rows, out):
    ny, nz = out.shape[-2:]
    half = ny // 2
    start_y, start_z = ny // 4, nz // 4
    flat = [plane for field in planes for plane in field]
    for n, plane in enumerate(flat):
        mid = 0.75 * plane(pl.ds(start_y, half))
        even = mid + 0.25 * plane(pl.ds(start_y - 1, half))
        odd = mid + 0.25 * plane(pl.ds(start_y + 1, half))
        for h in range(nz // LANES):
            lanes = slice(h * LANES, (h + 1) * LANES)
            rows[h, pl.ds(n * ny, half, stride=2), :] = even[:, lanes]
            rows[h, pl.ds(n * ny + 1, half, stride=2), :] = odd[:, lanes]

    def weights(r, c):
        mid = start_z + lax.shift_right_logical(c, 1)
        side = mid - 1 + 2 * (c & 1)
        return jnp.where(r == mid, 0.75, jnp.where(r == side, 0.25, 0.0)).astype(F32)

    matrix = lane_matrix(nz, weights)
    wide = jnp.concatenate([rows[h, pl.ds(0, len(flat) * ny), :] for h in range(nz // LANES)], axis=1)
    fine = dot(wide, matrix)
    at = 0
    for field, layers in enumerate(planes):
        for n in range(len(layers)):
            out[field, n] = fine[at * ny : (at + 1) * ny]
            at += 1


def split_flux(fluid, lapse, shift, conf, out, out_at, scale=None):
    root = lax.rsqrt(conf)
    transport = lapse * fluid(5) - shift
    weight = lapse * (root * root * root) * fluid(6)
    speed = lapse + jnp.abs(shift)
    for n in range(5):
        u = fluid(n)
        flux = u * transport
        if n == 1:
            flux = flux + weight
        if n == 4:
            flux = flux + weight * fluid(5)
        moved = speed * u
        plus, minus = flux + moved, flux - moved
        if scale is not None:
            plus, minus = plus * scale, minus * scale
        out[n, out_at] = plus
        out[5 + n, out_at] = minus


def weno_cells(flux, field, rows, first, count, emit):
    def differences(which, low, high):
        v = {j: flux[which, j, rows, :] for j in range(low, high + 1)}
        e = {j: v[j + 1] - v[j] for j in range(low, high)}
        d = {j: e[j] - e[j - 1] for j in range(low + 1, high)}
        t = {j: d[j + 1] - d[j] for j in range(low + 1, high - 1)}
        h = {j: 0.5 * d[j] for j in d}
        s = {j: (13.0 / 12.0) * (d[j] * d[j]) + 4.0 * weno_eps for j in d}
        return v, e, d, t, h, s

    faces = range(first - 1, first + count)
    v, e, d, t, h, s = differences(field, first - 3, first + count + 1)
    u, eu, du, tu, hu, su = differences(5 + field, first - 2, first + count + 2)

    def quotient(b0, b1, b2, t0, t2):
        w0, w1, w2 = b1 * b2, b0 * b2, b0 * b1
        w0, w1, w2 = w0 * w0, 6.0 * (w1 * w1), w2 * w2
        return (w0 * t0 + 1.5 * (w2 * t2)) / (w0 + w1 + 3.0 * w2)

    def square(x):
        return x * x

    previous = None
    for i in faces:
        left = quotient(
            s[i - 1] + square(h[i - 1] + e[i - 1]),
            s[i] + square(h[i] + e[i - 1]),
            s[i + 1] + square(h[i + 1] - e[i]),
            t[i - 1],
            t[i],
        )
        right = quotient(
            su[i + 2] + square(hu[i + 2] - eu[i + 1]),
            su[i + 1] + square(hu[i + 1] - eu[i + 1]),
            su[i] + square(hu[i] + eu[i]),
            tu[i + 1],
            tu[i],
        )
        face = (
            3.0 * (v[i] + u[i + 1])
            + 0.5 * (e[i - 1] - eu[i + 1])
            + (e[i] - eu[i])
            + (right - left)
        )
        if previous is not None:
            emit(i, (previous - face) * (1.0 / 3.0))
        previous = face


def local_kernel(
    lapse, conf, mean, metric, curv, shift, dens, mom, ener, velo, pres,
    rates, hydro, flux_out, source_out,
    state, fluid, coarse, flux, sources, rows, stage, hstage, sems,
):
    nx, ny, nz = lapse.shape
    fx = dens.shape[1]
    copies = Copies(sems)
    copies.start("c", lapse, state.at[0])
    copies.start("c", conf, state.at[1])
    copies.start("c", shift, state.at[pl.ds(15, 3)])
    copies.start("f", dens.at[0], fluid.at[0])
    copies.start("f", mom.at[0], fluid.at[pl.ds(1, 3)])
    copies.start("f", ener.at[0], fluid.at[4])
    copies.start("f", velo.at[0, 0], fluid.at[5])
    copies.start("f", pres.at[0], fluid.at[6])
    copies.start("f", velo.at[0, pl.ds(1, 2)], fluid.at[pl.ds(7, 2)])
    copies.start("m", mean, state.at[2])
    copies.start("m", metric, state.at[pl.ds(3, 6)])
    copies.start("m", curv, state.at[pl.ds(9, 6)])

    copies.wait("c")

    def coarse_plane(field, layer):
        return lambda sl: state[field, layer, sl, :]

    prolong_yz([[coarse_plane(f, l) for l in range(nx)] for f in (0, 15, 1)], rows, coarse)
    copies.wait("f")

    good = fx - 3

    @pl.loop(0, good)
    def _(i):
        mid = lax.shift_right_logical(i, 1) + 1
        side = mid - 1 + 2 * (i & 1)
        parts = [0.75 * coarse[n, mid] + 0.25 * coarse[n, side] for n in range(3)]
        split_flux(lambda n: fluid[n, i], *parts, flux, i)

    copies.start("o", flux, flux_out)

    def pair(layer):
        def one(x):
            return (
                fluid[4, x]
                + fluid[0, x]
                + (fluid[1, x] * fluid[5, x] + fluid[2, x] * fluid[7, x] + fluid[3, x] * fluid[8, x])
                + 3.0 * fluid[6, x]
            )

        return lambda: one(2 * layer) + one(2 * layer + 1)

    restrict_planes([pair(l) for l in range(nx - 1)], rows, sources, 1)
    copies.start("o", sources, source_out)

    @pl.loop(0, 5)
    def _(n):
        for part in range(ny // 8):
            sl = pl.ds(part * 8, 8)

            def emit(i, value):
                hstage[n, i - 3, sl, :] = value

            weno_cells(flux, n, sl, 3, fx - 9, emit)

    copies.start("o", hstage, hydro.at[0, :, pl.ds(3, fx - 9)])
    copies.wait("m")

    @pl.loop(0, nx - 4)
    def _(l):
        bssn_layer(state, sources, stage, l + 2, l + 2, l)

    copies.start("o", stage, rates.at[:, pl.ds(2, nx - 4)])
    copies.wait_all()


def halo_kernel(
    inside, below, above, rates_in, hydro_in, flux_in, source_in,
    lapse, conf, mean, metric, curv, shift, dens, mom, ener, velo, pres,
    rates, hydro,
    state, extra, own, fbelow, fabove, coarse, flux, sources, rows, stage, hstage, sems,
):
    nx, ny, nz = lapse.shape
    fx = dens.shape[1]
    copies = Copies(sems)
    tail = 2 * METRIC + 3 * FLUID
    for k in range(2):
        copies.start("m", below.at[pl.ds(k * METRIC, METRIC)], state.at[:, k])
        copies.start("m", above.at[pl.ds(k * METRIC, METRIC)], state.at[:, nx + 2 + k])
    for field, count, ref in metric_pieces(lapse, conf, mean, metric, curv, shift):
        if count is None:
            copies.start("m", ref, state.at[field, pl.ds(2, nx)])
        else:
            copies.start("m", ref, state.at[pl.ds(field, count), pl.ds(2, nx)])
    copies.start("m", above.at[pl.ds(tail, 3)], extra)
    for k in range(3):
        copies.start("f", below.at[pl.ds(2 * METRIC + k * FLUID, FLUID)], fbelow.at[pl.ds(0, FLUID), k])
        copies.start("f", above.at[pl.ds(2 * METRIC + k * FLUID, FLUID)], fabove.at[:, k])
    for k in range(2):
        copies.start("f", below.at[pl.ds(tail + 2 * k, 2)], fbelow.at[pl.ds(FLUID, 2), k + 1])
    last = pl.ds(fx - 3, 3)
    copies.start("f", dens.at[0, last], own.at[0])
    copies.start("f", mom.at[0, :, last], own.at[pl.ds(1, 3)])
    copies.start("f", ener.at[0, last], own.at[4])
    copies.start("f", velo.at[0, 0, last], own.at[5])
    copies.start("f", pres.at[0, last], own.at[6])
    copies.start("s", source_in, sources)
    copies.start("x", flux_in.at[:, pl.ds(0, 6)], flux.at[:, pl.ds(3, 6)])
    copies.start("x", flux_in.at[:, pl.ds(fx - 9, 6)], flux.at[:, pl.ds(fx - 6, 6)])

    copies.wait("m")

    def coarse_plane(field, layer):
        if layer == nx + 2:
            return lambda sl: extra[(0, 15, 1).index(field), sl, :]
        return lambda sl: state[field, layer + 2, sl, :]

    layers = (-1, 0, 1, nx - 1, nx, nx + 1, nx + 2)
    prolong_yz([[coarse_plane(f, l) for l in layers] for f in (0, 15, 1)], rows, coarse)
    copies.wait("f")

    for i in (-3, -2, -1) + tuple(range(fx - 3, fx + 3)):
        mid = i // 2 + 1
        side = mid - 1 + 2 * (i % 2)
        mid, side = layers.index(mid), layers.index(side)
        parts = [0.75 * coarse[n, mid] + 0.25 * coarse[n, side] for n in range(3)]
        if i < 0:
            source, at, scale = fbelow, i + 3, inside[0]
        elif i < fx:
            source, at, scale = own, i - fx + 3, None
        else:
            source, at, scale = fabove, i - fx, inside[1]
        split_flux(lambda n, s=source, a=at: s[n, a], *parts, flux, i + 3, scale)

    copies.wait("x")

    @pl.loop(0, 5)
    def _(n):
        for part in range(ny // 8):
            sl = pl.ds(part * 8, 8)

            def emit_low(i, value):
                hstage[n, i - 3, sl, :] = value

            def emit_high(i, value):
                hstage[n, 3 + i - (fx - 3), sl, :] = value

            weno_cells(flux, n, sl, 3, 3, emit_low)
            weno_cells(flux, n, sl, fx - 3, 6, emit_high)

    copies.start("o", hstage.at[:, pl.ds(0, 3)], hydro.at[0, :, pl.ds(0, 3)])
    copies.start("o", hstage.at[:, pl.ds(3, 6)], hydro.at[0, :, pl.ds(fx - 6, 6)])
    copies.wait("s")

    def pair():
        def one(x):
            return (
                fbelow[4, x]
                + fbelow[0, x]
                + (fbelow[1, x] * fbelow[5, x] + fbelow[2, x] * fbelow[7, x] + fbelow[3, x] * fbelow[8, x])
                + 3.0 * fbelow[6, x]
            )

        return one(1) + one(2)

    restrict_planes([pair], rows, sources, 0)

    @pl.loop(0, 4)
    def _(k):
        l = jnp.where(k < 2, k, k + nx - 4)
        bssn_layer(state, sources, stage, l + 2, l, k)

    copies.start("o", stage.at[:, pl.ds(0, 2)], rates.at[:, pl.ds(0, 2)])
    copies.start("o", stage.at[:, pl.ds(2, 2)], rates.at[:, pl.ds(nx - 2, 2)])
    copies.wait_all()


def on_device(*fields):
    lapse, dens = fields[0], fields[6]
    nx, ny, nz = lapse.shape
    fx = dens.shape[1]
    layer = (ny, nz)

    def shape(*leading):
        return jax.ShapeDtypeStruct(leading + layer, F32)

    def vmem(*leading):
        return pltpu.VMEM(leading + layer, F32)

    tail = 2 * METRIC + 3 * FLUID
    up, down = pl.pallas_call(
        pack_kernel,
        out_shape=(shape(tail + 4), shape(tail + 3)),
        in_specs=[ANY] * 11,
        out_specs=[ANY] * 2,
        scratch_shapes=[pltpu.SemaphoreType.DMA((64,))],
        name="pack",
    )(*fields)
    count = lax.axis_size(RING)
    pairs = [(i, (i + 1) % count) for i in range(count)]
    below = lax.ppermute(up, RING, pairs)
    above = lax.ppermute(down, RING, [(j, i) for i, j in pairs])

    def row_scratch(planes):
        return pltpu.VMEM((nz // LANES, planes * ny, LANES), F32)

    partial = pl.pallas_call(
        local_kernel,
        out_shape=(shape(15, nx), shape(1, 5, fx), shape(10, fx - 3), shape(nx)),
        in_specs=[ANY] * 11,
        out_specs=[ANY] * 4,
        scratch_shapes=[
            vmem(METRIC, nx),
            vmem(9, fx),
            vmem(3, nx),
            vmem(10, fx - 3),
            vmem(nx),
            row_scratch(3 * nx),
            vmem(15, nx - 4),
            vmem(5, fx - 9),
            pltpu.SemaphoreType.DMA((32,)),
        ],
        cost_estimate=pl.CostEstimate(flops=400_000_000, transcendentals=0, bytes_accessed=12_000_000),
        name="local",
    )(*fields)
    place = lax.axis_index("blk")
    inside = jnp.stack([place > 0, place < lax.axis_size("blk") - 1]).astype(F32)
    return pl.pallas_call(
        halo_kernel,
        out_shape=(shape(15, nx), shape(1, 5, fx)),
        in_specs=[pl.BlockSpec(memory_space=pltpu.SMEM)] + [ANY] * 17,
        out_specs=[ANY] * 2,
        input_output_aliases={3: 0, 4: 1},
        scratch_shapes=[
            vmem(METRIC, nx + 4),
            vmem(3),
            vmem(FLUID, 3),
            vmem(9, 3),
            vmem(FLUID, 3),
            vmem(3, 7),
            vmem(10, fx + 6),
            vmem(nx),
            row_scratch(21),
            vmem(15, 4),
            vmem(5, 9),
            pltpu.SemaphoreType.DMA((64,)),
        ],
        cost_estimate=pl.CostEstimate(flops=400_000_000, transcendentals=0, bytes_accessed=12_000_000),
        name="halo",
    )(inside, below, above, *partial, *fields)


def solution(mesh):
    in_specs = (
        P(RING, None, None),
        P(RING, None, None),
        P(RING, None, None),
        P(None, RING, None, None),
        P(None, RING, None, None),
        P(None, RING, None, None),
        P("star", "blk", None, None),
        P("star", None, "blk", None, None),
        P("star", "blk", None, None),
        P("star", None, "blk", None, None),
        P("star", "blk", None, None),
    )
    out_specs = (P(None, RING, None, None), P("star", None, "blk", None, None))
    return jax.shard_map(
        on_device, mesh=mesh, in_specs=in_specs, out_specs=out_specs, check_vma=False
    )
```

```python
import functools
import math

import jax
import jax.numpy as jnp
from jax import lax
from jax.experimental import pallas as pl
from jax.experimental.pallas import tpu as pltpu
from jax.sharding import PartitionSpec as P

pair_index = ((0, 1, 2), (1, 3, 4), (2, 4, 5))
sym_pairs = ((0, 0), (0, 1), (0, 2), (1, 1), (1, 2), (2, 2))
weno_eps = 1e-06
RING = ("star", "blk")
LANES = 128
METRIC = 18
FLUID = 7
ANY = pl.BlockSpec(memory_space=pl.ANY)
VMEM = pl.BlockSpec(memory_space=pltpu.VMEM)
F32 = jnp.float32


class Copies:
    def __init__(self, sems):
        self.sems = sems
        self.count = 0
        self.groups = {}

    def start(self, group, src, dst):
        copy = pltpu.make_async_copy(src, dst, self.sems.at[self.count])
        copy.start()
        self.count += 1
        self.groups.setdefault(group, []).append(copy)

    def wait(self, group):
        for copy in self.groups.pop(group):
            copy.wait()

    def wait_all(self):
        for group in list(self.groups):
            self.wait(group)


def metric_pieces(lapse, conf, mean, metric, curv, shift):
    singles = [(n, None, ref) for n, ref in enumerate((lapse, conf, mean))]
    return singles + [(3, 6, metric), (9, 6, curv), (15, 3, shift)]


def pack_kernel(lapse, conf, mean, metric, curv, shift, dens, mom, ener, velo, pres, up, down, sems):
    nx = lapse.shape[0]
    fx = dens.shape[1]
    copies = Copies(sems)
    for buf, first, fluid_first in ((up, nx - 2, fx - 3), (down, 0, 0)):
        for k in range(2):
            for field, count, ref in metric_pieces(lapse, conf, mean, metric, curv, shift):
                at = k * METRIC + field
                if count is None:
                    copies.start(0, ref.at[first + k], buf.at[at])
                else:
                    copies.start(0, ref.at[:, first + k], buf.at[pl.ds(at, count)])
        for k in range(3):
            at = 2 * METRIC + k * FLUID
            row = fluid_first + k
            copies.start(0, dens.at[0, row], buf.at[at])
            copies.start(0, mom.at[0, :, row], buf.at[pl.ds(at + 1, 3)])
            copies.start(0, ener.at[0, row], buf.at[at + 4])
            copies.start(0, velo.at[0, 0, row], buf.at[at + 5])
            copies.start(0, pres.at[0, row], buf.at[at + 6])
    tail = 2 * METRIC + 3 * FLUID
    for k in range(2):
        copies.start(0, velo.at[0, pl.ds(1, 2), fx - 2 + k], up.at[pl.ds(tail + 2 * k, 2)])
    copies.start(0, lapse.at[2], down.at[tail])
    copies.start(0, shift.at[0, 2], down.at[tail + 1])
    copies.start(0, conf.at[2], down.at[tail + 2])
    copies.wait_all()


def bssn_layer(state, sources, out, at, src_at, out_at):
    ny, nz = state.shape[-2:]

    def value(field, off=0):
        return state[field, at + off]

    def rolled(v, axis):
        n = (ny, nz)[axis]
        return tuple(pltpu.roll(v, s % n, axis) for s in (2, 1, -1, -2))

    def first(taps):
        m2, m1, p1, p2 = taps
        return (m2 - p2) + 8.0 * (p1 - m1)

    def second(taps, mid):
        m2, m1, p1, p2 = taps
        return 16.0 * (m1 + p1) - (m2 + p2) - 30.0 * mid

    def xtaps(field):
        return tuple(value(field, o) for o in (-2, -1, 1, 2))

    twelfth = 1.0 / 12.0
    third = 1.0 / 3.0
    lapse = value(0)
    conf = value(1)
    mean = value(2)
    shift12 = [value(15 + n) * twelfth for n in range(3)]

    def gradient(field):
        v = value(field)
        return first(xtaps(field)), first(rolled(v, 0)), first(rolled(v, 1))

    def along_shift(field):
        gx, gy, gz = gradient(field)
        return shift12[0] * gx + shift12[1] * gy + shift12[2] * gz

    dshift = [[None] * 3 for _ in range(3)]
    for n in range(3):
        for k, g in enumerate(gradient(15 + n)):
            dshift[k][n] = g * twelfth
    div_shift = dshift[0][0] + dshift[1][1] + dshift[2][2]
    div23 = (2.0 / 3.0) * div_shift

    taps_x = xtaps(0)
    taps_y = rolled(lapse, 0)
    taps_z = rolled(lapse, 1)
    lx, ly, lz = first(taps_x), first(taps_y), first(taps_z)
    out[0, out_at] = (shift12[0] * lx + shift12[1] * ly + shift12[2] * lz) - 2.0 * lapse * mean
    sq = twelfth * twelfth
    hess = (
        second(taps_x, lapse) * twelfth,
        first(rolled(lx, 0)) * sq,
        first(rolled(lx, 1)) * sq,
        second(taps_y, lapse) * twelfth,
        first(rolled(lz, 0)) * sq,
        second(taps_z, lapse) * twelfth,
    )
    out[1, out_at] = along_shift(1) + conf * ((2.0 / 3.0) * (lapse * mean) - div23)

    a, b, c, d, e, f = g = [value(3 + n) for n in range(6)]
    cof = (d * f - e * e, c * e - b * f, b * e - c * d, a * f - c * c, b * c - a * e, a * d - b * b)
    scale = 1.0 / (a * cof[0] + b * cof[1] + c * cof[2])
    inv = [entry * scale for entry in cof]
    trace = (inv[0] * hess[0] + inv[3] * hess[3] + inv[5] * hess[5]) + 2.0 * (
        inv[1] * hess[1] + inv[2] * hess[2] + inv[4] * hess[4]
    )
    trace3 = trace * third
    curv = [value(9 + n) for n in range(6)]

    def pick(six, i, j):
        return six[pair_index[i][j]]

    def total(terms):
        return functools.reduce(lambda x, y: x + y, terms)

    mixed = [
        [total([pick(curv, i, l) * pick(inv, l, j) for l in range(3)]) for j in range(3)]
        for i in range(3)
    ]
    square = (mixed[0][0] * mixed[0][0] + mixed[1][1] * mixed[1][1] + mixed[2][2] * mixed[2][2]) + 2.0 * (
        mixed[0][1] * mixed[1][0] + mixed[0][2] * mixed[2][0] + mixed[1][2] * mixed[2][1]
    )
    out[2, out_at] = (
        along_shift(2)
        - conf * trace
        + lapse * (square + mean * mean * third + (4.0 * math.pi) * sources[src_at])
    )
    lapse2 = 2.0 * lapse
    mean_lapse = lapse * mean

    def stretched(six, i, j):
        if i == j:
            return 2.0 * total([pick(six, i, k) * dshift[i][k] for k in range(3)])
        return total([pick(six, i, k) * dshift[j][k] + pick(six, j, k) * dshift[i][k] for k in range(3)])

    for p, (i, j) in enumerate(sym_pairs):
        product = total([mixed[i][k] * pick(curv, k, j) for k in range(3)])
        out[9 + p, out_at] = (
            along_shift(9 + p)
            + (mean_lapse - div23) * curv[p]
            - lapse2 * product
            + stretched(curv, i, j)
            - conf * (hess[p] - trace3 * g[p])
        )
    for p, (i, j) in enumerate(sym_pairs):
        out[3 + p, out_at] = along_shift(3 + p) - lapse2 * curv[p] + stretched(g, i, j) - div23 * g[p]


def lane_matrix(nz, weights):
    row = lax.broadcasted_iota(jnp.int32, (nz, nz), 0)
    col = lax.broadcasted_iota(jnp.int32, (nz, nz), 1)
    return weights(row, col)


def dot(x, y):
    return jnp.dot(x, y, precision=lax.Precision.HIGHEST, preferred_element_type=F32)


def restrict_planes(pairs, rows, out, out_first):
    ny, nz = out.shape[-2:]
    half = ny // 2
    quarter_y, quarter_z = ny // 4, nz // 4
    count = len(pairs)
    for n, plane in enumerate(pairs):
        for h in range(nz // LANES):
            rows[h, pl.ds(n * ny, ny), :] = plane()[:, h * LANES : (h + 1) * LANES]
    halves = [
        rows[h, pl.ds(0, count * half, stride=2), :] + rows[h, pl.ds(1, count * half, stride=2), :]
        for h in range(nz // LANES)
    ]
    matrix = lane_matrix(
        nz, lambda r, c: jnp.where(c == quarter_z + lax.shift_right_logical(r, 1), 0.125, 0.0).astype(F32)
    )
    level = dot(jnp.concatenate(halves, axis=1), matrix)
    for n in range(count):
        out[out_first + n] = jnp.zeros((ny, nz), F32)
        out[out_first + n, pl.ds(quarter_y, half), :] = level[n * half : (n + 1) * half]


def prolong_yz(planes, rows, out):
    ny, nz = out.shape[-2:]
    half = ny // 2
    start_y, start_z = ny // 4, nz // 4
    flat = [plane for field in planes for plane in field]
    for n, plane in enumerate(flat):
        mid = 0.75 * plane(pl.ds(start_y, half))
        even = mid + 0.25 * plane(pl.ds(start_y - 1, half))
        odd = mid + 0.25 * plane(pl.ds(start_y + 1, half))
        for h in range(nz // LANES):
            lanes = slice(h * LANES, (h + 1) * LANES)
            rows[h, pl.ds(n * ny, half, stride=2), :] = even[:, lanes]
            rows[h, pl.ds(n * ny + 1, half, stride=2), :] = odd[:, lanes]

    def weights(r, c):
        mid = start_z + lax.shift_right_logical(c, 1)
        side = mid - 1 + 2 * (c & 1)
        return jnp.where(r == mid, 0.75, jnp.where(r == side, 0.25, 0.0)).astype(F32)

    matrix = lane_matrix(nz, weights)
    wide = jnp.concatenate([rows[h, pl.ds(0, len(flat) * ny), :] for h in range(nz // LANES)], axis=1)
    fine = dot(wide, matrix)
    at = 0
    for field, layers in enumerate(planes):
        for n in range(len(layers)):
            out[field, n] = fine[at * ny : (at + 1) * ny]
            at += 1


def split_flux(fluid, lapse, shift, conf, out, out_at, scale=None):
    root = lax.rsqrt(conf)
    transport = lapse * fluid(5) - shift
    weight = lapse * (root * root * root) * fluid(6)
    speed = lapse + jnp.abs(shift)
    for n in range(5):
        u = fluid(n)
        flux = u * transport
        if n == 1:
            flux = flux + weight
        if n == 4:
            flux = flux + weight * fluid(5)
        moved = speed * u
        plus, minus = flux + moved, flux - moved
        if scale is not None:
            plus, minus = plus * scale, minus * scale
        out[n, out_at] = plus
        out[5 + n, out_at] = minus


def weno_cells(flux, field, rows, first, count, emit):
    def differences(which, low, high):
        v = {j: flux[which, j, rows, :] for j in range(low, high + 1)}
        e = {j: v[j + 1] - v[j] for j in range(low, high)}
        d = {j: e[j] - e[j - 1] for j in range(low + 1, high)}
        t = {j: d[j + 1] - d[j] for j in range(low + 1, high - 1)}
        h = {j: 0.5 * d[j] for j in d}
        s = {j: (13.0 / 12.0) * (d[j] * d[j]) + 4.0 * weno_eps for j in d}
        return v, e, d, t, h, s

    faces = range(first - 1, first + count)
    v, e, d, t, h, s = differences(field, first - 3, first + count + 1)
    u, eu, du, tu, hu, su = differences(5 + field, first - 2, first + count + 2)

    def quotient(b0, b1, b2, t0, t2):
        w0, w1, w2 = b1 * b2, b0 * b2, b0 * b1
        w0, w1, w2 = w0 * w0, 6.0 * (w1 * w1), w2 * w2
        return (w0 * t0 + 1.5 * (w2 * t2)) / (w0 + w1 + 3.0 * w2)

    def square(x):
        return x * x

    previous = None
    for i in faces:
        left = quotient(
            s[i - 1] + square(h[i - 1] + e[i - 1]),
            s[i] + square(h[i] + e[i - 1]),
            s[i + 1] + square(h[i + 1] - e[i]),
            t[i - 1],
            t[i],
        )
        right = quotient(
            su[i + 2] + square(hu[i + 2] - eu[i + 1]),
            su[i + 1] + square(hu[i + 1] - eu[i + 1]),
            su[i] + square(hu[i] + eu[i]),
            tu[i + 1],
            tu[i],
        )
        face = (
            3.0 * (v[i] + u[i + 1])
            + 0.5 * (e[i - 1] - eu[i + 1])
            + (e[i] - eu[i])
            + (right - left)
        )
        if previous is not None:
            emit(i, (previous - face) * (1.0 / 3.0))
        previous = face


def local_kernel(
    lapse, conf, mean, metric, curv, shift, dens, mom, ener, velo, pres,
    rates, hydro, flux_out, source_out,
    state, fluid, coarse, flux, sources, rows, stage, hstage, sems,
):
    nx, ny, nz = lapse.shape
    fx = dens.shape[1]
    copies = Copies(sems)
    copies.start("c", lapse, state.at[0])
    copies.start("c", conf, state.at[1])
    copies.start("c", shift, state.at[pl.ds(15, 3)])
    copies.start("f", dens.at[0], fluid.at[0])
    copies.start("f", mom.at[0], fluid.at[pl.ds(1, 3)])
    copies.start("f", ener.at[0], fluid.at[4])
    copies.start("f", velo.at[0, 0], fluid.at[5])
    copies.start("f", pres.at[0], fluid.at[6])
    copies.start("f", velo.at[0, pl.ds(1, 2)], fluid.at[pl.ds(7, 2)])
    copies.start("m", mean, state.at[2])
    copies.start("m", metric, state.at[pl.ds(3, 6)])
    copies.start("m", curv, state.at[pl.ds(9, 6)])

    copies.wait("c")

    def coarse_plane(field, layer):
        return lambda sl: state[field, layer, sl, :]

    prolong_yz([[coarse_plane(f, l) for l in range(nx)] for f in (0, 15, 1)], rows, coarse)
    copies.wait("f")

    good = fx - 3

    @pl.loop(0, good)
    def _(i):
        mid = lax.shift_right_logical(i, 1) + 1
        side = mid - 1 + 2 * (i & 1)
        parts = [0.75 * coarse[n, mid] + 0.25 * coarse[n, side] for n in range(3)]
        split_flux(lambda n: fluid[n, i], *parts, flux, i)

    copies.start("o", flux, flux_out)

    def pair(layer):
        def one(x):
            return (
                fluid[4, x]
                + fluid[0, x]
                + (fluid[1, x] * fluid[5, x] + fluid[2, x] * fluid[7, x] + fluid[3, x] * fluid[8, x])
                + 3.0 * fluid[6, x]
            )

        return lambda: one(2 * layer) + one(2 * layer + 1)

    restrict_planes([pair(l) for l in range(nx - 1)], rows, sources, 1)
    copies.start("o", sources, source_out)

    @pl.loop(0, 5)
    def _(n):
        for part in range(ny // 8):
            sl = pl.ds(part * 8, 8)

            def emit(i, value):
                hstage[n, i - 3, sl, :] = value

            weno_cells(flux, n, sl, 3, fx - 9, emit)

    copies.start("o", hstage, hydro.at[0, :, pl.ds(3, fx - 9)])
    copies.wait("m")

    @pl.loop(0, nx - 4)
    def _(l):
        bssn_layer(state, sources, stage, l + 2, l + 2, l)

    copies.start("o", stage, rates.at[:, pl.ds(2, nx - 4)])
    copies.wait_all()


def halo_kernel(
    below, above, rates_in, hydro_in, flux_in, source_in,
    lapse, conf, mean, metric, curv, shift, dens, mom, ener, velo, pres,
    rates, hydro,
    state, extra, own, fbelow, fabove, coarse, flux, sources, rows, stage, hstage, sems,
):
    nx, ny, nz = lapse.shape
    fx = dens.shape[1]
    copies = Copies(sems)
    tail = 2 * METRIC + 3 * FLUID
    place = lax.axis_index("blk")
    inside = (
        jnp.where(place > 0, 1.0, 0.0).astype(F32),
        jnp.where(place < lax.axis_size("blk") - 1, 1.0, 0.0).astype(F32),
    )
    for k in range(2):
        copies.start("m", below.at[pl.ds(k * METRIC, METRIC)], state.at[:, k])
        copies.start("m", above.at[pl.ds(k * METRIC, METRIC)], state.at[:, nx + 2 + k])
    for field, count, ref in metric_pieces(lapse, conf, mean, metric, curv, shift):
        if count is None:
            copies.start("m", ref, state.at[field, pl.ds(2, nx)])
        else:
            copies.start("m", ref, state.at[pl.ds(field, count), pl.ds(2, nx)])
    copies.start("m", above.at[pl.ds(tail, 3)], extra)
    for k in range(3):
        copies.start("f", below.at[pl.ds(2 * METRIC + k * FLUID, FLUID)], fbelow.at[pl.ds(0, FLUID), k])
        copies.start("f", above.at[pl.ds(2 * METRIC + k * FLUID, FLUID)], fabove.at[:, k])
    for k in range(2):
        copies.start("f", below.at[pl.ds(tail + 2 * k, 2)], fbelow.at[pl.ds(FLUID, 2), k + 1])
    last = pl.ds(fx - 3, 3)
    copies.start("f", dens.at[0, last], own.at[0])
    copies.start("f", mom.at[0, :, last], own.at[pl.ds(1, 3)])
    copies.start("f", ener.at[0, last], own.at[4])
    copies.start("f", velo.at[0, 0, last], own.at[5])
    copies.start("f", pres.at[0, last], own.at[6])
    copies.start("s", source_in, sources)
    copies.start("x", flux_in.at[:, pl.ds(0, 6)], flux.at[:, pl.ds(3, 6)])
    copies.start("x", flux_in.at[:, pl.ds(fx - 9, 6)], flux.at[:, pl.ds(fx - 6, 6)])

    copies.wait("m")

    def coarse_plane(field, layer):
        if layer == nx + 2:
            return lambda sl: extra[(0, 15, 1).index(field), sl, :]
        return lambda sl: state[field, layer + 2, sl, :]

    layers = (-1, 0, 1, nx - 1, nx, nx + 1, nx + 2)
    prolong_yz([[coarse_plane(f, l) for l in layers] for f in (0, 15, 1)], rows, coarse)
    copies.wait("f")

    for i in (-3, -2, -1) + tuple(range(fx - 3, fx + 3)):
        mid = i // 2 + 1
        side = mid - 1 + 2 * (i % 2)
        mid, side = layers.index(mid), layers.index(side)
        parts = [0.75 * coarse[n, mid] + 0.25 * coarse[n, side] for n in range(3)]
        if i < 0:
            source, at, scale = fbelow, i + 3, inside[0]
        elif i < fx:
            source, at, scale = own, i - fx + 3, None
        else:
            source, at, scale = fabove, i - fx, inside[1]
        split_flux(lambda n, s=source, a=at: s[n, a], *parts, flux, i + 3, scale)

    copies.wait("x")

    @pl.loop(0, 5)
    def _(n):
        for part in range(ny // 8):
            sl = pl.ds(part * 8, 8)

            def emit_low(i, value):
                hstage[n, i - 3, sl, :] = value

            def emit_high(i, value):
                hstage[n, 3 + i - (fx - 3), sl, :] = value

            weno_cells(flux, n, sl, 3, 3, emit_low)
            weno_cells(flux, n, sl, fx - 3, 6, emit_high)

    copies.start("o", hstage.at[:, pl.ds(0, 3)], hydro.at[0, :, pl.ds(0, 3)])
    copies.start("o", hstage.at[:, pl.ds(3, 6)], hydro.at[0, :, pl.ds(fx - 6, 6)])
    copies.wait("s")

    def pair():
        def one(x):
            return (
                fbelow[4, x]
                + fbelow[0, x]
                + (fbelow[1, x] * fbelow[5, x] + fbelow[2, x] * fbelow[7, x] + fbelow[3, x] * fbelow[8, x])
                + 3.0 * fbelow[6, x]
            )

        return one(1) + one(2)

    restrict_planes([pair], rows, sources, 0)

    @pl.loop(0, 4)
    def _(k):
        l = jnp.where(k < 2, k, k + nx - 4)
        bssn_layer(state, sources, stage, l + 2, l, k)

    copies.start("o", stage.at[:, pl.ds(0, 2)], rates.at[:, pl.ds(0, 2)])
    copies.start("o", stage.at[:, pl.ds(2, 2)], rates.at[:, pl.ds(nx - 2, 2)])
    copies.wait_all()


def on_device(*fields):
    lapse, dens = fields[0], fields[6]
    nx, ny, nz = lapse.shape
    fx = dens.shape[1]
    layer = (ny, nz)

    def shape(*leading):
        return jax.ShapeDtypeStruct(leading + layer, F32)

    def vmem(*leading):
        return pltpu.VMEM(leading + layer, F32)

    tail = 2 * METRIC + 3 * FLUID
    up, down = pl.pallas_call(
        pack_kernel,
        out_shape=(shape(tail + 4), shape(tail + 3)),
        in_specs=[ANY] * 11,
        out_specs=[VMEM] * 2,
        scratch_shapes=[pltpu.SemaphoreType.DMA((64,))],
        name="pack",
    )(*fields)
    count = lax.axis_size(RING)
    pairs = [(i, (i + 1) % count) for i in range(count)]
    below = lax.ppermute(up, RING, pairs)
    above = lax.ppermute(down, RING, [(j, i) for i, j in pairs])

    def row_scratch(planes):
        return pltpu.VMEM((nz // LANES, planes * ny, LANES), F32)

    partial = pl.pallas_call(
        local_kernel,
        out_shape=(shape(15, nx), shape(1, 5, fx), shape(10, fx - 3), shape(nx)),
        in_specs=[ANY] * 11,
        out_specs=[ANY] * 4,
        scratch_shapes=[
            vmem(METRIC, nx),
            vmem(9, fx),
            vmem(3, nx),
            vmem(10, fx - 3),
            vmem(nx),
            row_scratch(3 * nx),
            vmem(15, nx - 4),
            vmem(5, fx - 9),
            pltpu.SemaphoreType.DMA((32,)),
        ],
        cost_estimate=pl.CostEstimate(flops=400_000_000, transcendentals=0, bytes_accessed=12_000_000),
        name="local",
    )(*fields)
    return pl.pallas_call(
        halo_kernel,
        out_shape=(shape(15, nx), shape(1, 5, fx)),
        in_specs=[VMEM] * 2 + [ANY] * 15,
        out_specs=[ANY] * 2,
        input_output_aliases={2: 0, 3: 1},
        scratch_shapes=[
            vmem(METRIC, nx + 4),
            vmem(3),
            vmem(FLUID, 3),
            vmem(9, 3),
            vmem(FLUID, 3),
            vmem(3, 7),
            vmem(10, fx + 6),
            vmem(nx),
            row_scratch(21),
            vmem(15, 4),
            vmem(5, 9),
            pltpu.SemaphoreType.DMA((64,)),
        ],
        cost_estimate=pl.CostEstimate(flops=400_000_000, transcendentals=0, bytes_accessed=12_000_000),
        name="halo",
    )(below, above, *partial, *fields)


def solution(mesh):
    in_specs = (
        P(RING, None, None),
        P(RING, None, None),
        P(RING, None, None),
        P(None, RING, None, None),
        P(None, RING, None, None),
        P(None, RING, None, None),
        P("star", "blk", None, None),
        P("star", None, "blk", None, None),
        P("star", "blk", None, None),
        P("star", None, "blk", None, None),
        P("star", "blk", None, None),
    )
    out_specs = (P(None, RING, None, None), P("star", None, "blk", None, None))
    return jax.shard_map(
        on_device, mesh=mesh, in_specs=in_specs, out_specs=out_specs, check_vma=False
    )
```

```python
import functools
import math

import jax
import jax.numpy as jnp
from jax import lax
from jax.experimental import pallas as pl
from jax.experimental.pallas import tpu as pltpu
from jax.sharding import PartitionSpec as P

pair_index = ((0, 1, 2), (1, 3, 4), (2, 4, 5))
sym_pairs = ((0, 0), (0, 1), (0, 2), (1, 1), (1, 2), (2, 2))
weno_eps = 1e-06
RING = ("star", "blk")
LANES = 128
METRIC = 18
FLUID = 7
ANY = pl.BlockSpec(memory_space=pl.ANY)
GRANT = 24 * 1024 * 1024
VMEM = pl.BlockSpec(memory_space=pltpu.VMEM)
F32 = jnp.float32


class Copies:
    def __init__(self, sems):
        self.sems = sems
        self.count = 0
        self.groups = {}

    def start(self, group, src, dst):
        copy = pltpu.make_async_copy(src, dst, self.sems.at[self.count])
        copy.start()
        self.count += 1
        self.groups.setdefault(group, []).append(copy)

    def wait(self, group):
        for copy in self.groups.pop(group):
            copy.wait()

    def wait_all(self):
        for group in list(self.groups):
            self.wait(group)


def metric_pieces(lapse, conf, mean, metric, curv, shift):
    singles = [(n, None, ref) for n, ref in enumerate((lapse, conf, mean))]
    return singles + [(3, 6, metric), (9, 6, curv), (15, 3, shift)]


def pack_kernel(lapse, conf, mean, metric, curv, shift, dens, mom, ener, velo, pres, up, down, sems):
    nx = lapse.shape[0]
    fx = dens.shape[1]
    copies = Copies(sems)
    for buf, first, fluid_first in ((up, nx - 2, fx - 3), (down, 0, 0)):
        for k in range(2):
            for field, count, ref in metric_pieces(lapse, conf, mean, metric, curv, shift):
                at = k * METRIC + field
                if count is None:
                    copies.start(0, ref.at[first + k], buf.at[at])
                else:
                    copies.start(0, ref.at[:, first + k], buf.at[pl.ds(at, count)])
        for k in range(3):
            at = 2 * METRIC + k * FLUID
            row = fluid_first + k
            copies.start(0, dens.at[0, row], buf.at[at])
            copies.start(0, mom.at[0, :, row], buf.at[pl.ds(at + 1, 3)])
            copies.start(0, ener.at[0, row], buf.at[at + 4])
            copies.start(0, velo.at[0, 0, row], buf.at[at + 5])
            copies.start(0, pres.at[0, row], buf.at[at + 6])
    tail = 2 * METRIC + 3 * FLUID
    for k in range(2):
        copies.start(0, velo.at[0, pl.ds(1, 2), fx - 2 + k], up.at[pl.ds(tail + 2 * k, 2)])
    copies.start(0, lapse.at[2], down.at[tail])
    copies.start(0, shift.at[0, 2], down.at[tail + 1])
    copies.start(0, conf.at[2], down.at[tail + 2])
    copies.wait_all()


def bssn_layer(state, sources, out, at, src_at, out_at):
    ny, nz = state.shape[-2:]

    def value(field, off=0):
        return state[field, at + off]

    def rolled(v, axis):
        n = (ny, nz)[axis]
        return tuple(pltpu.roll(v, s % n, axis) for s in (2, 1, -1, -2))

    def first(taps):
        m2, m1, p1, p2 = taps
        return (m2 - p2) + 8.0 * (p1 - m1)

    def second(taps, mid):
        m2, m1, p1, p2 = taps
        return 16.0 * (m1 + p1) - (m2 + p2) - 30.0 * mid

    def xtaps(field):
        return tuple(value(field, o) for o in (-2, -1, 1, 2))

    twelfth = 1.0 / 12.0
    third = 1.0 / 3.0
    lapse = value(0)
    conf = value(1)
    mean = value(2)
    shift12 = [value(15 + n) * twelfth for n in range(3)]

    def gradient(field):
        v = value(field)
        return first(xtaps(field)), first(rolled(v, 0)), first(rolled(v, 1))

    def along_shift(field):
        gx, gy, gz = gradient(field)
        return shift12[0] * gx + shift12[1] * gy + shift12[2] * gz

    dshift = [[None] * 3 for _ in range(3)]
    for n in range(3):
        for k, g in enumerate(gradient(15 + n)):
            dshift[k][n] = g * twelfth
    div_shift = dshift[0][0] + dshift[1][1] + dshift[2][2]
    div23 = (2.0 / 3.0) * div_shift

    taps_x = xtaps(0)
    taps_y = rolled(lapse, 0)
    taps_z = rolled(lapse, 1)
    lx, ly, lz = first(taps_x), first(taps_y), first(taps_z)
    out[0, out_at] = (shift12[0] * lx + shift12[1] * ly + shift12[2] * lz) - 2.0 * lapse * mean
    sq = twelfth * twelfth
    hess = (
        second(taps_x, lapse) * twelfth,
        first(rolled(lx, 0)) * sq,
        first(rolled(lx, 1)) * sq,
        second(taps_y, lapse) * twelfth,
        first(rolled(lz, 0)) * sq,
        second(taps_z, lapse) * twelfth,
    )
    out[1, out_at] = along_shift(1) + conf * ((2.0 / 3.0) * (lapse * mean) - div23)

    a, b, c, d, e, f = g = [value(3 + n) for n in range(6)]
    cof = (d * f - e * e, c * e - b * f, b * e - c * d, a * f - c * c, b * c - a * e, a * d - b * b)
    scale = 1.0 / (a * cof[0] + b * cof[1] + c * cof[2])
    inv = [entry * scale for entry in cof]
    trace = (inv[0] * hess[0] + inv[3] * hess[3] + inv[5] * hess[5]) + 2.0 * (
        inv[1] * hess[1] + inv[2] * hess[2] + inv[4] * hess[4]
    )
    trace3 = trace * third
    curv = [value(9 + n) for n in range(6)]

    def pick(six, i, j):
        return six[pair_index[i][j]]

    def total(terms):
        return functools.reduce(lambda x, y: x + y, terms)

    mixed = [
        [total([pick(curv, i, l) * pick(inv, l, j) for l in range(3)]) for j in range(3)]
        for i in range(3)
    ]
    square = (mixed[0][0] * mixed[0][0] + mixed[1][1] * mixed[1][1] + mixed[2][2] * mixed[2][2]) + 2.0 * (
        mixed[0][1] * mixed[1][0] + mixed[0][2] * mixed[2][0] + mixed[1][2] * mixed[2][1]
    )
    out[2, out_at] = (
        along_shift(2)
        - conf * trace
        + lapse * (square + mean * mean * third + (4.0 * math.pi) * sources[src_at])
    )
    lapse2 = 2.0 * lapse
    mean_lapse = lapse * mean

    def stretched(six, i, j):
        if i == j:
            return 2.0 * total([pick(six, i, k) * dshift[i][k] for k in range(3)])
        return total([pick(six, i, k) * dshift[j][k] + pick(six, j, k) * dshift[i][k] for k in range(3)])

    for p, (i, j) in enumerate(sym_pairs):
        product = total([mixed[i][k] * pick(curv, k, j) for k in range(3)])
        out[9 + p, out_at] = (
            along_shift(9 + p)
            + (mean_lapse - div23) * curv[p]
            - lapse2 * product
            + stretched(curv, i, j)
            - conf * (hess[p] - trace3 * g[p])
        )
    for p, (i, j) in enumerate(sym_pairs):
        out[3 + p, out_at] = along_shift(3 + p) - lapse2 * curv[p] + stretched(g, i, j) - div23 * g[p]


def lane_matrix(nz, weights):
    row = lax.broadcasted_iota(jnp.int32, (nz, nz), 0)
    col = lax.broadcasted_iota(jnp.int32, (nz, nz), 1)
    return weights(row, col)


def dot(x, y):
    return jnp.dot(x, y, precision=lax.Precision.HIGHEST, preferred_element_type=F32)


def restrict_planes(pairs, rows, out, out_first):
    ny, nz = out.shape[-2:]
    half = ny // 2
    quarter_y, quarter_z = ny // 4, nz // 4
    count = len(pairs)
    for n, plane in enumerate(pairs):
        for h in range(nz // LANES):
            rows[h, pl.ds(n * ny, ny), :] = plane()[:, h * LANES : (h + 1) * LANES]
    halves = [
        rows[h, pl.ds(0, count * half, stride=2), :] + rows[h, pl.ds(1, count * half, stride=2), :]
        for h in range(nz // LANES)
    ]
    matrix = lane_matrix(
        nz, lambda r, c: jnp.where(c == quarter_z + lax.shift_right_logical(r, 1), 0.125, 0.0).astype(F32)
    )
    level = dot(jnp.concatenate(halves, axis=1), matrix)
    for n in range(count):
        out[out_first + n] = jnp.zeros((ny, nz), F32)
        out[out_first + n, pl.ds(quarter_y, half), :] = level[n * half : (n + 1) * half]


def prolong_yz(planes, rows, out):
    ny, nz = out.shape[-2:]
    half = ny // 2
    start_y, start_z = ny // 4, nz // 4
    flat = [plane for field in planes for plane in field]
    for n, plane in enumerate(flat):
        mid = 0.75 * plane(pl.ds(start_y, half))
        even = mid + 0.25 * plane(pl.ds(start_y - 1, half))
        odd = mid + 0.25 * plane(pl.ds(start_y + 1, half))
        for h in range(nz // LANES):
            lanes = slice(h * LANES, (h + 1) * LANES)
            rows[h, pl.ds(n * ny, half, stride=2), :] = even[:, lanes]
            rows[h, pl.ds(n * ny + 1, half, stride=2), :] = odd[:, lanes]

    def weights(r, c):
        mid = start_z + lax.shift_right_logical(c, 1)
        side = mid - 1 + 2 * (c & 1)
        return jnp.where(r == mid, 0.75, jnp.where(r == side, 0.25, 0.0)).astype(F32)

    matrix = lane_matrix(nz, weights)
    wide = jnp.concatenate([rows[h, pl.ds(0, len(flat) * ny), :] for h in range(nz // LANES)], axis=1)
    fine = dot(wide, matrix)
    at = 0
    for field, layers in enumerate(planes):
        for n in range(len(layers)):
            out[field, n] = fine[at * ny : (at + 1) * ny]
            at += 1


def split_flux(fluid, lapse, shift, conf, out, out_at, scale=None):
    root = lax.rsqrt(conf)
    transport = lapse * fluid(5) - shift
    weight = lapse * (root * root * root) * fluid(6)
    speed = lapse + jnp.abs(shift)
    for n in range(5):
        u = fluid(n)
        flux = u * transport
        if n == 1:
            flux = flux + weight
        if n == 4:
            flux = flux + weight * fluid(5)
        moved = speed * u
        plus, minus = flux + moved, flux - moved
        if scale is not None:
            plus, minus = plus * scale, minus * scale
        out[n, out_at] = plus
        out[5 + n, out_at] = minus


def weno_cells(flux, field, rows, first, count, emit):
    def differences(which, low, high):
        v = {j: flux[which, j, rows, :] for j in range(low, high + 1)}
        e = {j: v[j + 1] - v[j] for j in range(low, high)}
        d = {j: e[j] - e[j - 1] for j in range(low + 1, high)}
        t = {j: d[j + 1] - d[j] for j in range(low + 1, high - 1)}
        h = {j: 0.5 * d[j] for j in d}
        s = {j: (13.0 / 12.0) * (d[j] * d[j]) + 4.0 * weno_eps for j in d}
        return v, e, d, t, h, s

    faces = range(first - 1, first + count)
    v, e, d, t, h, s = differences(field, first - 3, first + count + 1)
    u, eu, du, tu, hu, su = differences(5 + field, first - 2, first + count + 2)

    def quotient(b0, b1, b2, t0, t2):
        w0, w1, w2 = b1 * b2, b0 * b2, b0 * b1
        w0, w1, w2 = w0 * w0, 6.0 * (w1 * w1), w2 * w2
        return (w0 * t0 + 1.5 * (w2 * t2)) / (w0 + w1 + 3.0 * w2)

    def square(x):
        return x * x

    previous = None
    for i in faces:
        left = quotient(
            s[i - 1] + square(h[i - 1] + e[i - 1]),
            s[i] + square(h[i] + e[i - 1]),
            s[i + 1] + square(h[i + 1] - e[i]),
            t[i - 1],
            t[i],
        )
        right = quotient(
            su[i + 2] + square(hu[i + 2] - eu[i + 1]),
            su[i + 1] + square(hu[i + 1] - eu[i + 1]),
            su[i] + square(hu[i] + eu[i]),
            tu[i + 1],
            tu[i],
        )
        face = (
            3.0 * (v[i] + u[i + 1])
            + 0.5 * (e[i - 1] - eu[i + 1])
            + (e[i] - eu[i])
            + (right - left)
        )
        if previous is not None:
            emit(i, (previous - face) * (1.0 / 3.0))
        previous = face


def local_kernel(
    lapse, conf, mean, metric, curv, shift, dens, mom, ener, velo, pres,
    rates, hydro, flux_out, source_out,
    state, fluid, coarse, flux, sources, rows, stage, hstage, sems,
):
    nx, ny, nz = lapse.shape
    fx = dens.shape[1]
    copies = Copies(sems)
    copies.start("c", lapse, state.at[0])
    copies.start("c", conf, state.at[1])
    copies.start("c", shift, state.at[pl.ds(15, 3)])
    copies.start("f", dens.at[0], fluid.at[0])
    copies.start("f", mom.at[0], fluid.at[pl.ds(1, 3)])
    copies.start("f", ener.at[0], fluid.at[4])
    copies.start("f", velo.at[0, 0], fluid.at[5])
    copies.start("f", pres.at[0], fluid.at[6])
    copies.start("f", velo.at[0, pl.ds(1, 2)], fluid.at[pl.ds(7, 2)])
    copies.start("m", mean, state.at[2])
    copies.start("m", metric, state.at[pl.ds(3, 6)])
    copies.start("m", curv, state.at[pl.ds(9, 6)])

    copies.wait("c")

    def coarse_plane(field, layer):
        return lambda sl: state[field, layer, sl, :]

    prolong_yz([[coarse_plane(f, l) for l in range(nx)] for f in (0, 15, 1)], rows, coarse)
    copies.wait("f")

    good = fx - 3

    @pl.loop(0, good)
    def _(i):
        mid = lax.shift_right_logical(i, 1) + 1
        side = mid - 1 + 2 * (i & 1)
        parts = [0.75 * coarse[n, mid] + 0.25 * coarse[n, side] for n in range(3)]
        split_flux(lambda n: fluid[n, i], *parts, flux, i)

    copies.start("o", flux, flux_out)

    def pair(layer):
        def one(x):
            return (
                fluid[4, x]
                + fluid[0, x]
                + (fluid[1, x] * fluid[5, x] + fluid[2, x] * fluid[7, x] + fluid[3, x] * fluid[8, x])
                + 3.0 * fluid[6, x]
            )

        return lambda: one(2 * layer) + one(2 * layer + 1)

    restrict_planes([pair(l) for l in range(nx - 1)], rows, sources, 1)
    copies.start("o", sources, source_out)

    @pl.loop(0, 5)
    def _(n):
        for part in range(ny // 8):
            sl = pl.ds(part * 8, 8)

            def emit(i, value):
                hstage[n, i - 3, sl, :] = value

            weno_cells(flux, n, sl, 3, fx - 9, emit)

    copies.start("o", hstage, hydro.at[0, :, pl.ds(3, fx - 9)])
    copies.wait("m")

    @pl.loop(0, nx - 4)
    def _(l):
        bssn_layer(state, sources, stage, l + 2, l + 2, l)

    copies.start("o", stage, rates.at[:, pl.ds(2, nx - 4)])
    copies.wait_all()


def halo_kernel(
    below, above, rates_in, hydro_in, flux_in, source_in,
    lapse, conf, mean, metric, curv, shift, dens, mom, ener, velo, pres,
    rates, hydro,
    state, extra, own, fbelow, fabove, coarse, flux, sources, rows, stage, hstage, sems,
):
    nx, ny, nz = lapse.shape
    fx = dens.shape[1]
    copies = Copies(sems)
    tail = 2 * METRIC + 3 * FLUID
    place = lax.axis_index("blk")
    inside = (
        jnp.where(place > 0, 1.0, 0.0).astype(F32),
        jnp.where(place < lax.axis_size("blk") - 1, 1.0, 0.0).astype(F32),
    )
    for k in range(2):
        copies.start("m", below.at[pl.ds(k * METRIC, METRIC)], state.at[:, k])
        copies.start("m", above.at[pl.ds(k * METRIC, METRIC)], state.at[:, nx + 2 + k])
    for field, count, ref in metric_pieces(lapse, conf, mean, metric, curv, shift):
        if count is None:
            copies.start("m", ref, state.at[field, pl.ds(2, nx)])
        else:
            copies.start("m", ref, state.at[pl.ds(field, count), pl.ds(2, nx)])
    copies.start("m", above.at[pl.ds(tail, 3)], extra)
    for k in range(3):
        copies.start("f", below.at[pl.ds(2 * METRIC + k * FLUID, FLUID)], fbelow.at[pl.ds(0, FLUID), k])
        copies.start("f", above.at[pl.ds(2 * METRIC + k * FLUID, FLUID)], fabove.at[:, k])
    for k in range(2):
        copies.start("f", below.at[pl.ds(tail + 2 * k, 2)], fbelow.at[pl.ds(FLUID, 2), k + 1])
    last = pl.ds(fx - 3, 3)
    copies.start("f", dens.at[0, last], own.at[0])
    copies.start("f", mom.at[0, :, last], own.at[pl.ds(1, 3)])
    copies.start("f", ener.at[0, last], own.at[4])
    copies.start("f", velo.at[0, 0, last], own.at[5])
    copies.start("f", pres.at[0, last], own.at[6])
    copies.start("s", source_in, sources)
    copies.start("x", flux_in.at[:, pl.ds(0, 6)], flux.at[:, pl.ds(3, 6)])
    copies.start("x", flux_in.at[:, pl.ds(fx - 9, 6)], flux.at[:, pl.ds(fx - 6, 6)])

    copies.wait("m")

    def coarse_plane(field, layer):
        if layer == nx + 2:
            return lambda sl: extra[(0, 15, 1).index(field), sl, :]
        return lambda sl: state[field, layer + 2, sl, :]

    layers = (-1, 0, 1, nx - 1, nx, nx + 1, nx + 2)
    prolong_yz([[coarse_plane(f, l) for l in layers] for f in (0, 15, 1)], rows, coarse)
    copies.wait("f")

    for i in (-3, -2, -1) + tuple(range(fx - 3, fx + 3)):
        mid = i // 2 + 1
        side = mid - 1 + 2 * (i % 2)
        mid, side = layers.index(mid), layers.index(side)
        parts = [0.75 * coarse[n, mid] + 0.25 * coarse[n, side] for n in range(3)]
        if i < 0:
            source, at, scale = fbelow, i + 3, inside[0]
        elif i < fx:
            source, at, scale = own, i - fx + 3, None
        else:
            source, at, scale = fabove, i - fx, inside[1]
        split_flux(lambda n, s=source, a=at: s[n, a], *parts, flux, i + 3, scale)

    copies.wait("x")

    @pl.loop(0, 5)
    def _(n):
        for part in range(ny // 8):
            sl = pl.ds(part * 8, 8)

            def emit_low(i, value):
                hstage[n, i - 3, sl, :] = value

            def emit_high(i, value):
                hstage[n, 3 + i - (fx - 3), sl, :] = value

            weno_cells(flux, n, sl, 3, 3, emit_low)
            weno_cells(flux, n, sl, fx - 3, 6, emit_high)

    copies.start("o", hstage.at[:, pl.ds(0, 3)], hydro.at[0, :, pl.ds(0, 3)])
    copies.start("o", hstage.at[:, pl.ds(3, 6)], hydro.at[0, :, pl.ds(fx - 6, 6)])
    copies.wait("s")

    def pair():
        def one(x):
            return (
                fbelow[4, x]
                + fbelow[0, x]
                + (fbelow[1, x] * fbelow[5, x] + fbelow[2, x] * fbelow[7, x] + fbelow[3, x] * fbelow[8, x])
                + 3.0 * fbelow[6, x]
            )

        return one(1) + one(2)

    restrict_planes([pair], rows, sources, 0)

    @pl.loop(0, 4)
    def _(k):
        l = jnp.where(k < 2, k, k + nx - 4)
        bssn_layer(state, sources, stage, l + 2, l, k)

    copies.start("o", stage.at[:, pl.ds(0, 2)], rates.at[:, pl.ds(0, 2)])
    copies.start("o", stage.at[:, pl.ds(2, 2)], rates.at[:, pl.ds(nx - 2, 2)])
    copies.wait_all()


def on_device(*fields):
    lapse, dens = fields[0], fields[6]
    nx, ny, nz = lapse.shape
    fx = dens.shape[1]
    layer = (ny, nz)

    def shape(*leading):
        return jax.ShapeDtypeStruct(leading + layer, F32)

    def vmem(*leading):
        return pltpu.VMEM(leading + layer, F32)

    tail = 2 * METRIC + 3 * FLUID
    up, down = pl.pallas_call(
        pack_kernel,
        out_shape=(shape(tail + 4), shape(tail + 3)),
        in_specs=[ANY] * 11,
        out_specs=[VMEM] * 2,
        scratch_shapes=[pltpu.SemaphoreType.DMA((64,))],
        compiler_params=pltpu.CompilerParams(vmem_limit_bytes=GRANT),
        name="pack",
    )(*fields)
    count = lax.axis_size(RING)
    pairs = [(i, (i + 1) % count) for i in range(count)]
    below = lax.ppermute(up, RING, pairs)
    above = lax.ppermute(down, RING, [(j, i) for i, j in pairs])

    def row_scratch(planes):
        return pltpu.VMEM((nz // LANES, planes * ny, LANES), F32)

    partial = pl.pallas_call(
        local_kernel,
        out_shape=(shape(15, nx), shape(1, 5, fx), shape(10, fx - 3), shape(nx)),
        in_specs=[ANY] * 11,
        out_specs=[ANY] * 4,
        scratch_shapes=[
            vmem(METRIC, nx),
            vmem(9, fx),
            vmem(3, nx),
            vmem(10, fx - 3),
            vmem(nx),
            row_scratch(3 * nx),
            vmem(15, nx - 4),
            vmem(5, fx - 9),
            pltpu.SemaphoreType.DMA((32,)),
        ],
        cost_estimate=pl.CostEstimate(flops=400_000_000, transcendentals=0, bytes_accessed=12_000_000),
        compiler_params=pltpu.CompilerParams(vmem_limit_bytes=GRANT),
        name="local",
    )(*fields)
    return pl.pallas_call(
        halo_kernel,
        out_shape=(shape(15, nx), shape(1, 5, fx)),
        in_specs=[VMEM] * 2 + [ANY] * 15,
        out_specs=[ANY] * 2,
        input_output_aliases={2: 0, 3: 1},
        scratch_shapes=[
            vmem(METRIC, nx + 4),
            vmem(3),
            vmem(FLUID, 3),
            vmem(9, 3),
            vmem(FLUID, 3),
            vmem(3, 7),
            vmem(10, fx + 6),
            vmem(nx),
            row_scratch(21),
            vmem(15, 4),
            vmem(5, 9),
            pltpu.SemaphoreType.DMA((64,)),
        ],
        cost_estimate=pl.CostEstimate(flops=400_000_000, transcendentals=0, bytes_accessed=12_000_000),
        compiler_params=pltpu.CompilerParams(vmem_limit_bytes=GRANT),
        name="halo",
    )(below, above, *partial, *fields)


def solution(mesh):
    in_specs = (
        P(RING, None, None),
        P(RING, None, None),
        P(RING, None, None),
        P(None, RING, None, None),
        P(None, RING, None, None),
        P(None, RING, None, None),
        P("star", "blk", None, None),
        P("star", None, "blk", None, None),
        P("star", "blk", None, None),
        P("star", None, "blk", None, None),
        P("star", "blk", None, None),
    )
    out_specs = (P(None, RING, None, None), P("star", None, "blk", None, None))
    return jax.shard_map(
        on_device, mesh=mesh, in_specs=in_specs, out_specs=out_specs, check_vma=False
    )
```

```python
import functools
import math

import jax
import jax.numpy as jnp
from jax import lax
from jax.experimental import pallas as pl
from jax.experimental.pallas import tpu as pltpu
from jax.sharding import PartitionSpec as P

pair_index = ((0, 1, 2), (1, 3, 4), (2, 4, 5))
sym_pairs = ((0, 0), (0, 1), (0, 2), (1, 1), (1, 2), (2, 2))
weno_eps = 1e-06
RING = ("star", "blk")
LANES = 128
METRIC = 18
EARLY = 5
LATE = 13
FLUID = 7
HBM = pl.BlockSpec(memory_space=pltpu.HBM)
GRANT = 24 * 1024 * 1024
VMEM = pl.BlockSpec(memory_space=pltpu.VMEM)
F32 = jnp.float32


class Copies:
    def __init__(self, sems):
        self.sems = sems
        self.count = 0
        self.groups = {}

    def start(self, group, src, dst):
        copy = pltpu.make_async_copy(src, dst, self.sems.at[self.count])
        copy.start()
        self.count += 1
        self.groups.setdefault(group, []).append(copy)

    def wait(self, group):
        for copy in self.groups.pop(group):
            copy.wait()

    def wait_all(self):
        for group in list(self.groups):
            self.wait(group)


def pack_kernel(lapse, conf, shift, dens, mom, ener, velo, pres, up, down, sems):
    nx = lapse.shape[0]
    fx = dens.shape[1]
    copies = Copies(sems)
    for buf, first, fluid_first in ((up, nx - 2, fx - 3), (down, 0, 0)):
        for k in range(2):
            at = k * EARLY
            copies.start(0, lapse.at[first + k], buf.at[at])
            copies.start(0, conf.at[first + k], buf.at[at + 1])
            copies.start(0, shift.at[:, first + k], buf.at[pl.ds(at + 2, 3)])
        for k in range(3):
            at = 2 * EARLY + k * FLUID
            row = fluid_first + k
            copies.start(0, dens.at[0, row], buf.at[at])
            copies.start(0, mom.at[0, :, row], buf.at[pl.ds(at + 1, 3)])
            copies.start(0, ener.at[0, row], buf.at[at + 4])
            copies.start(0, velo.at[0, 0, row], buf.at[at + 5])
            copies.start(0, pres.at[0, row], buf.at[at + 6])
    tail = 2 * EARLY + 3 * FLUID
    copies.start(0, lapse.at[2], down.at[tail])
    copies.start(0, shift.at[0, 2], down.at[tail + 1])
    copies.start(0, conf.at[2], down.at[tail + 2])
    copies.wait_all()


def bssn_layer(state, sources, out, at, src_at, out_at):
    ny, nz = state.shape[-2:]

    def value(field, off=0):
        return state[field, at + off]

    def rolled(v, axis):
        n = (ny, nz)[axis]
        return tuple(pltpu.roll(v, s % n, axis) for s in (2, 1, -1, -2))

    def first(taps):
        m2, m1, p1, p2 = taps
        return (m2 - p2) + 8.0 * (p1 - m1)

    def second(taps, mid):
        m2, m1, p1, p2 = taps
        return 16.0 * (m1 + p1) - (m2 + p2) - 30.0 * mid

    def xtaps(field):
        return tuple(value(field, o) for o in (-2, -1, 1, 2))

    twelfth = 1.0 / 12.0
    third = 1.0 / 3.0
    lapse = value(0)
    conf = value(1)
    mean = value(2)
    shift12 = [value(15 + n) * twelfth for n in range(3)]

    def gradient(field):
        v = value(field)
        return first(xtaps(field)), first(rolled(v, 0)), first(rolled(v, 1))

    def along_shift(field):
        gx, gy, gz = gradient(field)
        return shift12[0] * gx + shift12[1] * gy + shift12[2] * gz

    dshift = [[None] * 3 for _ in range(3)]
    for n in range(3):
        for k, g in enumerate(gradient(15 + n)):
            dshift[k][n] = g * twelfth
    div_shift = dshift[0][0] + dshift[1][1] + dshift[2][2]
    div23 = (2.0 / 3.0) * div_shift

    taps_x = xtaps(0)
    taps_y = rolled(lapse, 0)
    taps_z = rolled(lapse, 1)
    lx, ly, lz = first(taps_x), first(taps_y), first(taps_z)
    out[0, out_at] = (shift12[0] * lx + shift12[1] * ly + shift12[2] * lz) - 2.0 * lapse * mean
    sq = twelfth * twelfth
    hess = (
        second(taps_x, lapse) * twelfth,
        first(rolled(lx, 0)) * sq,
        first(rolled(lx, 1)) * sq,
        second(taps_y, lapse) * twelfth,
        first(rolled(lz, 0)) * sq,
        second(taps_z, lapse) * twelfth,
    )
    out[1, out_at] = along_shift(1) + conf * ((2.0 / 3.0) * (lapse * mean) - div23)

    a, b, c, d, e, f = g = [value(3 + n) for n in range(6)]
    cof = (d * f - e * e, c * e - b * f, b * e - c * d, a * f - c * c, b * c - a * e, a * d - b * b)
    scale = 1.0 / (a * cof[0] + b * cof[1] + c * cof[2])
    inv = [entry * scale for entry in cof]
    trace = (inv[0] * hess[0] + inv[3] * hess[3] + inv[5] * hess[5]) + 2.0 * (
        inv[1] * hess[1] + inv[2] * hess[2] + inv[4] * hess[4]
    )
    trace3 = trace * third
    curv = [value(9 + n) for n in range(6)]

    def pick(six, i, j):
        return six[pair_index[i][j]]

    def total(terms):
        return functools.reduce(lambda x, y: x + y, terms)

    mixed = [
        [total([pick(curv, i, l) * pick(inv, l, j) for l in range(3)]) for j in range(3)]
        for i in range(3)
    ]
    square = (mixed[0][0] * mixed[0][0] + mixed[1][1] * mixed[1][1] + mixed[2][2] * mixed[2][2]) + 2.0 * (
        mixed[0][1] * mixed[1][0] + mixed[0][2] * mixed[2][0] + mixed[1][2] * mixed[2][1]
    )
    out[2, out_at] = (
        along_shift(2)
        - conf * trace
        + lapse * (square + mean * mean * third + (4.0 * math.pi) * sources[src_at])
    )
    lapse2 = 2.0 * lapse
    mean_lapse = lapse * mean

    def stretched(six, i, j):
        if i == j:
            return 2.0 * total([pick(six, i, k) * dshift[i][k] for k in range(3)])
        return total([pick(six, i, k) * dshift[j][k] + pick(six, j, k) * dshift[i][k] for k in range(3)])

    for p, (i, j) in enumerate(sym_pairs):
        product = total([mixed[i][k] * pick(curv, k, j) for k in range(3)])
        out[9 + p, out_at] = (
            along_shift(9 + p)
            + (mean_lapse - div23) * curv[p]
            - lapse2 * product
            + stretched(curv, i, j)
            - conf * (hess[p] - trace3 * g[p])
        )
    for p, (i, j) in enumerate(sym_pairs):
        out[3 + p, out_at] = along_shift(3 + p) - lapse2 * curv[p] + stretched(g, i, j) - div23 * g[p]


def lane_matrix(nz, weights):
    row = lax.broadcasted_iota(jnp.int32, (nz, nz), 0)
    col = lax.broadcasted_iota(jnp.int32, (nz, nz), 1)
    return weights(row, col)


def dot(x, y):
    return jnp.dot(x, y, precision=lax.Precision.HIGHEST, preferred_element_type=F32)


def restrict_planes(pairs, rows, outs):
    ny, nz = outs[0][0].shape[-2:]
    half = ny // 2
    quarter_y, quarter_z = ny // 4, nz // 4
    count = len(pairs)
    for n, plane in enumerate(pairs):
        for h in range(nz // LANES):
            rows[h, pl.ds(n * ny, ny), :] = plane()[:, h * LANES : (h + 1) * LANES]
    halves = [
        rows[h, pl.ds(0, count * half, stride=2), :] + rows[h, pl.ds(1, count * half, stride=2), :]
        for h in range(nz // LANES)
    ]
    matrix = lane_matrix(
        nz, lambda r, c: jnp.where(c == quarter_z + lax.shift_right_logical(r, 1), 0.125, 0.0).astype(F32)
    )
    level = dot(jnp.concatenate(halves, axis=1), matrix)
    for n, (out, at) in enumerate(outs):
        out[at] = jnp.zeros((ny, nz), F32)
        out[at, pl.ds(quarter_y, half), :] = level[n * half : (n + 1) * half]


def prolong_yz(planes, rows, out):
    ny, nz = out.shape[-2:]
    half = ny // 2
    start_y, start_z = ny // 4, nz // 4
    flat = [plane for field in planes for plane in field]
    for n, plane in enumerate(flat):
        mid = 0.75 * plane(pl.ds(start_y, half))
        even = mid + 0.25 * plane(pl.ds(start_y - 1, half))
        odd = mid + 0.25 * plane(pl.ds(start_y + 1, half))
        for h in range(nz // LANES):
            lanes = slice(h * LANES, (h + 1) * LANES)
            rows[h, pl.ds(n * ny, half, stride=2), :] = even[:, lanes]
            rows[h, pl.ds(n * ny + 1, half, stride=2), :] = odd[:, lanes]

    def weights(r, c):
        mid = start_z + lax.shift_right_logical(c, 1)
        side = mid - 1 + 2 * (c & 1)
        return jnp.where(r == mid, 0.75, jnp.where(r == side, 0.25, 0.0)).astype(F32)

    matrix = lane_matrix(nz, weights)
    wide = jnp.concatenate([rows[h, pl.ds(0, len(flat) * ny), :] for h in range(nz // LANES)], axis=1)
    fine = dot(wide, matrix)
    at = 0
    for field, layers in enumerate(planes):
        for n in range(len(layers)):
            out[field, n] = fine[at * ny : (at + 1) * ny]
            at += 1


def split_flux(fluid, lapse, shift, conf, out, out_at, scale=None):
    root = lax.rsqrt(conf)
    transport = lapse * fluid(5) - shift
    weight = lapse * (root * root * root) * fluid(6)
    speed = lapse + jnp.abs(shift)
    for n in range(5):
        u = fluid(n)
        flux = u * transport
        if n == 1:
            flux = flux + weight
        if n == 4:
            flux = flux + weight * fluid(5)
        moved = speed * u
        plus, minus = flux + moved, flux - moved
        if scale is not None:
            plus, minus = plus * scale, minus * scale
        out[n, out_at] = plus
        out[5 + n, out_at] = minus


def weno_cells(flux, field, rows, first, count, emit):
    def differences(which, low, high):
        v = {j: flux[which, j, rows, :] for j in range(low, high + 1)}
        e = {j: v[j + 1] - v[j] for j in range(low, high)}
        d = {j: e[j] - e[j - 1] for j in range(low + 1, high)}
        t = {j: d[j + 1] - d[j] for j in range(low + 1, high - 1)}
        h = {j: 0.5 * d[j] for j in d}
        s = {j: (13.0 / 12.0) * (d[j] * d[j]) + 4.0 * weno_eps for j in d}
        return v, e, d, t, h, s

    faces = range(first - 1, first + count)
    v, e, d, t, h, s = differences(field, first - 3, first + count + 1)
    u, eu, du, tu, hu, su = differences(5 + field, first - 2, first + count + 2)

    def quotient(b0, b1, b2, t0, t2):
        w0, w1, w2 = b1 * b2, b0 * b2, b0 * b1
        w0, w1, w2 = w0 * w0, 6.0 * (w1 * w1), w2 * w2
        return (w0 * t0 + 1.5 * (w2 * t2)) / (w0 + w1 + 3.0 * w2)

    def square(x):
        return x * x

    previous = None
    for i in faces:
        left = quotient(
            s[i - 1] + square(h[i - 1] + e[i - 1]),
            s[i] + square(h[i] + e[i - 1]),
            s[i + 1] + square(h[i + 1] - e[i]),
            t[i - 1],
            t[i],
        )
        right = quotient(
            su[i + 2] + square(hu[i + 2] - eu[i + 1]),
            su[i + 1] + square(hu[i + 1] - eu[i + 1]),
            su[i] + square(hu[i] + eu[i]),
            tu[i + 1],
            tu[i],
        )
        face = (
            3.0 * (v[i] + u[i + 1])
            + 0.5 * (e[i - 1] - eu[i + 1])
            + (e[i] - eu[i])
            + (right - left)
        )
        if previous is not None:
            emit(i, (previous - face) * (1.0 / 3.0))
        previous = face


def local_kernel(
    lapse, conf, mean, metric, curv, shift, dens, mom, ener, velo, pres,
    rates, hydro, state, flux, sources, up, down,
    fluid, coarse, rows, stage, hstage, sems,
):
    nx, ny, nz = lapse.shape
    fx = dens.shape[1]
    copies = Copies(sems)
    inner = pl.ds(2, nx)
    copies.start("c", lapse, state.at[0, inner])
    copies.start("c", conf, state.at[1, inner])
    copies.start("c", shift, state.at[pl.ds(15, 3), inner])
    copies.start("f", dens.at[0], fluid.at[0])
    copies.start("f", mom.at[0], fluid.at[pl.ds(1, 3)])
    copies.start("f", ener.at[0], fluid.at[4])
    copies.start("f", velo.at[0, 0], fluid.at[5])
    copies.start("f", pres.at[0], fluid.at[6])
    copies.start("f", velo.at[0, pl.ds(1, 2)], fluid.at[pl.ds(7, 2)])
    copies.start("m", mean, state.at[2, inner])
    copies.start("m", metric, state.at[pl.ds(3, 6), inner])
    copies.start("m", curv, state.at[pl.ds(9, 6), inner])
    for buf, first in ((up, nx - 2), (down, 0)):
        for k in range(2):
            copies.start("o", mean.at[first + k], buf.at[k * LATE])
            copies.start("o", metric.at[:, first + k], buf.at[pl.ds(k * LATE + 1, 6)])
            copies.start("o", curv.at[:, first + k], buf.at[pl.ds(k * LATE + 7, 6)])

    @pl.loop(2, 15)
    def _(n):
        for k in (0, 1, nx + 2, nx + 3):
            state[n, k] = jnp.zeros((ny, nz), F32)

    copies.wait("c")

    def coarse_plane(field, layer):
        return lambda sl: state[field, layer + 2, sl, :]

    prolong_yz([[coarse_plane(f, l) for l in range(nx)] for f in (0, 15, 1)], rows, coarse)
    copies.wait("f")

    @pl.loop(0, fx - 3)
    def _(i):
        mid = lax.shift_right_logical(i, 1) + 1
        side = mid - 1 + 2 * (i & 1)
        parts = [0.75 * coarse[n, mid] + 0.25 * coarse[n, side] for n in range(3)]
        split_flux(lambda n: fluid[n, i], *parts, flux, i + 3)

    def pair(layer):
        def one(x):
            return (
                fluid[4, x]
                + fluid[0, x]
                + (fluid[1, x] * fluid[5, x] + fluid[2, x] * fluid[7, x] + fluid[3, x] * fluid[8, x])
                + 3.0 * fluid[6, x]
            )

        return lambda: one(2 * layer) + one(2 * layer + 1)

    restrict_planes(
        [pair(l) for l in range(nx)],
        rows,
        [(sources, l + 1) for l in range(nx - 1)] + [(up, 2 * LATE)],
    )
    sources[0] = jnp.zeros((ny, nz), F32)

    @pl.loop(0, 5)
    def _(n):
        for part in range(ny // 8):
            sl = pl.ds(part * 8, 8)

            def emit(i, value):
                hstage[n, i - 6, sl, :] = value

            weno_cells(flux, n, sl, 6, fx - 9, emit)

    copies.start("o", hstage, hydro.at[0, :, pl.ds(3, fx - 9)])
    copies.wait("m")

    @pl.loop(0, nx - 4)
    def _(l):
        bssn_layer(state, sources, stage, l + 4, l + 2, l)

    copies.start("o", stage, rates.at[:, pl.ds(2, nx - 4)])
    copies.wait_all()


def halo_kernel(
    below, above, hydro_in, state_in, flux_in, sources, dens, mom, ener, velo, pres,
    hydro, state, flux, stage,
    own, coarse, rows, hstage, sems,
):
    nx = sources.shape[0]
    ny, nz = sources.shape[-2:]
    fx = dens.shape[1]
    copies = Copies(sems)
    last = pl.ds(fx - 3, 3)
    copies.start("f", dens.at[0, last], own.at[0])
    copies.start("f", mom.at[0, :, last], own.at[pl.ds(1, 3)])
    copies.start("f", ener.at[0, last], own.at[4])
    copies.start("f", velo.at[0, 0, last], own.at[5])
    copies.start("f", pres.at[0, last], own.at[6])
    place = lax.axis_index("blk")
    inside = (
        jnp.where(place > 0, 1.0, 0.0).astype(F32),
        jnp.where(place < lax.axis_size("blk") - 1, 1.0, 0.0).astype(F32),
    )
    for k in range(2):
        for n, field in enumerate((0, 1, 15, 16, 17)):
            state[field, k] = below[k * EARLY + n]
            state[field, nx + 2 + k] = above[k * EARLY + n]

    def coarse_plane(field, layer):
        if layer == nx + 2:
            return lambda sl: above[2 * EARLY + 3 * FLUID + (0, 15, 1).index(field), sl, :]
        return lambda sl: state[field, layer + 2, sl, :]

    layers = (-1, 0, 1, nx - 1, nx, nx + 1, nx + 2)
    prolong_yz([[coarse_plane(f, l) for l in layers] for f in (0, 15, 1)], rows, coarse)
    copies.wait("f")

    for i in (-3, -2, -1) + tuple(range(fx - 3, fx + 3)):
        mid = i // 2 + 1
        side = mid - 1 + 2 * (i % 2)
        mid, side = layers.index(mid), layers.index(side)
        parts = [0.75 * coarse[n, mid] + 0.25 * coarse[n, side] for n in range(3)]
        if i < 0:
            fluid = lambda n, at=2 * EARLY + (i + 3) * FLUID: below[at + n]
            scale = inside[0]
        elif i < fx:
            fluid = lambda n, at=i - fx + 3: own[n, at]
            scale = None
        else:
            fluid = lambda n, at=2 * EARLY + (i - fx) * FLUID: above[at + n]
            scale = inside[1]
        split_flux(fluid, *parts, flux, i + 3, scale)

    @pl.loop(0, 5)
    def _(n):
        for part in range(ny // 8):
            sl = pl.ds(part * 8, 8)

            def emit_low(i, value):
                hstage[n, i - 3, sl, :] = value

            def emit_high(i, value):
                hstage[n, 3 + i - (fx - 3), sl, :] = value

            weno_cells(flux, n, sl, 3, 3, emit_low)
            weno_cells(flux, n, sl, fx - 3, 6, emit_high)

    copies.start("o", hstage.at[:, pl.ds(0, 3)], hydro.at[0, :, pl.ds(0, 3)])
    copies.start("o", hstage.at[:, pl.ds(3, 6)], hydro.at[0, :, pl.ds(fx - 6, 6)])

    @pl.loop(0, 4)
    def _(k):
        l = jnp.where(k < 2, k, k + nx - 4)
        bssn_layer(state, sources, stage, l + 2, l, k)

    copies.wait_all()


def late_kernel(below, above, stage_in, lapse, shift, rates_in, rates, stage, edge, sems):
    nx = lapse.shape[0]
    copies = Copies(sems)
    copies.start("i", shift.at[0, pl.ds(0, 2)], edge.at[pl.ds(0, 2)])
    copies.start("i", shift.at[0, pl.ds(nx - 2, 2)], edge.at[pl.ds(2, 2)])
    copies.start("i", lapse.at[0], edge.at[4])
    copies.wait("i")
    steps = [edge[k] * (1.0 / 12.0) for k in range(4)]
    for field in range(15):
        late = field - 2
        for k in range(4):
            value = stage_in[field, k]
            if late >= 0:
                if k == 0:
                    tap = below[late] - 8.0 * below[LATE + late]
                elif k == 1:
                    tap = below[LATE + late]
                elif k == 2:
                    tap = -above[late]
                else:
                    tap = 8.0 * above[late] - above[LATE + late]
                value = value + steps[k] * tap
            if field == 2 and k == 0:
                value = value + (4.0 * math.pi) * edge[4] * below[2 * LATE]
            stage[field, k] = value
    copies.start("o", stage.at[:, pl.ds(0, 2)], rates.at[:, pl.ds(0, 2)])
    copies.start("o", stage.at[:, pl.ds(2, 2)], rates.at[:, pl.ds(nx - 2, 2)])
    copies.wait_all()


def on_device(*fields):
    fields = [pltpu.with_memory_space_constraint(field, pltpu.HBM) for field in fields]
    lapse, conf, mean, metric, curv, shift, dens, mom, ener, velo, pres = fields
    nx, ny, nz = lapse.shape
    fx = dens.shape[1]
    layer = (ny, nz)

    def shape(*leading):
        return jax.ShapeDtypeStruct(leading + layer, F32)

    def vmem(*leading):
        return pltpu.VMEM(leading + layer, F32)

    def row_scratch(planes):
        return pltpu.VMEM((nz // LANES, planes * ny, LANES), F32)

    def sems(n):
        return pltpu.SemaphoreType.DMA((n,))

    count = lax.axis_size(RING)
    pairs = [(i, (i + 1) % count) for i in range(count)]

    def exchanged(up, down):
        return lax.ppermute(up, RING, pairs), lax.ppermute(down, RING, [(j, i) for i, j in pairs])

    params = pltpu.CompilerParams(vmem_limit_bytes=GRANT)
    early = 2 * EARLY + 3 * FLUID
    early_halo = exchanged(
        *pl.pallas_call(
            pack_kernel,
            out_shape=(shape(early), shape(early + 3)),
            in_specs=[HBM] * 8,
            out_specs=[VMEM] * 2,
            scratch_shapes=[sems(48)],
            compiler_params=params,
            name="pack",
        )(lapse, conf, shift, dens, mom, ener, velo, pres)
    )
    rates, hydro, state, flux, sources, up, down = pl.pallas_call(
        local_kernel,
        out_shape=(
            shape(15, nx),
            shape(1, 5, fx),
            shape(METRIC, nx + 4),
            shape(10, fx + 6),
            shape(nx),
            shape(2 * LATE + 1),
            shape(2 * LATE),
        ),
        in_specs=[HBM] * 11,
        out_specs=[HBM] * 2 + [VMEM] * 5,
        scratch_shapes=[
            vmem(9, fx),
            vmem(3, nx),
            row_scratch(3 * nx),
            vmem(15, nx - 4),
            vmem(5, fx - 9),
            sems(32),
        ],
        cost_estimate=pl.CostEstimate(flops=400_000_000, transcendentals=0, bytes_accessed=12_000_000),
        compiler_params=params,
        name="local",
    )(*fields)
    late_halo = exchanged(up, down)
    hydro, _, _, stage = pl.pallas_call(
        halo_kernel,
        out_shape=(shape(1, 5, fx), shape(METRIC, nx + 4), shape(10, fx + 6), shape(15, 4)),
        in_specs=[VMEM] * 2 + [HBM] + [VMEM] * 3 + [HBM] * 5,
        out_specs=[HBM] + [VMEM] * 3,
        input_output_aliases={2: 0, 3: 1, 4: 2},
        scratch_shapes=[vmem(FLUID, 3), vmem(3, 7), row_scratch(21), vmem(5, 9), sems(16)],
        cost_estimate=pl.CostEstimate(flops=400_000_000, transcendentals=0, bytes_accessed=12_000_000),
        compiler_params=params,
        name="halo",
    )(*early_halo, hydro, state, flux, sources, dens, mom, ener, velo, pres)
    rates = pl.pallas_call(
        late_kernel,
        out_shape=shape(15, nx),
        in_specs=[VMEM] * 3 + [HBM] * 3,
        out_specs=HBM,
        input_output_aliases={5: 0},
        scratch_shapes=[vmem(15, 4), vmem(5), sems(8)],
        compiler_params=params,
        name="late",
    )(*late_halo, stage, lapse, shift, rates)
    return rates, hydro


def solution(mesh):
    in_specs = (
        P(RING, None, None),
        P(RING, None, None),
        P(RING, None, None),
        P(None, RING, None, None),
        P(None, RING, None, None),
        P(None, RING, None, None),
        P("star", "blk", None, None),
        P("star", None, "blk", None, None),
        P("star", "blk", None, None),
        P("star", None, "blk", None, None),
        P("star", "blk", None, None),
    )
    out_specs = (P(None, RING, None, None), P("star", None, "blk", None, None))
    return jax.shard_map(
        on_device, mesh=mesh, in_specs=in_specs, out_specs=out_specs, check_vma=False
    )
```

```python
import functools
import math

import jax
import jax.numpy as jnp
from jax import lax
from jax.experimental import pallas as pl
from jax.experimental.pallas import tpu as pltpu
from jax.sharding import PartitionSpec as P

pair_index = ((0, 1, 2), (1, 3, 4), (2, 4, 5))
sym_pairs = ((0, 0), (0, 1), (0, 2), (1, 1), (1, 2), (2, 2))
weno_eps = 1e-06
RING = ("star", "blk")
LANES = 128
METRIC = 18
EARLY = 5
LATE = 13
FLUID = 7
HBM = pl.BlockSpec(memory_space=pltpu.HBM)
GRANT = 24 * 1024 * 1024
VMEM = pl.BlockSpec(memory_space=pltpu.VMEM)
F32 = jnp.float32


class Copies:
    def __init__(self, sems):
        self.sems = sems
        self.count = 0
        self.groups = {}

    def start(self, group, src, dst):
        copy = pltpu.make_async_copy(src, dst, self.sems.at[self.count])
        copy.start()
        self.count += 1
        self.groups.setdefault(group, []).append(copy)

    def wait(self, group):
        for copy in self.groups.pop(group):
            copy.wait()

    def wait_all(self):
        for group in list(self.groups):
            self.wait(group)


def pack_kernel(lapse, conf, shift, dens, mom, ener, velo, pres, up, down, sems):
    nx = lapse.shape[0]
    fx = dens.shape[1]
    copies = Copies(sems)
    layer = lapse.shape[1:]
    for buf, first, fluid_first in ((up, nx - 2, fx - 3), (down, 0, 0)):
        rows = pl.ds(first, 2)
        copies.start(0, lapse.at[rows], buf.at[pl.ds(0, 2)])
        copies.start(0, conf.at[rows], buf.at[pl.ds(2, 2)])
        copies.start(0, shift.at[:, rows], buf.at[pl.ds(4, 6)].reshape(3, 2, *layer))
        rows = pl.ds(fluid_first, 3)
        at = 2 * EARLY
        copies.start(0, dens.at[0, rows], buf.at[pl.ds(at, 3)])
        copies.start(0, mom.at[0, :, rows], buf.at[pl.ds(at + 3, 9)].reshape(3, 3, *layer))
        copies.start(0, ener.at[0, rows], buf.at[pl.ds(at + 12, 3)])
        copies.start(0, velo.at[0, 0, rows], buf.at[pl.ds(at + 15, 3)])
        copies.start(0, pres.at[0, rows], buf.at[pl.ds(at + 18, 3)])
    tail = 2 * EARLY + 3 * FLUID
    copies.start(0, lapse.at[2], down.at[tail])
    copies.start(0, shift.at[0, 2], down.at[tail + 1])
    copies.start(0, conf.at[2], down.at[tail + 2])
    copies.wait_all()


def bssn_layer(state, sources, out, at, src_at, out_at):
    ny, nz = state.shape[-2:]

    def value(field, off=0):
        return state[field, at + off]

    def rolled(v, axis):
        n = (ny, nz)[axis]
        return tuple(pltpu.roll(v, s % n, axis) for s in (2, 1, -1, -2))

    def first(taps):
        m2, m1, p1, p2 = taps
        return (m2 - p2) + 8.0 * (p1 - m1)

    def second(taps, mid):
        m2, m1, p1, p2 = taps
        return 16.0 * (m1 + p1) - (m2 + p2) - 30.0 * mid

    def xtaps(field):
        return tuple(value(field, o) for o in (-2, -1, 1, 2))

    twelfth = 1.0 / 12.0
    third = 1.0 / 3.0
    lapse = value(0)
    conf = value(1)
    mean = value(2)
    shift12 = [value(15 + n) * twelfth for n in range(3)]

    def gradient(field):
        v = value(field)
        return first(xtaps(field)), first(rolled(v, 0)), first(rolled(v, 1))

    def along_shift(field):
        gx, gy, gz = gradient(field)
        return shift12[0] * gx + shift12[1] * gy + shift12[2] * gz

    dshift = [[None] * 3 for _ in range(3)]
    for n in range(3):
        for k, g in enumerate(gradient(15 + n)):
            dshift[k][n] = g * twelfth
    div_shift = dshift[0][0] + dshift[1][1] + dshift[2][2]
    div23 = (2.0 / 3.0) * div_shift

    taps_x = xtaps(0)
    taps_y = rolled(lapse, 0)
    taps_z = rolled(lapse, 1)
    lx, ly, lz = first(taps_x), first(taps_y), first(taps_z)
    out[0, out_at] = (shift12[0] * lx + shift12[1] * ly + shift12[2] * lz) - 2.0 * lapse * mean
    sq = twelfth * twelfth
    hess = (
        second(taps_x, lapse) * twelfth,
        first(rolled(lx, 0)) * sq,
        first(rolled(lx, 1)) * sq,
        second(taps_y, lapse) * twelfth,
        first(rolled(lz, 0)) * sq,
        second(taps_z, lapse) * twelfth,
    )
    out[1, out_at] = along_shift(1) + conf * ((2.0 / 3.0) * (lapse * mean) - div23)

    a, b, c, d, e, f = g = [value(3 + n) for n in range(6)]
    cof = (d * f - e * e, c * e - b * f, b * e - c * d, a * f - c * c, b * c - a * e, a * d - b * b)
    scale = 1.0 / (a * cof[0] + b * cof[1] + c * cof[2])
    inv = [entry * scale for entry in cof]
    trace = (inv[0] * hess[0] + inv[3] * hess[3] + inv[5] * hess[5]) + 2.0 * (
        inv[1] * hess[1] + inv[2] * hess[2] + inv[4] * hess[4]
    )
    trace3 = trace * third
    curv = [value(9 + n) for n in range(6)]

    def pick(six, i, j):
        return six[pair_index[i][j]]

    def total(terms):
        return functools.reduce(lambda x, y: x + y, terms)

    mixed = [
        [total([pick(curv, i, l) * pick(inv, l, j) for l in range(3)]) for j in range(3)]
        for i in range(3)
    ]
    square = (mixed[0][0] * mixed[0][0] + mixed[1][1] * mixed[1][1] + mixed[2][2] * mixed[2][2]) + 2.0 * (
        mixed[0][1] * mixed[1][0] + mixed[0][2] * mixed[2][0] + mixed[1][2] * mixed[2][1]
    )
    out[2, out_at] = (
        along_shift(2)
        - conf * trace
        + lapse * (square + mean * mean * third + (4.0 * math.pi) * sources[src_at])
    )
    lapse2 = 2.0 * lapse
    mean_lapse = lapse * mean

    def stretched(six, i, j):
        if i == j:
            return 2.0 * total([pick(six, i, k) * dshift[i][k] for k in range(3)])
        return total([pick(six, i, k) * dshift[j][k] + pick(six, j, k) * dshift[i][k] for k in range(3)])

    for p, (i, j) in enumerate(sym_pairs):
        product = total([mixed[i][k] * pick(curv, k, j) for k in range(3)])
        out[9 + p, out_at] = (
            along_shift(9 + p)
            + (mean_lapse - div23) * curv[p]
            - lapse2 * product
            + stretched(curv, i, j)
            - conf * (hess[p] - trace3 * g[p])
        )
    for p, (i, j) in enumerate(sym_pairs):
        out[3 + p, out_at] = along_shift(3 + p) - lapse2 * curv[p] + stretched(g, i, j) - div23 * g[p]


def lane_matrix(nz, weights):
    row = lax.broadcasted_iota(jnp.int32, (nz, nz), 0)
    col = lax.broadcasted_iota(jnp.int32, (nz, nz), 1)
    return weights(row, col)


def dot(x, y):
    return jnp.dot(x, y, precision=lax.Precision.HIGHEST, preferred_element_type=F32)


def restrict_planes(pairs, rows, outs):
    ny, nz = outs[0][0].shape[-2:]
    half = ny // 2
    quarter_y, quarter_z = ny // 4, nz // 4
    count = len(pairs)
    for n, plane in enumerate(pairs):
        for h in range(nz // LANES):
            rows[h, pl.ds(n * ny, ny), :] = plane()[:, h * LANES : (h + 1) * LANES]
    halves = [
        rows[h, pl.ds(0, count * half, stride=2), :] + rows[h, pl.ds(1, count * half, stride=2), :]
        for h in range(nz // LANES)
    ]
    matrix = lane_matrix(
        nz, lambda r, c: jnp.where(c == quarter_z + lax.shift_right_logical(r, 1), 0.125, 0.0).astype(F32)
    )
    level = dot(jnp.concatenate(halves, axis=1), matrix)
    for n, (out, at) in enumerate(outs):
        out[at] = jnp.zeros((ny, nz), F32)
        out[at, pl.ds(quarter_y, half), :] = level[n * half : (n + 1) * half]


def prolong_yz(planes, rows, out):
    ny, nz = out.shape[-2:]
    half = ny // 2
    start_y, start_z = ny // 4, nz // 4
    flat = [plane for field in planes for plane in field]
    for n, plane in enumerate(flat):
        mid = 0.75 * plane(pl.ds(start_y, half))
        even = mid + 0.25 * plane(pl.ds(start_y - 1, half))
        odd = mid + 0.25 * plane(pl.ds(start_y + 1, half))
        for h in range(nz // LANES):
            lanes = slice(h * LANES, (h + 1) * LANES)
            rows[h, pl.ds(n * ny, half, stride=2), :] = even[:, lanes]
            rows[h, pl.ds(n * ny + 1, half, stride=2), :] = odd[:, lanes]

    def weights(r, c):
        mid = start_z + lax.shift_right_logical(c, 1)
        side = mid - 1 + 2 * (c & 1)
        return jnp.where(r == mid, 0.75, jnp.where(r == side, 0.25, 0.0)).astype(F32)

    matrix = lane_matrix(nz, weights)
    wide = jnp.concatenate([rows[h, pl.ds(0, len(flat) * ny), :] for h in range(nz // LANES)], axis=1)
    fine = dot(wide, matrix)
    at = 0
    for field, layers in enumerate(planes):
        for n in range(len(layers)):
            out[field, n] = fine[at * ny : (at + 1) * ny]
            at += 1


def split_flux(fluid, lapse, shift, conf, out, out_at, scale=None):
    root = lax.rsqrt(conf)
    transport = lapse * fluid(5) - shift
    weight = lapse * (root * root * root) * fluid(6)
    speed = lapse + jnp.abs(shift)
    for n in range(5):
        u = fluid(n)
        flux = u * transport
        if n == 1:
            flux = flux + weight
        if n == 4:
            flux = flux + weight * fluid(5)
        moved = speed * u
        plus, minus = flux + moved, flux - moved
        if scale is not None:
            plus, minus = plus * scale, minus * scale
        out[n, out_at] = plus
        out[5 + n, out_at] = minus


def weno_cells(flux, field, rows, first, count, emit):
    def differences(which, low, high):
        v = {j: flux[which, j, rows, :] for j in range(low, high + 1)}
        e = {j: v[j + 1] - v[j] for j in range(low, high)}
        d = {j: e[j] - e[j - 1] for j in range(low + 1, high)}
        t = {j: d[j + 1] - d[j] for j in range(low + 1, high - 1)}
        h = {j: 0.5 * d[j] for j in d}
        s = {j: (13.0 / 12.0) * (d[j] * d[j]) + 4.0 * weno_eps for j in d}
        return v, e, d, t, h, s

    faces = range(first - 1, first + count)
    v, e, d, t, h, s = differences(field, first - 3, first + count + 1)
    u, eu, du, tu, hu, su = differences(5 + field, first - 2, first + count + 2)

    def quotient(b0, b1, b2, t0, t2):
        w0, w1, w2 = b1 * b2, b0 * b2, b0 * b1
        w0, w1, w2 = w0 * w0, 6.0 * (w1 * w1), w2 * w2
        return (w0 * t0 + 1.5 * (w2 * t2)) / (w0 + w1 + 3.0 * w2)

    def square(x):
        return x * x

    previous = None
    for i in faces:
        left = quotient(
            s[i - 1] + square(h[i - 1] + e[i - 1]),
            s[i] + square(h[i] + e[i - 1]),
            s[i + 1] + square(h[i + 1] - e[i]),
            t[i - 1],
            t[i],
        )
        right = quotient(
            su[i + 2] + square(hu[i + 2] - eu[i + 1]),
            su[i + 1] + square(hu[i + 1] - eu[i + 1]),
            su[i] + square(hu[i] + eu[i]),
            tu[i + 1],
            tu[i],
        )
        face = (
            3.0 * (v[i] + u[i + 1])
            + 0.5 * (e[i - 1] - eu[i + 1])
            + (e[i] - eu[i])
            + (right - left)
        )
        if previous is not None:
            emit(i, (previous - face) * (1.0 / 3.0))
        previous = face


def local_kernel(
    lapse, conf, mean, metric, curv, shift, dens, mom, ener, velo, pres,
    state, flux, sources, up, down,
    fluid, coarse, rows, sems,
):
    nx, ny, nz = lapse.shape
    fx = dens.shape[1]
    copies = Copies(sems)
    inner = pl.ds(2, nx)
    copies.start("c", lapse, state.at[0, inner])
    copies.start("c", conf, state.at[1, inner])
    copies.start("c", shift, state.at[pl.ds(15, 3), inner])
    copies.start("f", dens.at[0], fluid.at[0])
    copies.start("f", mom.at[0], fluid.at[pl.ds(1, 3)])
    copies.start("f", ener.at[0], fluid.at[4])
    copies.start("f", velo.at[0, 0], fluid.at[5])
    copies.start("f", pres.at[0], fluid.at[6])
    copies.start("f", velo.at[0, pl.ds(1, 2)], fluid.at[pl.ds(7, 2)])
    copies.start("m", mean, state.at[2, inner])
    copies.start("m", metric, state.at[pl.ds(3, 6), inner])
    copies.start("m", curv, state.at[pl.ds(9, 6), inner])
    for buf, first in ((up, nx - 2), (down, 0)):
        for k in range(2):
            copies.start("o", mean.at[first + k], buf.at[k * LATE])
            copies.start("o", metric.at[:, first + k], buf.at[pl.ds(k * LATE + 1, 6)])
            copies.start("o", curv.at[:, first + k], buf.at[pl.ds(k * LATE + 7, 6)])

    @pl.loop(2, 15)
    def _(n):
        for k in (0, 1, nx + 2, nx + 3):
            state[n, k] = jnp.zeros((ny, nz), F32)

    copies.wait("c")

    def coarse_plane(field, layer):
        return lambda sl: state[field, layer + 2, sl, :]

    prolong_yz([[coarse_plane(f, l) for l in range(nx)] for f in (0, 15, 1)], rows, coarse)
    copies.wait("f")

    @pl.loop(0, fx - 3)
    def _(i):
        mid = lax.shift_right_logical(i, 1) + 1
        side = mid - 1 + 2 * (i & 1)
        parts = [0.75 * coarse[n, mid] + 0.25 * coarse[n, side] for n in range(3)]
        split_flux(lambda n: fluid[n, i], *parts, flux, i + 3)

    def pair(layer):
        def one(x):
            return (
                fluid[4, x]
                + fluid[0, x]
                + (fluid[1, x] * fluid[5, x] + fluid[2, x] * fluid[7, x] + fluid[3, x] * fluid[8, x])
                + 3.0 * fluid[6, x]
            )

        return lambda: one(2 * layer) + one(2 * layer + 1)

    restrict_planes(
        [pair(l) for l in range(nx)],
        rows,
        [(sources, l + 1) for l in range(nx - 1)] + [(up, 2 * LATE)],
    )
    sources[0] = jnp.zeros((ny, nz), F32)

    copies.wait_all()


def inner_kernel(state, flux, sources, rates, hydro, stage, hstage, sems):
    nx, ny, nz = sources.shape
    fx = hydro.shape[2]
    copies = Copies(sems)

    @pl.loop(0, 5)
    def _(n):
        for part in range(ny // 8):
            sl = pl.ds(part * 8, 8)

            def emit(i, value):
                hstage[n, i - 6, sl, :] = value

            weno_cells(flux, n, sl, 6, fx - 9, emit)

    copies.start("o", hstage, hydro.at[0, :, pl.ds(3, fx - 9)])
    @pl.loop(0, nx - 4)
    def _(l):
        bssn_layer(state, sources, stage, l + 4, l + 2, l)

    copies.start("o", stage, rates.at[:, pl.ds(2, nx - 4)])
    copies.wait_all()


def halo_kernel(
    below, above, hydro_in, state_in, flux_in, sources, dens, mom, ener, velo, pres,
    hydro, state, flux, stage,
    own, coarse, rows, hstage, sems,
):
    nx = sources.shape[0]
    ny, nz = sources.shape[-2:]
    fx = dens.shape[1]
    copies = Copies(sems)
    last = pl.ds(fx - 3, 3)
    copies.start("f", dens.at[0, last], own.at[0])
    copies.start("f", mom.at[0, :, last], own.at[pl.ds(1, 3)])
    copies.start("f", ener.at[0, last], own.at[4])
    copies.start("f", velo.at[0, 0, last], own.at[5])
    copies.start("f", pres.at[0, last], own.at[6])
    place = lax.axis_index("blk")
    inside = (
        jnp.where(place > 0, 1.0, 0.0).astype(F32),
        jnp.where(place < lax.axis_size("blk") - 1, 1.0, 0.0).astype(F32),
    )
    for k in range(2):
        for n, field in enumerate((0, 1, 15, 16, 17)):
            state[field, k] = below[2 * n + k]
            state[field, nx + 2 + k] = above[2 * n + k]

    def coarse_plane(field, layer):
        if layer == nx + 2:
            return lambda sl: above[2 * EARLY + 3 * FLUID + (0, 15, 1).index(field), sl, :]
        return lambda sl: state[field, layer + 2, sl, :]

    layers = (-1, 0, 1, nx - 1, nx, nx + 1, nx + 2)
    prolong_yz([[coarse_plane(f, l) for l in layers] for f in (0, 15, 1)], rows, coarse)
    copies.wait("f")

    for i in (-3, -2, -1) + tuple(range(fx - 3, fx + 3)):
        mid = i // 2 + 1
        side = mid - 1 + 2 * (i % 2)
        mid, side = layers.index(mid), layers.index(side)
        parts = [0.75 * coarse[n, mid] + 0.25 * coarse[n, side] for n in range(3)]
        if i < 0:
            fluid = lambda n, at=2 * EARLY + i + 3: below[at + 3 * n]
            scale = inside[0]
        elif i < fx:
            fluid = lambda n, at=i - fx + 3: own[n, at]
            scale = None
        else:
            fluid = lambda n, at=2 * EARLY + i - fx: above[at + 3 * n]
            scale = inside[1]
        split_flux(fluid, *parts, flux, i + 3, scale)

    @pl.loop(0, 5)
    def _(n):
        for part in range(ny // 8):
            sl = pl.ds(part * 8, 8)

            def emit_low(i, value):
                hstage[n, i - 3, sl, :] = value

            def emit_high(i, value):
                hstage[n, 3 + i - (fx - 3), sl, :] = value

            weno_cells(flux, n, sl, 3, 3, emit_low)
            weno_cells(flux, n, sl, fx - 3, 6, emit_high)

    copies.start("o", hstage.at[:, pl.ds(0, 3)], hydro.at[0, :, pl.ds(0, 3)])
    copies.start("o", hstage.at[:, pl.ds(3, 6)], hydro.at[0, :, pl.ds(fx - 6, 6)])

    @pl.loop(0, 4)
    def _(k):
        l = jnp.where(k < 2, k, k + nx - 4)
        bssn_layer(state, sources, stage, l + 2, l, k)

    copies.wait_all()


def late_kernel(below, above, stage_in, state, rates_in, rates, stage, sems):
    nx = rates.shape[1]
    copies = Copies(sems)
    steps = [state[15, at] * (1.0 / 12.0) for at in (2, 3, nx, nx + 1)]
    for field in range(15):
        late = field - 2
        for k in range(4):
            value = stage_in[field, k]
            if late >= 0:
                if k == 0:
                    tap = below[late] - 8.0 * below[LATE + late]
                elif k == 1:
                    tap = below[LATE + late]
                elif k == 2:
                    tap = -above[late]
                else:
                    tap = 8.0 * above[late] - above[LATE + late]
                value = value + steps[k] * tap
            if field == 2 and k == 0:
                value = value + (4.0 * math.pi) * state[0, 2] * below[2 * LATE]
            stage[field, k] = value
    copies.start("o", stage.at[:, pl.ds(0, 2)], rates.at[:, pl.ds(0, 2)])
    copies.start("o", stage.at[:, pl.ds(2, 2)], rates.at[:, pl.ds(nx - 2, 2)])
    copies.wait_all()


def on_device(*fields):
    fields = [pltpu.with_memory_space_constraint(field, pltpu.HBM) for field in fields]
    lapse, conf, mean, metric, curv, shift, dens, mom, ener, velo, pres = fields
    nx, ny, nz = lapse.shape
    fx = dens.shape[1]
    layer = (ny, nz)

    def shape(*leading):
        return jax.ShapeDtypeStruct(leading + layer, F32)

    def vmem(*leading):
        return pltpu.VMEM(leading + layer, F32)

    def row_scratch(planes):
        return pltpu.VMEM((nz // LANES, planes * ny, LANES), F32)

    def sems(n):
        return pltpu.SemaphoreType.DMA((n,))

    count = lax.axis_size(RING)
    pairs = [(i, (i + 1) % count) for i in range(count)]

    def exchanged(up, down):
        return lax.ppermute(up, RING, pairs), lax.ppermute(down, RING, [(j, i) for i, j in pairs])

    params = pltpu.CompilerParams(vmem_limit_bytes=GRANT)
    early = 2 * EARLY + 3 * FLUID
    early_halo = exchanged(
        *pl.pallas_call(
            pack_kernel,
            out_shape=(shape(early), shape(early + 3)),
            in_specs=[HBM] * 8,
            out_specs=[VMEM] * 2,
            scratch_shapes=[sems(48)],
            compiler_params=params,
            name="pack",
        )(lapse, conf, shift, dens, mom, ener, velo, pres)
    )
    state, flux, sources, up, down = pl.pallas_call(
        local_kernel,
        out_shape=(
            shape(METRIC, nx + 4),
            shape(10, fx + 6),
            shape(nx),
            shape(2 * LATE + 1),
            shape(2 * LATE),
        ),
        in_specs=[HBM] * 11,
        out_specs=[VMEM] * 5,
        scratch_shapes=[vmem(9, fx), vmem(3, nx), row_scratch(3 * nx), sems(32)],
        cost_estimate=pl.CostEstimate(flops=200_000_000, transcendentals=0, bytes_accessed=6_000_000),
        compiler_params=params,
        name="local",
    )(*fields)
    late_halo = exchanged(up, down)
    rates, hydro = pl.pallas_call(
        inner_kernel,
        out_shape=(shape(15, nx), shape(1, 5, fx)),
        in_specs=[VMEM] * 3,
        out_specs=[HBM] * 2,
        scratch_shapes=[vmem(15, nx - 4), vmem(5, fx - 9), sems(4)],
        cost_estimate=pl.CostEstimate(flops=400_000_000, transcendentals=0, bytes_accessed=6_000_000),
        compiler_params=params,
        name="inner",
    )(state, flux, sources)
    hydro, state, _, stage = pl.pallas_call(
        halo_kernel,
        out_shape=(shape(1, 5, fx), shape(METRIC, nx + 4), shape(10, fx + 6), shape(15, 4)),
        in_specs=[VMEM] * 2 + [HBM] + [VMEM] * 3 + [HBM] * 5,
        out_specs=[HBM] + [VMEM] * 3,
        input_output_aliases={2: 0, 3: 1, 4: 2},
        scratch_shapes=[vmem(FLUID, 3), vmem(3, 7), row_scratch(21), vmem(5, 9), sems(16)],
        cost_estimate=pl.CostEstimate(flops=400_000_000, transcendentals=0, bytes_accessed=12_000_000),
        compiler_params=params,
        name="halo",
    )(*early_halo, hydro, state, flux, sources, dens, mom, ener, velo, pres)
    rates = pl.pallas_call(
        late_kernel,
        out_shape=shape(15, nx),
        in_specs=[VMEM] * 4 + [HBM],
        out_specs=HBM,
        input_output_aliases={4: 0},
        scratch_shapes=[vmem(15, 4), sems(8)],
        compiler_params=params,
        name="late",
    )(*late_halo, stage, state, rates)
    return rates, hydro


def solution(mesh):
    in_specs = (
        P(RING, None, None),
        P(RING, None, None),
        P(RING, None, None),
        P(None, RING, None, None),
        P(None, RING, None, None),
        P(None, RING, None, None),
        P("star", "blk", None, None),
        P("star", None, "blk", None, None),
        P("star", "blk", None, None),
        P("star", None, "blk", None, None),
        P("star", "blk", None, None),
    )
    out_specs = (P(None, RING, None, None), P("star", None, "blk", None, None))
    return jax.shard_map(
        on_device, mesh=mesh, in_specs=in_specs, out_specs=out_specs, check_vma=False
    )
```

```python
import functools
import math

import jax
import jax.numpy as jnp
from jax import lax
from jax.experimental import pallas as pl
from jax.experimental.pallas import tpu as pltpu
from jax.sharding import PartitionSpec as P


pair_index = ((0, 1, 2), (1, 3, 4), (2, 4, 5))
sym_pairs = ((0, 0), (0, 1), (0, 2), (1, 1), (1, 2), (2, 2))
weno_eps = 1e-06
RING = ("star", "blk")
LANES = 128
METRIC = 18
EARLY = 5
LATE = 13
FLUID = 7
EARLY_LAYERS = 2 * EARLY + 3 * FLUID + 3
HBM = pl.BlockSpec(memory_space=pltpu.HBM)
GRANT = 24 * 1024 * 1024
VMEM = pl.BlockSpec(memory_space=pltpu.VMEM)
F32 = jnp.float32


class Copies:
    def __init__(self, sems):
        self.sems = sems
        self.count = 0
        self.groups = {}

    def start(self, group, src, dst):
        copy = pltpu.make_async_copy(src, dst, self.sems.at[self.count])
        copy.start()
        self.count += 1
        self.groups.setdefault(group, []).append(copy)

    def wait(self, group):
        for copy in self.groups.pop(group):
            copy.wait()

    def wait_all(self):
        for group in list(self.groups):
            self.wait(group)


def slow_side():
    return lax.rem(lax.axis_index(RING[-1]), 2)


def send_early(copies, group, side, lapse, conf, shift, dens, mom, ener, velo, pres, buf):
    layer = lapse.shape[1:]
    rows = pl.ds(side * (lapse.shape[0] - 2), 2)
    copies.start(group, lapse.at[rows], buf.at[pl.ds(0, 2)])
    copies.start(group, conf.at[rows], buf.at[pl.ds(2, 2)])
    copies.start(group, shift.at[:, rows], buf.at[pl.ds(4, 6)].reshape(3, 2, *layer))
    rows = pl.ds(side * (dens.shape[1] - 3), 3)
    at = 2 * EARLY
    copies.start(group, dens.at[0, rows], buf.at[pl.ds(at, 3)])
    copies.start(group, mom.at[0, :, rows], buf.at[pl.ds(at + 3, 9)].reshape(3, 3, *layer))
    copies.start(group, ener.at[0, rows], buf.at[pl.ds(at + 12, 3)])
    copies.start(group, velo.at[0, 0, rows], buf.at[pl.ds(at + 15, 3)])
    copies.start(group, pres.at[0, rows], buf.at[pl.ds(at + 18, 3)])
    at = at + 3 * FLUID
    copies.start(group, lapse.at[2], buf.at[at])
    copies.start(group, conf.at[2], buf.at[at + 1])
    copies.start(group, shift.at[0, 2], buf.at[at + 2])


def send_late(copies, group, side, mean, metric, curv, buf, at):
    layer = mean.shape[1:]
    rows = pl.ds(side * (mean.shape[0] - 2), 2)
    copies.start(group, mean.at[rows], buf.at[pl.ds(at, 2)])
    copies.start(group, metric.at[:, rows], buf.at[pl.ds(at + 2, 12)].reshape(6, 2, *layer))
    copies.start(group, curv.at[:, rows], buf.at[pl.ds(at + 14, 12)].reshape(6, 2, *layer))


def pack_kernel(lapse, conf, shift, dens, mom, ener, velo, pres, buf, sems):
    copies = Copies(sems)
    send_early(copies, 0, slow_side(), lapse, conf, shift, dens, mom, ener, velo, pres, buf)
    copies.wait_all()


def bssn_layer(state, source, out, at, out_at):
    ny, nz = state.shape[-2:]

    def value(field, off=0):
        return state[field, at + off]

    def rolled(v, axis):
        n = (ny, nz)[axis]
        return tuple(pltpu.roll(v, s % n, axis) for s in (2, 1, -1, -2))

    def first(taps):
        m2, m1, p1, p2 = taps
        return (m2 - p2) + 8.0 * (p1 - m1)

    def second(taps, mid):
        m2, m1, p1, p2 = taps
        return 16.0 * (m1 + p1) - (m2 + p2) - 30.0 * mid

    def xtaps(field):
        return tuple(value(field, o) for o in (-2, -1, 1, 2))

    twelfth = 1.0 / 12.0
    third = 1.0 / 3.0
    lapse = value(0)
    conf = value(1)
    mean = value(2)
    shift12 = [value(15 + n) * twelfth for n in range(3)]

    def gradient(field):
        v = value(field)
        return first(xtaps(field)), first(rolled(v, 0)), first(rolled(v, 1))

    def along_shift(field):
        gx, gy, gz = gradient(field)
        return shift12[0] * gx + shift12[1] * gy + shift12[2] * gz

    dshift = [[None] * 3 for _ in range(3)]
    for n in range(3):
        for k, g in enumerate(gradient(15 + n)):
            dshift[k][n] = g * twelfth
    div_shift = dshift[0][0] + dshift[1][1] + dshift[2][2]
    div23 = (2.0 / 3.0) * div_shift

    taps_x = xtaps(0)
    taps_y = rolled(lapse, 0)
    taps_z = rolled(lapse, 1)
    lx, ly, lz = first(taps_x), first(taps_y), first(taps_z)
    out[0, out_at] = (shift12[0] * lx + shift12[1] * ly + shift12[2] * lz) - 2.0 * lapse * mean
    sq = twelfth * twelfth
    hess = (
        second(taps_x, lapse) * twelfth,
        first(rolled(lx, 0)) * sq,
        first(rolled(lx, 1)) * sq,
        second(taps_y, lapse) * twelfth,
        first(rolled(lz, 0)) * sq,
        second(taps_z, lapse) * twelfth,
    )
    out[1, out_at] = along_shift(1) + conf * ((2.0 / 3.0) * (lapse * mean) - div23)

    a, b, c, d, e, f = g = [value(3 + n) for n in range(6)]
    cof = (d * f - e * e, c * e - b * f, b * e - c * d, a * f - c * c, b * c - a * e, a * d - b * b)
    scale = 1.0 / (a * cof[0] + b * cof[1] + c * cof[2])
    inv = [entry * scale for entry in cof]
    trace = (inv[0] * hess[0] + inv[3] * hess[3] + inv[5] * hess[5]) + 2.0 * (
        inv[1] * hess[1] + inv[2] * hess[2] + inv[4] * hess[4]
    )
    trace3 = trace * third
    curv = [value(9 + n) for n in range(6)]

    def pick(six, i, j):
        return six[pair_index[i][j]]

    def total(terms):
        return functools.reduce(lambda x, y: x + y, terms)

    mixed = [
        [total([pick(curv, i, l) * pick(inv, l, j) for l in range(3)]) for j in range(3)]
        for i in range(3)
    ]
    square = (mixed[0][0] * mixed[0][0] + mixed[1][1] * mixed[1][1] + mixed[2][2] * mixed[2][2]) + 2.0 * (
        mixed[0][1] * mixed[1][0] + mixed[0][2] * mixed[2][0] + mixed[1][2] * mixed[2][1]
    )
    out[2, out_at] = (
        along_shift(2)
        - conf * trace
        + lapse * (square + mean * mean * third + (4.0 * math.pi) * source)
    )
    lapse2 = 2.0 * lapse
    mean_lapse = lapse * mean

    def stretched(six, i, j):
        if i == j:
            return 2.0 * total([pick(six, i, k) * dshift[i][k] for k in range(3)])
        return total([pick(six, i, k) * dshift[j][k] + pick(six, j, k) * dshift[i][k] for k in range(3)])

    for p, (i, j) in enumerate(sym_pairs):
        product = total([mixed[i][k] * pick(curv, k, j) for k in range(3)])
        out[9 + p, out_at] = (
            along_shift(9 + p)
            + (mean_lapse - div23) * curv[p]
            - lapse2 * product
            + stretched(curv, i, j)
            - conf * (hess[p] - trace3 * g[p])
        )
    for p, (i, j) in enumerate(sym_pairs):
        out[3 + p, out_at] = along_shift(3 + p) - lapse2 * curv[p] + stretched(g, i, j) - div23 * g[p]


def lane_matrix(nz, weights):
    row = lax.broadcasted_iota(jnp.int32, (nz, nz), 0)
    col = lax.broadcasted_iota(jnp.int32, (nz, nz), 1)
    return weights(row, col)


def dot(x, y):
    return jnp.dot(x, y, precision=lax.Precision.HIGHEST, preferred_element_type=F32)


def restrict_planes(pairs, rows, outs):
    ny, nz = outs[0][0].shape[-2:]
    half = ny // 2
    quarter_y, quarter_z = ny // 4, nz // 4
    count = len(pairs)
    for n, plane in enumerate(pairs):
        for h in range(nz // LANES):
            rows[h, pl.ds(n * ny, ny), :] = plane()[:, h * LANES : (h + 1) * LANES]
    halves = [
        rows[h, pl.ds(0, count * half, stride=2), :] + rows[h, pl.ds(1, count * half, stride=2), :]
        for h in range(nz // LANES)
    ]
    matrix = lane_matrix(
        nz, lambda r, c: jnp.where(c == quarter_z + lax.shift_right_logical(r, 1), 0.125, 0.0).astype(F32)
    )
    level = dot(jnp.concatenate(halves, axis=1), matrix)
    for n, (out, at) in enumerate(outs):
        out[at] = jnp.zeros((ny, nz), F32)
        out[at, pl.ds(quarter_y, half), :] = level[n * half : (n + 1) * half]


def prolong_yz(planes, rows, out):
    ny, nz = out.shape[-2:]
    half = ny // 2
    start_y, start_z = ny // 4, nz // 4
    flat = [plane for field in planes for plane in field]
    for n, plane in enumerate(flat):
        mid = 0.75 * plane(pl.ds(start_y, half))
        even = mid + 0.25 * plane(pl.ds(start_y - 1, half))
        odd = mid + 0.25 * plane(pl.ds(start_y + 1, half))
        for h in range(nz // LANES):
            lanes = slice(h * LANES, (h + 1) * LANES)
            rows[h, pl.ds(n * ny, half, stride=2), :] = even[:, lanes]
            rows[h, pl.ds(n * ny + 1, half, stride=2), :] = odd[:, lanes]

    def weights(r, c):
        mid = start_z + lax.shift_right_logical(c, 1)
        side = mid - 1 + 2 * (c & 1)
        return jnp.where(r == mid, 0.75, jnp.where(r == side, 0.25, 0.0)).astype(F32)

    matrix = lane_matrix(nz, weights)
    wide = jnp.concatenate([rows[h, pl.ds(0, len(flat) * ny), :] for h in range(nz // LANES)], axis=1)
    fine = dot(wide, matrix)
    at = 0
    for field, layers in enumerate(planes):
        for n in range(len(layers)):
            out[field, n] = fine[at * ny : (at + 1) * ny]
            at += 1


def split_flux(fluid, lapse, shift, conf, out, out_at):
    root = lax.rsqrt(conf)
    transport = lapse * fluid(5) - shift
    weight = lapse * (root * root * root) * fluid(6)
    speed = lapse + jnp.abs(shift)
    for n in range(5):
        u = fluid(n)
        flux = u * transport
        if n == 1:
            flux = flux + weight
        if n == 4:
            flux = flux + weight * fluid(5)
        moved = speed * u
        plus, minus = flux + moved, flux - moved
        out[n, out_at] = plus
        out[5 + n, out_at] = minus


def weno_cells(flux, field, rows, base, count, emit):
    def differences(which, low, high):
        v = {j: flux[which, base + j, rows, :] for j in range(low, high + 1)}
        e = {j: v[j + 1] - v[j] for j in range(low, high)}
        d = {j: e[j] - e[j - 1] for j in range(low + 1, high)}
        t = {j: d[j + 1] - d[j] for j in range(low + 1, high - 1)}
        h = {j: 0.5 * d[j] for j in d}
        s = {j: (13.0 / 12.0) * (d[j] * d[j]) + 4.0 * weno_eps for j in d}
        return v, e, d, t, h, s

    faces = range(-1, count)
    v, e, _, t, h, s = differences(field, -3, count + 1)
    u, eu, _, tu, hu, su = differences(5 + field, -2, count + 2)

    def quotient(b0, b1, b2, t0, t2):
        w0, w1, w2 = b1 * b2, b0 * b2, b0 * b1
        w0, w1, w2 = w0 * w0, 6.0 * (w1 * w1), w2 * w2
        return (w0 * t0 + 1.5 * (w2 * t2)) / (w0 + w1 + 3.0 * w2)

    def square(x):
        return x * x

    previous = None
    for i in faces:
        left = quotient(
            s[i - 1] + square(h[i - 1] + e[i - 1]),
            s[i] + square(h[i] + e[i - 1]),
            s[i + 1] + square(h[i + 1] - e[i]),
            t[i - 1],
            t[i],
        )
        right = quotient(
            su[i + 2] + square(hu[i + 2] - eu[i + 1]),
            su[i + 1] + square(hu[i + 1] - eu[i + 1]),
            su[i] + square(hu[i] + eu[i]),
            tu[i + 1],
            tu[i],
        )
        face = (
            3.0 * (v[i] + u[i + 1])
            + 0.5 * (e[i - 1] - eu[i + 1])
            + (e[i] - eu[i])
            + (right - left)
        )
        if previous is not None:
            emit(i, (previous - face) * (1.0 / 3.0))
        previous = face


def local_kernel(
    packed, lapse, conf, mean, metric, curv, shift, dens, mom, ener, velo, pres,
    state, flux, sources, fluid, fast, late,
    coarse, rows, sems,
):
    nx, ny, nz = lapse.shape
    fx = dens.shape[1]
    copies = Copies(sems)
    inner = pl.ds(2, nx)
    copies.start("c", lapse, state.at[0, inner])
    copies.start("c", conf, state.at[1, inner])
    copies.start("c", shift, state.at[pl.ds(15, 3), inner])
    copies.start("f", dens.at[0], fluid.at[0])
    copies.start("f", mom.at[0], fluid.at[pl.ds(1, 3)])
    copies.start("f", ener.at[0], fluid.at[4])
    copies.start("f", velo.at[0, 0], fluid.at[5])
    copies.start("f", pres.at[0], fluid.at[6])
    copies.start("f", velo.at[0, pl.ds(1, 2)], fluid.at[pl.ds(7, 2)])
    side = slow_side()
    send_late(copies, "o", side, mean, metric, curv, late, 0)
    send_early(copies, "o", 1 - side, lapse, conf, shift, dens, mom, ener, velo, pres, fast)
    send_late(copies, "o", 1 - side, mean, metric, curv, fast, EARLY_LAYERS)
    copies.start("o", mean, state.at[2, inner])
    copies.start("o", metric, state.at[pl.ds(3, 6), inner])
    copies.start("o", curv, state.at[pl.ds(9, 6), inner])

    @pl.loop(2, 15)
    def _(n):
        for k in (0, 1, nx + 2, nx + 3):
            state[n, k] = jnp.zeros((ny, nz), F32)

    copies.wait("c")

    def coarse_plane(field, layer):
        return lambda sl: state[field, layer + 2, sl, :]

    prolong_yz([[coarse_plane(f, l) for l in range(nx)] for f in (0, 15, 1)], rows, coarse)
    copies.wait("f")

    @pl.loop(0, fx - 3)
    def _(i):
        mid = lax.shift_right_logical(i, 1) + 1
        side = mid - 1 + 2 * (i & 1)
        parts = [0.75 * coarse[n, mid] + 0.25 * coarse[n, side] for n in range(3)]
        split_flux(lambda n: fluid[n, i], *parts, flux, i + 3)

    def pair(layer):
        def one(x):
            return (
                fluid[4, x]
                + fluid[0, x]
                + (fluid[1, x] * fluid[5, x] + fluid[2, x] * fluid[7, x] + fluid[3, x] * fluid[8, x])
                + 3.0 * fluid[6, x]
            )

        return lambda: one(2 * layer) + one(2 * layer + 1)

    plane = EARLY_LAYERS + 2 * LATE
    restrict_planes(
        [pair(l) for l in range(nx)],
        rows,
        [(sources, l + 1) for l in range(nx - 1)] + [(late, 2 * LATE)],
    )
    fast[plane] = late[2 * LATE]
    sources[0] = jnp.zeros((ny, nz), F32)
    copies.wait_all()


def inner_kernel(state, flux, sources, rates, hydro, stage, hstage, sems):
    nx, ny, _ = sources.shape
    fx = hydro.shape[2]
    copies = Copies(sems)

    @pl.loop(0, 5)
    def _(n):
        for part in range(ny // 8):
            sl = pl.ds(part * 8, 8)

            def emit(i, value):
                hstage[n, i, sl, :] = value

            weno_cells(flux, n, sl, 9, fx - 12, emit)

    copies.start("o", hstage, hydro.at[0, :, pl.ds(6, fx - 12)])

    @pl.loop(0, nx - 4)
    def _(l):
        bssn_layer(state, sources[l + 2], stage, l + 4, l)

    copies.start("o", stage, rates.at[:, pl.ds(2, nx - 4)])
    copies.wait_all()


def side_work(copies, side, recv, complete, state, flux, sources, fluid, hydro, stage, six, coarse, rows, hstage):
    nx = sources.shape[0]
    ny, _ = sources.shape[-2:]
    fx = fluid.shape[1]
    halo = side * (nx + 2)
    for k in range(2):
        for n, field in enumerate((0, 1, 15, 16, 17)):
            state[field, halo + k] = recv[2 * n + k]
    for n, field in enumerate((0, 1, 15)):
        state[field, nx + 4] = recv[2 * EARLY + 3 * FLUID + n]
    if complete:

        @pl.loop(0, LATE)
        def _(n):
            for k in range(2):
                state[2 + n, halo + k] = recv[EARLY_LAYERS + 2 * n + k]

    place = lax.axis_index(RING[-1])
    outer = jnp.where(side == 0, place == 0, place == lax.axis_size(RING[-1]) - 1)
    inside = jnp.where(outer, 0.0, 1.0).astype(F32)
    for n in range(FLUID):
        for k in range(3):
            value = recv[2 * EARLY + 3 * n + k]
            six[n, 3 * side + k] = value if n == 5 else value * inside
            six[n, 3 - 3 * side + k] = fluid[n, side * (fx - 3) + k]

    def coarse_plane(field, layer):
        return lambda sl: state[field, side * nx + 1 + layer, sl, :]

    prolong_yz([[coarse_plane(f, l) for l in range(4)] for f in (0, 15, 1)], rows, coarse)

    @pl.loop(0, 6)
    def _(j):
        mid = lax.shift_right_logical(j + 1, 1)
        other = mid + 1 - 2 * (j & 1)
        parts = [0.75 * coarse[n, mid] + 0.25 * coarse[n, other] for n in range(3)]
        split_flux(lambda n: six[n, j], *parts, flux, side * fx + j)

    first = side * (fx - 6)

    @pl.loop(0, 5)
    def _(n):
        for part in range(ny // 8):
            sl = pl.ds(part * 8, 8)

            def emit(i, value):
                hstage[n, i, sl, :] = value

            weno_cells(flux, n, sl, first + 3, 6, emit)

    copies.start("o", hstage, hydro.at[0, :, pl.ds(first, 6)])

    @pl.loop(0, 2)
    def _(k):
        l = side * (nx - 2) + k
        source = sources[l]
        if complete:
            source = source + jnp.where(l == 0, 1.0, 0.0).astype(F32) * recv[EARLY_LAYERS + 2 * LATE]
        bssn_layer(state, source, stage, l + 2, k)


def fast_kernel(
    recv, rates_in, hydro_in, state_in, flux_in, sources, fluid,
    rates, hydro, state, flux,
    stage, six, coarse, rows, hstage, sems,
):
    copies = Copies(sems)
    side = 1 - slow_side()
    side_work(copies, side, recv, True, state, flux, sources, fluid, hydro, stage, six, coarse, rows, hstage)
    copies.start("o", stage, rates.at[:, pl.ds(side * (rates.shape[1] - 2), 2)])
    copies.wait_all()


def slow_kernel(
    recv, hydro_in, state_in, flux_in, sources, fluid,
    hydro, state, flux, stage,
    six, coarse, rows, hstage, sems,
):
    copies = Copies(sems)
    side_work(copies, slow_side(), recv, False, state, flux, sources, fluid, hydro, stage, six, coarse, rows, hstage)
    copies.wait_all()


def late_kernel(recv, stage_in, state, rates_in, rates, stage, sems):
    nx = rates.shape[1]
    copies = Copies(sems)
    side = slow_side()
    low = side == 0

    def pick(below, above):
        return jnp.where(low, below, above).astype(F32)

    taps = ((pick(1.0, -1.0), pick(-8.0, 0.0)), (pick(0.0, 8.0), pick(1.0, -1.0)))
    first = side * (nx - 2)
    for k in range(2):
        step = state[15, first + 2 + k] * (1.0 / 12.0)
        for field in range(15):
            value = stage_in[field, k]
            if field >= 2:
                at = 2 * (field - 2)
                value = value + step * (taps[k][0] * recv[at] + taps[k][1] * recv[at + 1])
            if field == 2 and k == 0:
                value = value + pick(4.0 * math.pi, 0.0) * state[0, 2] * recv[2 * LATE]
            stage[field, k] = value
    copies.start("o", stage, rates.at[:, pl.ds(first, 2)])
    copies.wait_all()


def substep(*fields):
    fields = [pltpu.with_memory_space_constraint(field, pltpu.HBM) for field in fields]
    lapse, conf, _, _, _, shift, dens, mom, ener, velo, pres = fields
    nx, ny, nz = lapse.shape
    fx = dens.shape[1]
    layer = (ny, nz)

    def shape(*leading):
        return jax.ShapeDtypeStruct(leading + layer, F32)

    def vmem(*leading):
        return pltpu.VMEM(leading + layer, F32)

    def row_scratch(planes):
        return pltpu.VMEM((nz // LANES, planes * ny, LANES), F32)

    def sems(n):
        return pltpu.SemaphoreType.DMA((n,))

    count = lax.axis_size(RING)
    fast_pairs = [(i, i ^ 1) for i in range(count)]
    slow_pairs = [(i, (i + (1 if i % 2 else -1)) % count) for i in range(count)]
    params = pltpu.CompilerParams(vmem_limit_bytes=GRANT)

    def cost(flops):
        return pl.CostEstimate(flops=flops, transcendentals=0, bytes_accessed=6_000_000)

    early = pl.pallas_call(
        pack_kernel,
        out_shape=shape(EARLY_LAYERS),
        in_specs=[HBM] * 8,
        out_specs=VMEM,
        scratch_shapes=[sems(16)],
        compiler_params=params,
        name="pack",
    )(lapse, conf, shift, dens, mom, ener, velo, pres)
    packed = early
    early = lax.ppermute(early, RING, slow_pairs)
    local = pl.pallas_call(
        local_kernel,
        out_shape=(
            shape(METRIC, nx + 5),
            shape(10, fx + 6),
            shape(nx),
            shape(9, fx),
            shape(EARLY_LAYERS + 2 * LATE + 1),
            shape(2 * LATE + 1),
        ),
        in_specs=[VMEM] + [HBM] * 11,
        out_specs=[VMEM] * 6,
        scratch_shapes=[vmem(3, nx), row_scratch(3 * nx), sems(40)],
        cost_estimate=cost(200_000_000),
        compiler_params=params,
        name="local",
    )
    state, flux, sources, fluid, fast, late = local(packed, *fields)
    fast = lax.ppermute(fast, RING, fast_pairs)
    late = lax.ppermute(late, RING, slow_pairs)
    rates, hydro = pl.pallas_call(
        inner_kernel,
        out_shape=(shape(15, nx), shape(1, 5, fx)),
        in_specs=[VMEM] * 3,
        out_specs=[HBM] * 2,
        scratch_shapes=[vmem(15, nx - 4), vmem(5, fx - 12), sems(4)],
        cost_estimate=cost(400_000_000),
        compiler_params=params,
        name="inner",
    )(state, flux, sources)
    work = [vmem(FLUID, 6), vmem(3, 4), row_scratch(12), vmem(5, 6), sems(4)]
    rates, hydro, state, flux = pl.pallas_call(
        fast_kernel,
        out_shape=(shape(15, nx), shape(1, 5, fx), shape(METRIC, nx + 5), shape(10, fx + 6)),
        in_specs=[VMEM] + [HBM] * 2 + [VMEM] * 4,
        out_specs=[HBM] * 2 + [VMEM] * 2,
        input_output_aliases={1: 0, 2: 1, 3: 2, 4: 3},
        scratch_shapes=[vmem(15, 2)] + work,
        cost_estimate=cost(300_000_000),
        compiler_params=params,
        name="fast",
    )(fast, rates, hydro, state, flux, sources, fluid)
    hydro, state, _, stage = pl.pallas_call(
        slow_kernel,
        out_shape=(shape(1, 5, fx), shape(METRIC, nx + 5), shape(10, fx + 6), shape(15, 2)),
        in_specs=[VMEM, HBM] + [VMEM] * 4,
        out_specs=[HBM] + [VMEM] * 3,
        input_output_aliases={1: 0, 2: 1, 3: 2},
        scratch_shapes=work,
        cost_estimate=cost(300_000_000),
        compiler_params=params,
        name="slow",
    )(early, hydro, state, flux, sources, fluid)
    rates = pl.pallas_call(
        late_kernel,
        out_shape=shape(15, nx),
        in_specs=[VMEM] * 3 + [HBM],
        out_specs=HBM,
        input_output_aliases={3: 0},
        scratch_shapes=[vmem(15, 2), sems(4)],
        compiler_params=params,
        name="late",
    )(late, stage, state, rates)
    return rates, hydro


def solution(mesh):
    in_specs = (
        P(RING, None, None),
        P(RING, None, None),
        P(RING, None, None),
        P(None, RING, None, None),
        P(None, RING, None, None),
        P(None, RING, None, None),
        P("star", "blk", None, None),
        P("star", None, "blk", None, None),
        P("star", "blk", None, None),
        P("star", None, "blk", None, None),
        P("star", "blk", None, None),
    )
    out_specs = (P(None, RING, None, None), P("star", None, "blk", None, None))
    return jax.shard_map(substep, mesh=mesh, in_specs=in_specs, out_specs=out_specs, check_vma=False)
```

```python
import functools
import math

import jax
import jax.numpy as jnp
from jax import lax
from jax.experimental import pallas as pl
from jax.experimental.pallas import tpu as pltpu
from jax.sharding import PartitionSpec as P


pair_index = ((0, 1, 2), (1, 3, 4), (2, 4, 5))
sym_pairs = ((0, 0), (0, 1), (0, 2), (1, 1), (1, 2), (2, 2))
weno_eps = 1e-06
RING = ("star", "blk")
LANES = 128
METRIC = 18
EARLY = 5
LATE = 13
PLANE = 2 * LATE - 2
FLUID = 7
EARLY_LAYERS = 2 * EARLY + 3 * FLUID + 2
SPARE = EARLY_LAYERS - 2
HBM = pl.BlockSpec(memory_space=pltpu.HBM)
GRANT = 24 * 1024 * 1024
VMEM = pl.BlockSpec(memory_space=pltpu.VMEM)
F32 = jnp.float32


class Copies:
    def __init__(self, sems):
        self.sems = sems
        self.count = 0
        self.groups = {}

    def start(self, group, src, dst):
        copy = pltpu.make_async_copy(src, dst, self.sems.at[self.count])
        copy.start()
        self.count += 1
        self.groups.setdefault(group, []).append(copy)

    def wait(self, group):
        for copy in self.groups.pop(group):
            copy.wait()

    def wait_all(self):
        for group in list(self.groups):
            self.wait(group)


def slow_side():
    return lax.rem(lax.axis_index(RING[-1]), 2)


def coarse_rows(ny):
    first, count = ny // 4 - 1, ny // 2 + 2
    parts = []
    for n in range(3):
        done = 0
        while done < count:
            at = n * count + done
            step = min(count - done, ny - at % ny)
            parts.append((n, first + done, step, at // ny, at % ny))
            done += step
    return parts


def send_early(copies, group, side, lapse, conf, shift, dens, mom, ener, velo, pres, buf):
    layer = lapse.shape[1:]
    rows = pl.ds(side * (lapse.shape[0] - 2), 2)
    copies.start(group, lapse.at[rows], buf.at[pl.ds(0, 2)])
    copies.start(group, conf.at[rows], buf.at[pl.ds(2, 2)])
    copies.start(group, shift.at[:, rows], buf.at[pl.ds(4, 6)].reshape(3, 2, *layer))
    rows = pl.ds(side * (dens.shape[1] - 3), 3)
    at = 2 * EARLY
    copies.start(group, dens.at[0, rows], buf.at[pl.ds(at, 3)])
    copies.start(group, mom.at[0, :, rows], buf.at[pl.ds(at + 3, 9)].reshape(3, 3, *layer))
    copies.start(group, ener.at[0, rows], buf.at[pl.ds(at + 12, 3)])
    copies.start(group, velo.at[0, 0, rows], buf.at[pl.ds(at + 15, 3)])
    copies.start(group, pres.at[0, rows], buf.at[pl.ds(at + 18, 3)])


def send_late(copies, group, side, mean, metric, curv, buf, at):
    layer = mean.shape[1:]
    rows = pl.ds(side * (mean.shape[0] - 2), 2)
    copies.start(group, metric.at[:, rows], buf.at[pl.ds(at, 12)].reshape(6, 2, *layer))
    copies.start(group, curv.at[:, rows], buf.at[pl.ds(at + 12, 12)].reshape(6, 2, *layer))
    copies.start(group, mean.at[rows], buf.at[pl.ds(at + 24, 2)])


def fill_spare(up, third, mean, buf):
    @pl.when(up)
    def _():
        for k in range(2):
            buf[SPARE + k] = mean(k)

    @pl.when(jnp.logical_not(up))
    def _():
        for n, row, count, layer, at in coarse_rows(buf.shape[1]):
            buf[SPARE + layer, pl.ds(at, count), :] = third(n, pl.ds(row, count))


def pack_kernel(lapse, conf, shift, mean, dens, mom, ener, velo, pres, buf, third, high, sems):
    copies = Copies(sems)
    side = slow_side()
    copies.start("s", lapse.at[2], third.at[0])
    copies.start("s", conf.at[2], third.at[1])
    copies.start("s", shift.at[0, 2], third.at[2])
    copies.start("s", mean.at[pl.ds(mean.shape[0] - 2, 2)], high)
    send_early(copies, 0, side, lapse, conf, shift, dens, mom, ener, velo, pres, buf)
    buf[EARLY_LAYERS - 1] = jnp.zeros(buf.shape[1:], F32)
    copies.wait("s")
    fill_spare(side == 1, lambda n, sl: third[n, sl, :], lambda k: high[k], buf)
    copies.wait_all()


def bssn_layer(state, source, out, at, out_at):
    ny, nz = state.shape[-2:]

    def value(field, off=0):
        return state[field, at + off]

    def rolled(v, axis):
        n = (ny, nz)[axis]
        return tuple(pltpu.roll(v, s % n, axis) for s in (2, 1, -1, -2))

    def first(taps):
        m2, m1, p1, p2 = taps
        return (m2 - p2) + 8.0 * (p1 - m1)

    def second(taps, mid):
        m2, m1, p1, p2 = taps
        return 16.0 * (m1 + p1) - (m2 + p2) - 30.0 * mid

    def xtaps(field):
        return tuple(value(field, o) for o in (-2, -1, 1, 2))

    twelfth = 1.0 / 12.0
    third = 1.0 / 3.0
    lapse = value(0)
    conf = value(1)
    mean = value(2)
    shift12 = [value(15 + n) * twelfth for n in range(3)]

    def gradient(field):
        v = value(field)
        return first(xtaps(field)), first(rolled(v, 0)), first(rolled(v, 1))

    def along_shift(field):
        gx, gy, gz = gradient(field)
        return shift12[0] * gx + shift12[1] * gy + shift12[2] * gz

    dshift = [[None] * 3 for _ in range(3)]
    for n in range(3):
        for k, g in enumerate(gradient(15 + n)):
            dshift[k][n] = g * twelfth
    div_shift = dshift[0][0] + dshift[1][1] + dshift[2][2]
    div23 = (2.0 / 3.0) * div_shift

    taps_x = xtaps(0)
    taps_y = rolled(lapse, 0)
    taps_z = rolled(lapse, 1)
    lx, ly, lz = first(taps_x), first(taps_y), first(taps_z)
    out[0, out_at] = (shift12[0] * lx + shift12[1] * ly + shift12[2] * lz) - 2.0 * lapse * mean
    sq = twelfth * twelfth
    hess = (
        second(taps_x, lapse) * twelfth,
        first(rolled(lx, 0)) * sq,
        first(rolled(lx, 1)) * sq,
        second(taps_y, lapse) * twelfth,
        first(rolled(lz, 0)) * sq,
        second(taps_z, lapse) * twelfth,
    )
    out[1, out_at] = along_shift(1) + conf * ((2.0 / 3.0) * (lapse * mean) - div23)

    a, b, c, d, e, f = g = [value(3 + n) for n in range(6)]
    cof = (d * f - e * e, c * e - b * f, b * e - c * d, a * f - c * c, b * c - a * e, a * d - b * b)
    scale = 1.0 / (a * cof[0] + b * cof[1] + c * cof[2])
    inv = [entry * scale for entry in cof]
    trace = (inv[0] * hess[0] + inv[3] * hess[3] + inv[5] * hess[5]) + 2.0 * (
        inv[1] * hess[1] + inv[2] * hess[2] + inv[4] * hess[4]
    )
    trace3 = trace * third
    curv = [value(9 + n) for n in range(6)]

    def pick(six, i, j):
        return six[pair_index[i][j]]

    def total(terms):
        return functools.reduce(lambda x, y: x + y, terms)

    mixed = [
        [total([pick(curv, i, l) * pick(inv, l, j) for l in range(3)]) for j in range(3)]
        for i in range(3)
    ]
    square = (mixed[0][0] * mixed[0][0] + mixed[1][1] * mixed[1][1] + mixed[2][2] * mixed[2][2]) + 2.0 * (
        mixed[0][1] * mixed[1][0] + mixed[0][2] * mixed[2][0] + mixed[1][2] * mixed[2][1]
    )
    out[2, out_at] = (
        along_shift(2)
        - conf * trace
        + lapse * (square + mean * mean * third + (4.0 * math.pi) * source)
    )
    lapse2 = 2.0 * lapse
    mean_lapse = lapse * mean

    def stretched(six, i, j):
        if i == j:
            return 2.0 * total([pick(six, i, k) * dshift[i][k] for k in range(3)])
        return total([pick(six, i, k) * dshift[j][k] + pick(six, j, k) * dshift[i][k] for k in range(3)])

    for p, (i, j) in enumerate(sym_pairs):
        product = total([mixed[i][k] * pick(curv, k, j) for k in range(3)])
        out[9 + p, out_at] = (
            along_shift(9 + p)
            + (mean_lapse - div23) * curv[p]
            - lapse2 * product
            + stretched(curv, i, j)
            - conf * (hess[p] - trace3 * g[p])
        )
    for p, (i, j) in enumerate(sym_pairs):
        out[3 + p, out_at] = along_shift(3 + p) - lapse2 * curv[p] + stretched(g, i, j) - div23 * g[p]


def lane_matrix(nz, weights):
    row = lax.broadcasted_iota(jnp.int32, (nz, nz), 0)
    col = lax.broadcasted_iota(jnp.int32, (nz, nz), 1)
    return weights(row, col)


def dot(x, y):
    return jnp.dot(x, y, precision=lax.Precision.HIGHEST, preferred_element_type=F32)


def restrict_planes(pairs, rows, outs):
    ny, nz = outs[0][0].shape[-2:]
    half = ny // 2
    quarter_y, quarter_z = ny // 4, nz // 4
    count = len(pairs)
    for n, plane in enumerate(pairs):
        for h in range(nz // LANES):
            rows[h, pl.ds(n * ny, ny), :] = plane()[:, h * LANES : (h + 1) * LANES]
    halves = [
        rows[h, pl.ds(0, count * half, stride=2), :] + rows[h, pl.ds(1, count * half, stride=2), :]
        for h in range(nz // LANES)
    ]
    matrix = lane_matrix(
        nz, lambda r, c: jnp.where(c == quarter_z + lax.shift_right_logical(r, 1), 0.125, 0.0).astype(F32)
    )
    level = dot(jnp.concatenate(halves, axis=1), matrix)
    for n, (out, at) in enumerate(outs):
        out[at] = jnp.zeros((ny, nz), F32)
        out[at, pl.ds(quarter_y, half), :] = level[n * half : (n + 1) * half]


def prolong_yz(planes, rows, out):
    ny, nz = out.shape[-2:]
    half = ny // 2
    start_y, start_z = ny // 4, nz // 4
    flat = [plane for field in planes for plane in field]
    for n, plane in enumerate(flat):
        mid = 0.75 * plane(pl.ds(start_y, half))
        even = mid + 0.25 * plane(pl.ds(start_y - 1, half))
        odd = mid + 0.25 * plane(pl.ds(start_y + 1, half))
        for h in range(nz // LANES):
            lanes = slice(h * LANES, (h + 1) * LANES)
            rows[h, pl.ds(n * ny, half, stride=2), :] = even[:, lanes]
            rows[h, pl.ds(n * ny + 1, half, stride=2), :] = odd[:, lanes]

    def weights(r, c):
        mid = start_z + lax.shift_right_logical(c, 1)
        side = mid - 1 + 2 * (c & 1)
        return jnp.where(r == mid, 0.75, jnp.where(r == side, 0.25, 0.0)).astype(F32)

    matrix = lane_matrix(nz, weights)
    wide = jnp.concatenate([rows[h, pl.ds(0, len(flat) * ny), :] for h in range(nz // LANES)], axis=1)
    fine = dot(wide, matrix)
    at = 0
    for field, layers in enumerate(planes):
        for n in range(len(layers)):
            out[field, n] = fine[at * ny : (at + 1) * ny]
            at += 1


def split_flux(fluid, lapse, shift, conf, out, out_at):
    root = lax.rsqrt(conf)
    transport = lapse * fluid(5) - shift
    weight = lapse * (root * root * root) * fluid(6)
    speed = lapse + jnp.abs(shift)
    for n in range(5):
        u = fluid(n)
        flux = u * transport
        if n == 1:
            flux = flux + weight
        if n == 4:
            flux = flux + weight * fluid(5)
        moved = speed * u
        plus, minus = flux + moved, flux - moved
        out[n, out_at] = plus
        out[5 + n, out_at] = minus


def weno_cells(flux, field, rows, base, count, emit):
    def differences(which, low, high):
        v = {j: flux[which, base + j, rows, :] for j in range(low, high + 1)}
        e = {j: v[j + 1] - v[j] for j in range(low, high)}
        d = {j: e[j] - e[j - 1] for j in range(low + 1, high)}
        t = {j: d[j + 1] - d[j] for j in range(low + 1, high - 1)}
        h = {j: 0.5 * d[j] for j in d}
        s = {j: (13.0 / 12.0) * (d[j] * d[j]) + 4.0 * weno_eps for j in d}
        return v, e, d, t, h, s

    faces = range(-1, count)
    v, e, _, t, h, s = differences(field, -3, count + 1)
    u, eu, _, tu, hu, su = differences(5 + field, -2, count + 2)

    def quotient(b0, b1, b2, t0, t2):
        w0, w1, w2 = b1 * b2, b0 * b2, b0 * b1
        w0, w1, w2 = w0 * w0, 6.0 * (w1 * w1), w2 * w2
        return (w0 * t0 + 1.5 * (w2 * t2)) / (w0 + w1 + 3.0 * w2)

    def square(x):
        return x * x

    previous = None
    for i in faces:
        left = quotient(
            s[i - 1] + square(h[i - 1] + e[i - 1]),
            s[i] + square(h[i] + e[i - 1]),
            s[i + 1] + square(h[i + 1] - e[i]),
            t[i - 1],
            t[i],
        )
        right = quotient(
            su[i + 2] + square(hu[i + 2] - eu[i + 1]),
            su[i + 1] + square(hu[i + 1] - eu[i + 1]),
            su[i] + square(hu[i] + eu[i]),
            tu[i + 1],
            tu[i],
        )
        face = (
            3.0 * (v[i] + u[i + 1])
            + 0.5 * (e[i - 1] - eu[i + 1])
            + (e[i] - eu[i])
            + (right - left)
        )
        if previous is not None:
            emit(i, (previous - face) * (1.0 / 3.0))
        previous = face


def local_kernel(
    packed, lapse, conf, mean, metric, curv, shift, dens, mom, ener, velo, pres,
    state, flux, sources, fluid, fast, late,
    coarse, rows, sems,
):
    nx, ny, nz = lapse.shape
    fx = dens.shape[1]
    copies = Copies(sems)
    inner = pl.ds(2, nx)
    copies.start("c", lapse, state.at[0, inner])
    copies.start("c", conf, state.at[1, inner])
    copies.start("c", shift, state.at[pl.ds(15, 3), inner])
    copies.start("f", dens.at[0], fluid.at[0])
    copies.start("f", mom.at[0], fluid.at[pl.ds(1, 3)])
    copies.start("f", ener.at[0], fluid.at[4])
    copies.start("f", velo.at[0, 0], fluid.at[5])
    copies.start("f", pres.at[0], fluid.at[6])
    copies.start("f", velo.at[0, pl.ds(1, 2)], fluid.at[pl.ds(7, 2)])
    side = slow_side()
    send_late(copies, "o", side, mean, metric, curv, late, 0)
    send_early(copies, "o", 1 - side, lapse, conf, shift, dens, mom, ener, velo, pres, fast)
    send_late(copies, "o", 1 - side, mean, metric, curv, fast, EARLY_LAYERS)
    copies.start("o", mean, state.at[2, inner])
    copies.start("o", metric, state.at[pl.ds(3, 6), inner])
    copies.start("o", curv, state.at[pl.ds(9, 6), inner])

    @pl.loop(2, 15)
    def _(n):
        for k in (0, 1, nx + 2, nx + 3):
            state[n, k] = jnp.zeros((ny, nz), F32)

    copies.wait("c")

    def coarse_plane(field, layer):
        return lambda sl: state[field, layer + 2, sl, :]

    prolong_yz([[coarse_plane(f, l) for l in range(nx)] for f in (0, 15, 1)], rows, coarse)
    copies.wait("f")

    @pl.loop(0, fx - 3)
    def _(i):
        mid = lax.shift_right_logical(i, 1) + 1
        side = mid - 1 + 2 * (i & 1)
        parts = [0.75 * coarse[n, mid] + 0.25 * coarse[n, side] for n in range(3)]
        split_flux(lambda n: fluid[n, i], *parts, flux, i + 3)

    def pair(layer):
        def one(x):
            return (
                fluid[4, x]
                + fluid[0, x]
                + (fluid[1, x] * fluid[5, x] + fluid[2, x] * fluid[7, x] + fluid[3, x] * fluid[8, x])
                + 3.0 * fluid[6, x]
            )

        return lambda: one(2 * layer) + one(2 * layer + 1)

    plane = EARLY_LAYERS + 2 * LATE
    restrict_planes(
        [pair(l) for l in range(nx)],
        rows,
        [(sources, l + 1) for l in range(nx - 1)] + [(fast, plane)],
    )
    sources[0] = jnp.zeros((ny, nz), F32)
    for k in range(2):
        fast[SPARE + k] = jnp.zeros((ny, nz), F32)
    for n, row, count, layer, at in coarse_rows(ny):
        fast[SPARE + layer, pl.ds(at, count), :] = state[(0, 1, 15)[n], 4, pl.ds(row, count), :]
    copies.wait_all()

    @pl.when(slow_side() == 1)
    def _():
        late[PLANE] = fast[plane]


def inner_kernel(state, flux, sources, rates, hydro, stage, hstage, sems):
    nx, ny, _ = sources.shape
    fx = hydro.shape[2]
    copies = Copies(sems)

    @pl.loop(0, 5)
    def _(n):
        for part in range(ny // 8):
            sl = pl.ds(part * 8, 8)

            def emit(i, value):
                hstage[n, i, sl, :] = value

            weno_cells(flux, n, sl, 9, fx - 12, emit)

    copies.start("o", hstage, hydro.at[0, :, pl.ds(6, fx - 12)])

    @pl.loop(0, nx - 4)
    def _(l):
        bssn_layer(state, sources[l + 2], stage, l + 4, l)

    copies.start("o", stage, rates.at[:, pl.ds(2, nx - 4)])
    copies.wait_all()


def side_work(copies, side, recv, complete, state, flux, sources, fluid, hydro, stage, six, coarse, rows, hstage):
    nx = sources.shape[0]
    ny, _ = sources.shape[-2:]
    fx = fluid.shape[1]
    halo = side * (nx + 2)
    for k in range(2):
        for n, field in enumerate((0, 1, 15, 16, 17)):
            state[field, halo + k] = recv[2 * n + k]
    for n, row, count, layer, at in coarse_rows(ny):
        state[(0, 1, 15)[n], nx + 4, pl.ds(row, count), :] = recv[SPARE + layer, pl.ds(at, count), :]
    if complete:

        @pl.loop(0, LATE)
        def _(n):
            for k in range(2):
                field = jnp.where(n == LATE - 1, 2, n + 3)
                state[field, halo + k] = recv[EARLY_LAYERS + 2 * n + k]

    place = lax.axis_index(RING[-1])
    outer = jnp.where(side == 0, place == 0, place == lax.axis_size(RING[-1]) - 1)
    inside = jnp.where(outer, 0.0, 1.0).astype(F32)
    for n in range(FLUID):
        for k in range(3):
            value = recv[2 * EARLY + 3 * n + k]
            six[n, 3 * side + k] = value if n == 5 else value * inside
            six[n, 3 - 3 * side + k] = fluid[n, side * (fx - 3) + k]

    def coarse_plane(field, layer):
        return lambda sl: state[field, side * nx + 1 + layer, sl, :]

    prolong_yz([[coarse_plane(f, l) for l in range(4)] for f in (0, 15, 1)], rows, coarse)

    @pl.loop(0, 6)
    def _(j):
        mid = lax.shift_right_logical(j + 1, 1)
        other = mid + 1 - 2 * (j & 1)
        parts = [0.75 * coarse[n, mid] + 0.25 * coarse[n, other] for n in range(3)]
        split_flux(lambda n: six[n, j], *parts, flux, side * fx + j)

    first = side * (fx - 6)

    @pl.loop(0, 5)
    def _(n):
        for part in range(ny // 8):
            sl = pl.ds(part * 8, 8)

            def emit(i, value):
                hstage[n, i, sl, :] = value

            weno_cells(flux, n, sl, first + 3, 6, emit)

    copies.start("o", hstage, hydro.at[0, :, pl.ds(first, 6)])

    @pl.loop(0, 2)
    def _(k):
        l = side * (nx - 2) + k
        source = sources[l]
        if complete:
            source = source + jnp.where(l == 0, 1.0, 0.0).astype(F32) * recv[EARLY_LAYERS + 2 * LATE]
        bssn_layer(state, source, stage, l + 2, k)


def fast_kernel(
    recv, rates_in, hydro_in, state_in, flux_in, sources, fluid,
    rates, hydro, state, flux,
    stage, six, coarse, rows, hstage, sems,
):
    copies = Copies(sems)
    side = 1 - slow_side()
    side_work(copies, side, recv, True, state, flux, sources, fluid, hydro, stage, six, coarse, rows, hstage)
    copies.start("o", stage, rates.at[:, pl.ds(side * (rates.shape[1] - 2), 2)])
    copies.wait_all()


def slow_kernel(
    recv, hydro_in, state_in, flux_in, sources, fluid,
    hydro, state, flux, stage,
    six, coarse, rows, hstage, sems,
):
    copies = Copies(sems)
    side_work(copies, slow_side(), recv, False, state, flux, sources, fluid, hydro, stage, six, coarse, rows, hstage)
    copies.wait_all()


def late_kernel(recv, early, stage_in, state, rates_in, rates, stage, sems):
    nx = rates.shape[1]
    copies = Copies(sems)
    side = slow_side()
    low = side == 0

    def pick(below, above):
        return jnp.where(low, below, above).astype(F32)

    taps = ((pick(1.0, -1.0), pick(-8.0, 0.0)), (pick(0.0, 8.0), pick(1.0, -1.0)))
    first = side * (nx - 2)
    for k in range(2):
        step = state[15, first + 2 + k] * (1.0 / 12.0)
        for field in range(15):
            value = stage_in[field, k]
            if field == 2:
                values = [jnp.where(low, early[SPARE + n], recv[PLANE + n]) for n in range(2)]
            elif field > 2:
                values = [recv[2 * (field - 3) + n] for n in range(2)]
            if field >= 2:
                value = value + step * (taps[k][0] * values[0] + taps[k][1] * values[1])
            if field == 2 and k == 0:
                value = value + pick(4.0 * math.pi, 0.0) * state[0, 2] * recv[PLANE]
            stage[field, k] = value
    copies.start("o", stage, rates.at[:, pl.ds(first, 2)])
    copies.wait_all()


def substep(*fields):
    fields = [pltpu.with_memory_space_constraint(field, pltpu.HBM) for field in fields]
    lapse, conf, mean, _, _, shift, dens, mom, ener, velo, pres = fields
    nx, ny, nz = lapse.shape
    fx = dens.shape[1]
    layer = (ny, nz)

    def shape(*leading):
        return jax.ShapeDtypeStruct(leading + layer, F32)

    def vmem(*leading):
        return pltpu.VMEM(leading + layer, F32)

    def row_scratch(planes):
        return pltpu.VMEM((nz // LANES, planes * ny, LANES), F32)

    def sems(n):
        return pltpu.SemaphoreType.DMA((n,))

    count = lax.axis_size(RING)
    fast_pairs = [(i, i ^ 1) for i in range(count)]
    slow_pairs = [(i, (i + (1 if i % 2 else -1)) % count) for i in range(count)]
    params = pltpu.CompilerParams(vmem_limit_bytes=GRANT)

    def cost(flops):
        return pl.CostEstimate(flops=flops, transcendentals=0, bytes_accessed=6_000_000)

    early = pl.pallas_call(
        pack_kernel,
        out_shape=shape(EARLY_LAYERS),
        in_specs=[HBM] * 9,
        out_specs=VMEM,
        scratch_shapes=[vmem(3), vmem(2), sems(16)],
        compiler_params=params,
        name="pack",
    )(lapse, conf, shift, mean, dens, mom, ener, velo, pres)
    packed = early
    early = lax.ppermute(early, RING, slow_pairs)
    local = pl.pallas_call(
        local_kernel,
        out_shape=(
            shape(METRIC, nx + 5),
            shape(10, fx + 6),
            shape(nx),
            shape(9, fx),
            shape(EARLY_LAYERS + 2 * LATE + 1),
            shape(2 * LATE),
        ),
        in_specs=[VMEM] + [HBM] * 11,
        out_specs=[VMEM] * 6,
        scratch_shapes=[vmem(3, nx), row_scratch(3 * nx), sems(40)],
        cost_estimate=cost(200_000_000),
        compiler_params=params,
        name="local",
    )
    state, flux, sources, fluid, fast, late = local(packed, *fields)
    fast = lax.ppermute(fast, RING, fast_pairs)
    late = lax.ppermute(late, RING, slow_pairs)
    rates, hydro = pl.pallas_call(
        inner_kernel,
        out_shape=(shape(15, nx), shape(1, 5, fx)),
        in_specs=[VMEM] * 3,
        out_specs=[HBM] * 2,
        scratch_shapes=[vmem(15, nx - 4), vmem(5, fx - 12), sems(4)],
        cost_estimate=cost(400_000_000),
        compiler_params=params,
        name="inner",
    )(state, flux, sources)
    work = [vmem(FLUID, 6), vmem(3, 4), row_scratch(12), vmem(5, 6), sems(4)]
    rates, hydro, state, flux = pl.pallas_call(
        fast_kernel,
        out_shape=(shape(15, nx), shape(1, 5, fx), shape(METRIC, nx + 5), shape(10, fx + 6)),
        in_specs=[VMEM] + [HBM] * 2 + [VMEM] * 4,
        out_specs=[HBM] * 2 + [VMEM] * 2,
        input_output_aliases={1: 0, 2: 1, 3: 2, 4: 3},
        scratch_shapes=[vmem(15, 2)] + work,
        cost_estimate=cost(300_000_000),
        compiler_params=params,
        name="fast",
    )(fast, rates, hydro, state, flux, sources, fluid)
    hydro, state, _, stage = pl.pallas_call(
        slow_kernel,
        out_shape=(shape(1, 5, fx), shape(METRIC, nx + 5), shape(10, fx + 6), shape(15, 2)),
        in_specs=[VMEM, HBM] + [VMEM] * 4,
        out_specs=[HBM] + [VMEM] * 3,
        input_output_aliases={1: 0, 2: 1, 3: 2},
        scratch_shapes=work,
        cost_estimate=cost(300_000_000),
        compiler_params=params,
        name="slow",
    )(early, hydro, state, flux, sources, fluid)
    rates = pl.pallas_call(
        late_kernel,
        out_shape=shape(15, nx),
        in_specs=[VMEM] * 4 + [HBM],
        out_specs=HBM,
        input_output_aliases={4: 0},
        scratch_shapes=[vmem(15, 2), sems(4)],
        compiler_params=params,
        name="late",
    )(late, early, stage, state, rates)
    return rates, hydro


def solution(mesh):
    in_specs = (
        P(RING, None, None),
        P(RING, None, None),
        P(RING, None, None),
        P(None, RING, None, None),
        P(None, RING, None, None),
        P(None, RING, None, None),
        P("star", "blk", None, None),
        P("star", None, "blk", None, None),
        P("star", "blk", None, None),
        P("star", None, "blk", None, None),
        P("star", "blk", None, None),
    )
    out_specs = (P(None, RING, None, None), P("star", None, "blk", None, None))
    return jax.shard_map(substep, mesh=mesh, in_specs=in_specs, out_specs=out_specs, check_vma=False)
```

```python
import functools
import math

import jax
import jax.numpy as jnp
from jax import lax
from jax.experimental import pallas as pl
from jax.experimental.pallas import tpu as pltpu
from jax.sharding import PartitionSpec as P


pair_index = ((0, 1, 2), (1, 3, 4), (2, 4, 5))
sym_pairs = ((0, 0), (0, 1), (0, 2), (1, 1), (1, 2), (2, 2))
weno_eps = 1e-06
RING = ("star", "blk")
LANES = 128
METRIC = 18
EARLY = 5
LATE = 13
LAST = 3
PLANE = 2 * (LATE - LAST) - 2
FLUID = 7
EARLY_LAYERS = 2 * EARLY + 3 * FLUID + 2
SPARE = EARLY_LAYERS - 2
HBM = pl.BlockSpec(memory_space=pltpu.HBM)
GRANT = 24 * 1024 * 1024
VMEM = pl.BlockSpec(memory_space=pltpu.VMEM)
F32 = jnp.float32


class Copies:
    def __init__(self, sems):
        self.sems = sems
        self.count = 0
        self.groups = {}

    def start(self, group, src, dst):
        copy = pltpu.make_async_copy(src, dst, self.sems.at[self.count])
        copy.start()
        self.count += 1
        self.groups.setdefault(group, []).append(copy)

    def wait(self, group):
        for copy in self.groups.pop(group):
            copy.wait()

    def wait_all(self):
        for group in list(self.groups):
            self.wait(group)


def slow_side():
    return lax.rem(lax.axis_index(RING[-1]), 2)


def coarse_rows(ny):
    first, count = ny // 4 - 1, ny // 2 + 2
    parts = []
    for n in range(3):
        done = 0
        while done < count:
            at = n * count + done
            step = min(count - done, ny - at % ny)
            parts.append((n, first + done, step, at // ny, at % ny))
            done += step
    return parts


def send_early(copies, group, side, lapse, conf, shift, dens, mom, ener, velo, pres, buf):
    layer = lapse.shape[1:]
    rows = pl.ds(side * (lapse.shape[0] - 2), 2)
    copies.start(group, lapse.at[rows], buf.at[pl.ds(0, 2)])
    copies.start(group, conf.at[rows], buf.at[pl.ds(2, 2)])
    copies.start(group, shift.at[:, rows], buf.at[pl.ds(4, 6)].reshape(3, 2, *layer))
    rows = pl.ds(side * (dens.shape[1] - 3), 3)
    at = 2 * EARLY
    copies.start(group, dens.at[0, rows], buf.at[pl.ds(at, 3)])
    copies.start(group, mom.at[0, :, rows], buf.at[pl.ds(at + 3, 9)].reshape(3, 3, *layer))
    copies.start(group, ener.at[0, rows], buf.at[pl.ds(at + 12, 3)])
    copies.start(group, velo.at[0, 0, rows], buf.at[pl.ds(at + 15, 3)])
    copies.start(group, pres.at[0, rows], buf.at[pl.ds(at + 18, 3)])


def send_late(copies, group, side, mean, metric, curv, buf, at):
    layer = mean.shape[1:]
    rows = pl.ds(side * (mean.shape[0] - 2), 2)
    copies.start(group, metric.at[:, rows], buf.at[pl.ds(at, 12)].reshape(6, 2, *layer))
    copies.start(group, curv.at[:, rows], buf.at[pl.ds(at + 12, 12)].reshape(6, 2, *layer))
    copies.start(group, mean.at[rows], buf.at[pl.ds(at + 24, 2)])


def fill_spare(up, third, mean, buf):
    @pl.when(up)
    def _():
        for k in range(2):
            buf[SPARE + k] = mean(k)

    @pl.when(jnp.logical_not(up))
    def _():
        for n, row, count, layer, at in coarse_rows(buf.shape[1]):
            buf[SPARE + layer, pl.ds(at, count), :] = third(n, pl.ds(row, count))


def pack_kernel(lapse, conf, shift, mean, dens, mom, ener, velo, pres, buf, third, high, sems):
    copies = Copies(sems)
    side = slow_side()
    copies.start("s", lapse.at[2], third.at[0])
    copies.start("s", conf.at[2], third.at[1])
    copies.start("s", shift.at[0, 2], third.at[2])
    copies.start("s", mean.at[pl.ds(mean.shape[0] - 2, 2)], high)
    send_early(copies, 0, side, lapse, conf, shift, dens, mom, ener, velo, pres, buf)
    buf[EARLY_LAYERS - 1] = jnp.zeros(buf.shape[1:], F32)
    copies.wait("s")
    fill_spare(side == 1, lambda n, sl: third[n, sl, :], lambda k: high[k], buf)
    copies.wait_all()


def bssn_layer(state, source, out, at, out_at):
    ny, nz = state.shape[-2:]

    def value(field, off=0):
        return state[field, at + off]

    def rolled(v, axis):
        n = (ny, nz)[axis]
        return tuple(pltpu.roll(v, s % n, axis) for s in (2, 1, -1, -2))

    def first(taps):
        m2, m1, p1, p2 = taps
        return (m2 - p2) + 8.0 * (p1 - m1)

    def second(taps, mid):
        m2, m1, p1, p2 = taps
        return 16.0 * (m1 + p1) - (m2 + p2) - 30.0 * mid

    def xtaps(field):
        return tuple(value(field, o) for o in (-2, -1, 1, 2))

    twelfth = 1.0 / 12.0
    third = 1.0 / 3.0
    lapse = value(0)
    conf = value(1)
    mean = value(2)
    shift12 = [value(15 + n) * twelfth for n in range(3)]

    def gradient(field):
        v = value(field)
        return first(xtaps(field)), first(rolled(v, 0)), first(rolled(v, 1))

    def along_shift(field):
        gx, gy, gz = gradient(field)
        return shift12[0] * gx + shift12[1] * gy + shift12[2] * gz

    dshift = [[None] * 3 for _ in range(3)]
    for n in range(3):
        for k, g in enumerate(gradient(15 + n)):
            dshift[k][n] = g * twelfth
    div_shift = dshift[0][0] + dshift[1][1] + dshift[2][2]
    div23 = (2.0 / 3.0) * div_shift

    taps_x = xtaps(0)
    taps_y = rolled(lapse, 0)
    taps_z = rolled(lapse, 1)
    lx, ly, lz = first(taps_x), first(taps_y), first(taps_z)
    out[0, out_at] = (shift12[0] * lx + shift12[1] * ly + shift12[2] * lz) - 2.0 * lapse * mean
    sq = twelfth * twelfth
    hess = (
        second(taps_x, lapse) * twelfth,
        first(rolled(lx, 0)) * sq,
        first(rolled(lx, 1)) * sq,
        second(taps_y, lapse) * twelfth,
        first(rolled(lz, 0)) * sq,
        second(taps_z, lapse) * twelfth,
    )
    out[1, out_at] = along_shift(1) + conf * ((2.0 / 3.0) * (lapse * mean) - div23)

    a, b, c, d, e, f = g = [value(3 + n) for n in range(6)]
    cof = (d * f - e * e, c * e - b * f, b * e - c * d, a * f - c * c, b * c - a * e, a * d - b * b)
    scale = 1.0 / (a * cof[0] + b * cof[1] + c * cof[2])
    inv = [entry * scale for entry in cof]
    trace = (inv[0] * hess[0] + inv[3] * hess[3] + inv[5] * hess[5]) + 2.0 * (
        inv[1] * hess[1] + inv[2] * hess[2] + inv[4] * hess[4]
    )
    trace3 = trace * third
    curv = [value(9 + n) for n in range(6)]

    def pick(six, i, j):
        return six[pair_index[i][j]]

    def total(terms):
        return functools.reduce(lambda x, y: x + y, terms)

    mixed = [
        [total([pick(curv, i, l) * pick(inv, l, j) for l in range(3)]) for j in range(3)]
        for i in range(3)
    ]
    square = (mixed[0][0] * mixed[0][0] + mixed[1][1] * mixed[1][1] + mixed[2][2] * mixed[2][2]) + 2.0 * (
        mixed[0][1] * mixed[1][0] + mixed[0][2] * mixed[2][0] + mixed[1][2] * mixed[2][1]
    )
    out[2, out_at] = (
        along_shift(2)
        - conf * trace
        + lapse * (square + mean * mean * third + (4.0 * math.pi) * source)
    )
    lapse2 = 2.0 * lapse
    mean_lapse = lapse * mean

    def stretched(six, i, j):
        if i == j:
            return 2.0 * total([pick(six, i, k) * dshift[i][k] for k in range(3)])
        return total([pick(six, i, k) * dshift[j][k] + pick(six, j, k) * dshift[i][k] for k in range(3)])

    for p, (i, j) in enumerate(sym_pairs):
        product = total([mixed[i][k] * pick(curv, k, j) for k in range(3)])
        out[9 + p, out_at] = (
            along_shift(9 + p)
            + (mean_lapse - div23) * curv[p]
            - lapse2 * product
            + stretched(curv, i, j)
            - conf * (hess[p] - trace3 * g[p])
        )
    for p, (i, j) in enumerate(sym_pairs):
        out[3 + p, out_at] = along_shift(3 + p) - lapse2 * curv[p] + stretched(g, i, j) - div23 * g[p]


def lane_matrix(nz, weights):
    row = lax.broadcasted_iota(jnp.int32, (nz, nz), 0)
    col = lax.broadcasted_iota(jnp.int32, (nz, nz), 1)
    return weights(row, col)


def dot(x, y):
    return jnp.dot(x, y, precision=lax.Precision.HIGHEST, preferred_element_type=F32)


def restrict_planes(pairs, rows, outs):
    ny, nz = outs[0][0].shape[-2:]
    half = ny // 2
    quarter_y, quarter_z = ny // 4, nz // 4
    count = len(pairs)
    for n, plane in enumerate(pairs):
        for h in range(nz // LANES):
            rows[h, pl.ds(n * ny, ny), :] = plane()[:, h * LANES : (h + 1) * LANES]
    halves = [
        rows[h, pl.ds(0, count * half, stride=2), :] + rows[h, pl.ds(1, count * half, stride=2), :]
        for h in range(nz // LANES)
    ]
    matrix = lane_matrix(
        nz, lambda r, c: jnp.where(c == quarter_z + lax.shift_right_logical(r, 1), 0.125, 0.0).astype(F32)
    )
    level = dot(jnp.concatenate(halves, axis=1), matrix)
    for n, (out, at) in enumerate(outs):
        out[at] = jnp.zeros((ny, nz), F32)
        out[at, pl.ds(quarter_y, half), :] = level[n * half : (n + 1) * half]


def prolong_yz(planes, rows, out):
    ny, nz = out.shape[-2:]
    half = ny // 2
    start_y, start_z = ny // 4, nz // 4
    flat = [plane for field in planes for plane in field]
    for n, plane in enumerate(flat):
        mid = 0.75 * plane(pl.ds(start_y, half))
        even = mid + 0.25 * plane(pl.ds(start_y - 1, half))
        odd = mid + 0.25 * plane(pl.ds(start_y + 1, half))
        for h in range(nz // LANES):
            lanes = slice(h * LANES, (h + 1) * LANES)
            rows[h, pl.ds(n * ny, half, stride=2), :] = even[:, lanes]
            rows[h, pl.ds(n * ny + 1, half, stride=2), :] = odd[:, lanes]

    def weights(r, c):
        mid = start_z + lax.shift_right_logical(c, 1)
        side = mid - 1 + 2 * (c & 1)
        return jnp.where(r == mid, 0.75, jnp.where(r == side, 0.25, 0.0)).astype(F32)

    matrix = lane_matrix(nz, weights)
    wide = jnp.concatenate([rows[h, pl.ds(0, len(flat) * ny), :] for h in range(nz // LANES)], axis=1)
    fine = dot(wide, matrix)
    at = 0
    for field, layers in enumerate(planes):
        for n in range(len(layers)):
            out[field, n] = fine[at * ny : (at + 1) * ny]
            at += 1


def split_flux(fluid, lapse, shift, conf, out, out_at):
    root = lax.rsqrt(conf)
    transport = lapse * fluid(5) - shift
    weight = lapse * (root * root * root) * fluid(6)
    speed = lapse + jnp.abs(shift)
    for n in range(5):
        u = fluid(n)
        flux = u * transport
        if n == 1:
            flux = flux + weight
        if n == 4:
            flux = flux + weight * fluid(5)
        moved = speed * u
        plus, minus = flux + moved, flux - moved
        out[n, out_at] = plus
        out[5 + n, out_at] = minus


def weno_cells(flux, field, rows, base, count, emit):
    def differences(which, low, high):
        v = {j: flux[which, base + j, rows, :] for j in range(low, high + 1)}
        e = {j: v[j + 1] - v[j] for j in range(low, high)}
        d = {j: e[j] - e[j - 1] for j in range(low + 1, high)}
        t = {j: d[j + 1] - d[j] for j in range(low + 1, high - 1)}
        h = {j: 0.5 * d[j] for j in d}
        s = {j: (13.0 / 12.0) * (d[j] * d[j]) + 4.0 * weno_eps for j in d}
        return v, e, d, t, h, s

    faces = range(-1, count)
    v, e, _, t, h, s = differences(field, -3, count + 1)
    u, eu, _, tu, hu, su = differences(5 + field, -2, count + 2)

    def quotient(b0, b1, b2, t0, t2):
        w0, w1, w2 = b1 * b2, b0 * b2, b0 * b1
        w0, w1, w2 = w0 * w0, 6.0 * (w1 * w1), w2 * w2
        return (w0 * t0 + 1.5 * (w2 * t2)) / (w0 + w1 + 3.0 * w2)

    def square(x):
        return x * x

    previous = None
    for i in faces:
        left = quotient(
            s[i - 1] + square(h[i - 1] + e[i - 1]),
            s[i] + square(h[i] + e[i - 1]),
            s[i + 1] + square(h[i + 1] - e[i]),
            t[i - 1],
            t[i],
        )
        right = quotient(
            su[i + 2] + square(hu[i + 2] - eu[i + 1]),
            su[i + 1] + square(hu[i + 1] - eu[i + 1]),
            su[i] + square(hu[i] + eu[i]),
            tu[i + 1],
            tu[i],
        )
        face = (
            3.0 * (v[i] + u[i + 1])
            + 0.5 * (e[i - 1] - eu[i + 1])
            + (e[i] - eu[i])
            + (right - left)
        )
        if previous is not None:
            emit(i, (previous - face) * (1.0 / 3.0))
        previous = face


def local_kernel(
    packed, lapse, conf, mean, metric, curv, shift, dens, mom, ener, velo, pres,
    state, flux, sources, fluid, fast, late, last,
    coarse, rows, sems,
):
    nx, ny, nz = lapse.shape
    fx = dens.shape[1]
    copies = Copies(sems)
    inner = pl.ds(2, nx)
    copies.start("c", lapse, state.at[0, inner])
    copies.start("c", conf, state.at[1, inner])
    copies.start("c", shift, state.at[pl.ds(15, 3), inner])
    copies.start("f", dens.at[0], fluid.at[0])
    copies.start("f", mom.at[0], fluid.at[pl.ds(1, 3)])
    copies.start("f", ener.at[0], fluid.at[4])
    copies.start("f", velo.at[0, 0], fluid.at[5])
    copies.start("f", pres.at[0], fluid.at[6])
    copies.start("f", velo.at[0, pl.ds(1, 2)], fluid.at[pl.ds(7, 2)])
    side = slow_side()
    layer = (ny, nz)
    edge = pl.ds(side * (nx - 2), 2)
    copies.start("o", metric.at[pl.ds(LAST, 3), edge], late.at[pl.ds(0, 6)].reshape(3, 2, *layer))
    copies.start("o", curv.at[:, edge], late.at[pl.ds(6, 12)].reshape(6, 2, *layer))
    copies.start("o", mean.at[edge], late.at[pl.ds(18, 2)])
    copies.start("o", metric.at[pl.ds(0, LAST), edge], last.at[...].reshape(LAST, 2, *layer))
    send_early(copies, "o", 1 - side, lapse, conf, shift, dens, mom, ener, velo, pres, fast)
    send_late(copies, "o", 1 - side, mean, metric, curv, fast, EARLY_LAYERS)
    copies.start("o", mean, state.at[2, inner])
    copies.start("o", metric, state.at[pl.ds(3, 6), inner])
    copies.start("o", curv, state.at[pl.ds(9, 6), inner])

    @pl.loop(2, 15)
    def _(n):
        for k in (0, 1, nx + 2, nx + 3):
            state[n, k] = jnp.zeros((ny, nz), F32)

    copies.wait("c")

    def coarse_plane(field, layer):
        return lambda sl: state[field, layer + 2, sl, :]

    prolong_yz([[coarse_plane(f, l) for l in range(nx)] for f in (0, 15, 1)], rows, coarse)
    copies.wait("f")

    @pl.loop(0, fx - 3)
    def _(i):
        mid = lax.shift_right_logical(i, 1) + 1
        side = mid - 1 + 2 * (i & 1)
        parts = [0.75 * coarse[n, mid] + 0.25 * coarse[n, side] for n in range(3)]
        split_flux(lambda n: fluid[n, i], *parts, flux, i + 3)

    def pair(layer):
        def one(x):
            return (
                fluid[4, x]
                + fluid[0, x]
                + (fluid[1, x] * fluid[5, x] + fluid[2, x] * fluid[7, x] + fluid[3, x] * fluid[8, x])
                + 3.0 * fluid[6, x]
            )

        return lambda: one(2 * layer) + one(2 * layer + 1)

    plane = EARLY_LAYERS + 2 * LATE
    restrict_planes(
        [pair(l) for l in range(nx)],
        rows,
        [(sources, l + 1) for l in range(nx - 1)] + [(fast, plane)],
    )
    sources[0] = jnp.zeros((ny, nz), F32)
    for k in range(2):
        fast[SPARE + k] = jnp.zeros((ny, nz), F32)
    for n, row, count, layer, at in coarse_rows(ny):
        fast[SPARE + layer, pl.ds(at, count), :] = state[(0, 1, 15)[n], 4, pl.ds(row, count), :]
    copies.wait_all()

    @pl.when(slow_side() == 1)
    def _():
        late[PLANE] = fast[plane]


def inner_kernel(state, flux, sources, rates, hydro, stage, hstage, sems):
    nx, ny, _ = sources.shape
    fx = hydro.shape[2]
    copies = Copies(sems)

    @pl.loop(0, 5)
    def _(n):
        for part in range(ny // 8):
            sl = pl.ds(part * 8, 8)

            def emit(i, value):
                hstage[n, i, sl, :] = value

            weno_cells(flux, n, sl, 9, fx - 12, emit)

    copies.start("o", hstage, hydro.at[0, :, pl.ds(6, fx - 12)])

    @pl.loop(0, nx - 4)
    def _(l):
        bssn_layer(state, sources[l + 2], stage, l + 4, l)

    copies.start("o", stage, rates.at[:, pl.ds(2, nx - 4)])
    copies.wait_all()


def side_work(copies, side, recv, complete, state, flux, sources, fluid, hydro, stage, six, coarse, rows, hstage):
    nx = sources.shape[0]
    ny, _ = sources.shape[-2:]
    fx = fluid.shape[1]
    halo = side * (nx + 2)
    for k in range(2):
        for n, field in enumerate((0, 1, 15, 16, 17)):
            state[field, halo + k] = recv[2 * n + k]
    for n, row, count, layer, at in coarse_rows(ny):
        state[(0, 1, 15)[n], nx + 4, pl.ds(row, count), :] = recv[SPARE + layer, pl.ds(at, count), :]
    if complete:

        @pl.loop(0, LATE)
        def _(n):
            for k in range(2):
                field = jnp.where(n == LATE - 1, 2, n + 3)
                state[field, halo + k] = recv[EARLY_LAYERS + 2 * n + k]

    place = lax.axis_index(RING[-1])
    outer = jnp.where(side == 0, place == 0, place == lax.axis_size(RING[-1]) - 1)
    inside = jnp.where(outer, 0.0, 1.0).astype(F32)
    for n in range(FLUID):
        for k in range(3):
            value = recv[2 * EARLY + 3 * n + k]
            six[n, 3 * side + k] = value if n == 5 else value * inside
            six[n, 3 - 3 * side + k] = fluid[n, side * (fx - 3) + k]

    def coarse_plane(field, layer):
        return lambda sl: state[field, side * nx + 1 + layer, sl, :]

    prolong_yz([[coarse_plane(f, l) for l in range(4)] for f in (0, 15, 1)], rows, coarse)

    @pl.loop(0, 6)
    def _(j):
        mid = lax.shift_right_logical(j + 1, 1)
        other = mid + 1 - 2 * (j & 1)
        parts = [0.75 * coarse[n, mid] + 0.25 * coarse[n, other] for n in range(3)]
        split_flux(lambda n: six[n, j], *parts, flux, side * fx + j)

    first = side * (fx - 6)

    @pl.loop(0, 5)
    def _(n):
        for part in range(ny // 8):
            sl = pl.ds(part * 8, 8)

            def emit(i, value):
                hstage[n, i, sl, :] = value

            weno_cells(flux, n, sl, first + 3, 6, emit)

    copies.start("o", hstage, hydro.at[0, :, pl.ds(first, 6)])

    @pl.loop(0, 2)
    def _(k):
        l = side * (nx - 2) + k
        source = sources[l]
        if complete:
            source = source + jnp.where(l == 0, 1.0, 0.0).astype(F32) * recv[EARLY_LAYERS + 2 * LATE]
        bssn_layer(state, source, stage, l + 2, k)


def fast_kernel(
    recv, rates_in, hydro_in, state_in, flux_in, sources, fluid,
    rates, hydro, state, flux,
    stage, six, coarse, rows, hstage, sems,
):
    copies = Copies(sems)
    side = 1 - slow_side()
    side_work(copies, side, recv, True, state, flux, sources, fluid, hydro, stage, six, coarse, rows, hstage)
    copies.start("o", stage, rates.at[:, pl.ds(side * (rates.shape[1] - 2), 2)])
    copies.wait_all()


def slow_kernel(
    recv, hydro_in, state_in, flux_in, sources, fluid,
    hydro, state, flux, stage,
    six, coarse, rows, hstage, sems,
):
    copies = Copies(sems)
    side_work(copies, slow_side(), recv, False, state, flux, sources, fluid, hydro, stage, six, coarse, rows, hstage)
    copies.wait_all()


def late_rates(copies, groups, tap, extra, stage_in, state, rates, stage):
    nx = rates.shape[1]
    side = slow_side()
    low = side == 0

    def pick(below, above):
        return jnp.where(low, below, above).astype(F32)

    taps = ((pick(1.0, -1.0), pick(-8.0, 0.0)), (pick(0.0, 8.0), pick(1.0, -1.0)))
    first = side * (nx - 2)
    layers = pl.ds(first, 2)
    steps = [state[15, first + 2 + k] * (1.0 / 12.0) for k in range(2)]
    for begin, end in groups:
        for field in range(begin, end):
            values = [tap(low, field, n) for n in range(2)]
            for k in range(2):
                value = stage_in[field, k] + steps[k] * (taps[k][0] * values[0] + taps[k][1] * values[1])
                if field == 2 and k == 0:
                    value = value + pick(4.0 * math.pi, 0.0) * extra()
                stage[field, k] = value
        group = pl.ds(begin, end - begin)
        copies.start("o", stage.at[group], rates.at[group, layers])


def late_kernel(recv, early, stage_in, state, rates_in, rates, stage, sems):
    copies = Copies(sems)
    layers = pl.ds(slow_side() * (rates.shape[1] - 2), 2)
    copies.start("o", stage_in.at[pl.ds(0, 2)], rates.at[pl.ds(0, 2), layers])

    def tap(low, field, n):
        if field == 2:
            return jnp.where(low, early[SPARE + n], recv[PLANE + n])
        return recv[2 * (field - 3 - LAST) + n]

    groups = ((3 + LAST, 9), (9, 12), (12, 15), (2, 3))
    late_rates(copies, groups, tap, lambda: state[0, 2] * recv[PLANE], stage_in, state, rates, stage)
    copies.wait_all()


def last_kernel(recv, stage_in, state, rates_in, rates, stage, sems):
    copies = Copies(sems)
    groups = tuple((n, n + 1) for n in range(3, 3 + LAST))
    late_rates(copies, groups, lambda low, field, n: recv[2 * (field - 3) + n], None, stage_in, state, rates, stage)
    copies.wait_all()


def substep(*fields):
    fields = [pltpu.with_memory_space_constraint(field, pltpu.HBM) for field in fields]
    lapse, conf, mean, _, _, shift, dens, mom, ener, velo, pres = fields
    nx, ny, nz = lapse.shape
    fx = dens.shape[1]
    layer = (ny, nz)

    def shape(*leading):
        return jax.ShapeDtypeStruct(leading + layer, F32)

    def vmem(*leading):
        return pltpu.VMEM(leading + layer, F32)

    def row_scratch(planes):
        return pltpu.VMEM((nz // LANES, planes * ny, LANES), F32)

    def sems(n):
        return pltpu.SemaphoreType.DMA((n,))

    count = lax.axis_size(RING)
    fast_pairs = [(i, i ^ 1) for i in range(count)]
    slow_pairs = [(i, (i + (1 if i % 2 else -1)) % count) for i in range(count)]
    params = pltpu.CompilerParams(vmem_limit_bytes=GRANT)

    def cost(flops):
        return pl.CostEstimate(flops=flops, transcendentals=0, bytes_accessed=6_000_000)

    early = pl.pallas_call(
        pack_kernel,
        out_shape=shape(EARLY_LAYERS),
        in_specs=[HBM] * 9,
        out_specs=VMEM,
        scratch_shapes=[vmem(3), vmem(2), sems(16)],
        compiler_params=params,
        name="pack",
    )(lapse, conf, shift, mean, dens, mom, ener, velo, pres)
    packed = early
    early = lax.ppermute(early, RING, slow_pairs)
    local = pl.pallas_call(
        local_kernel,
        out_shape=(
            shape(METRIC, nx + 5),
            shape(10, fx + 6),
            shape(nx),
            shape(9, fx),
            shape(EARLY_LAYERS + 2 * LATE + 1),
            shape(2 * (LATE - LAST)),
            shape(2 * LAST),
        ),
        in_specs=[VMEM] + [HBM] * 11,
        out_specs=[VMEM] * 7,
        scratch_shapes=[vmem(3, nx), row_scratch(3 * nx), sems(40)],
        cost_estimate=cost(200_000_000),
        compiler_params=params,
        name="local",
    )
    state, flux, sources, fluid, fast, late, last = local(packed, *fields)
    fast = lax.ppermute(fast, RING, fast_pairs)
    late = lax.ppermute(late, RING, slow_pairs)
    last = lax.ppermute(last, RING, slow_pairs)
    rates, hydro = pl.pallas_call(
        inner_kernel,
        out_shape=(shape(15, nx), shape(1, 5, fx)),
        in_specs=[VMEM] * 3,
        out_specs=[HBM] * 2,
        scratch_shapes=[vmem(15, nx - 4), vmem(5, fx - 12), sems(4)],
        cost_estimate=cost(400_000_000),
        compiler_params=params,
        name="inner",
    )(state, flux, sources)
    work = [vmem(FLUID, 6), vmem(3, 4), row_scratch(12), vmem(5, 6), sems(4)]
    rates, hydro, state, flux = pl.pallas_call(
        fast_kernel,
        out_shape=(shape(15, nx), shape(1, 5, fx), shape(METRIC, nx + 5), shape(10, fx + 6)),
        in_specs=[VMEM] + [HBM] * 2 + [VMEM] * 4,
        out_specs=[HBM] * 2 + [VMEM] * 2,
        input_output_aliases={1: 0, 2: 1, 3: 2, 4: 3},
        scratch_shapes=[vmem(15, 2)] + work,
        cost_estimate=cost(300_000_000),
        compiler_params=params,
        name="fast",
    )(fast, rates, hydro, state, flux, sources, fluid)
    hydro, state, _, stage = pl.pallas_call(
        slow_kernel,
        out_shape=(shape(1, 5, fx), shape(METRIC, nx + 5), shape(10, fx + 6), shape(15, 2)),
        in_specs=[VMEM, HBM] + [VMEM] * 4,
        out_specs=[HBM] + [VMEM] * 3,
        input_output_aliases={1: 0, 2: 1, 3: 2},
        scratch_shapes=work,
        cost_estimate=cost(300_000_000),
        compiler_params=params,
        name="slow",
    )(early, hydro, state, flux, sources, fluid)
    late_call = pl.pallas_call(
        late_kernel,
        out_shape=shape(15, nx),
        in_specs=[VMEM] * 4 + [HBM],
        out_specs=HBM,
        input_output_aliases={4: 0},
        scratch_shapes=[vmem(15, 2), sems(8)],
        compiler_params=params,
        name="late",
    )
    rates = late_call(late, early, stage, state, rates)
    rates = pl.pallas_call(
        last_kernel,
        out_shape=shape(15, nx),
        in_specs=[VMEM] * 3 + [HBM],
        out_specs=HBM,
        input_output_aliases={3: 0},
        scratch_shapes=[vmem(15, 2), sems(8)],
        compiler_params=params,
        name="last",
    )(last, stage, state, rates)
    return rates, hydro


def solution(mesh):
    in_specs = (
        P(RING, None, None),
        P(RING, None, None),
        P(RING, None, None),
        P(None, RING, None, None),
        P(None, RING, None, None),
        P(None, RING, None, None),
        P("star", "blk", None, None),
        P("star", None, "blk", None, None),
        P("star", "blk", None, None),
        P("star", None, "blk", None, None),
        P("star", "blk", None, None),
    )
    out_specs = (P(None, RING, None, None), P("star", None, "blk", None, None))
    return jax.shard_map(substep, mesh=mesh, in_specs=in_specs, out_specs=out_specs, check_vma=False)
```

```python
import functools
import math

import jax
import jax.numpy as jnp
from jax import lax
from jax.experimental import pallas as pl
from jax.experimental.pallas import tpu as pltpu
from jax.sharding import PartitionSpec as P


pair_index = ((0, 1, 2), (1, 3, 4), (2, 4, 5))
sym_pairs = ((0, 0), (0, 1), (0, 2), (1, 1), (1, 2), (2, 2))
weno_eps = 1e-06
RING = ("star", "blk")
LANES = 128
METRIC = 18
EARLY = 5
LATE = 13
PLANE = 2 * LATE - 2
FLUID = 7
EARLY_LAYERS = 2 * EARLY + 3 * FLUID + 2
SPARE = EARLY_LAYERS - 2
HBM = pl.BlockSpec(memory_space=pltpu.HBM)
GRANT = 24 * 1024 * 1024
VMEM = pl.BlockSpec(memory_space=pltpu.VMEM)
F32 = jnp.float32


class Copies:
    def __init__(self, sems):
        self.sems = sems
        self.count = 0
        self.groups = {}

    def start(self, group, src, dst):
        copy = pltpu.make_async_copy(src, dst, self.sems.at[self.count])
        copy.start()
        self.count += 1
        self.groups.setdefault(group, []).append(copy)

    def wait(self, group):
        for copy in self.groups.pop(group):
            copy.wait()

    def wait_all(self):
        for group in list(self.groups):
            self.wait(group)


def slow_side():
    return lax.rem(lax.axis_index(RING[-1]), 2)


def coarse_rows(ny):
    first, count = ny // 4 - 1, ny // 2 + 2
    parts = []
    for n in range(3):
        done = 0
        while done < count:
            at = n * count + done
            step = min(count - done, ny - at % ny)
            parts.append((n, first + done, step, at // ny, at % ny))
            done += step
    return parts


def send_early(copies, group, side, lapse, conf, shift, dens, mom, ener, velo, pres, buf):
    layer = lapse.shape[1:]
    rows = pl.ds(side * (lapse.shape[0] - 2), 2)
    copies.start(group, lapse.at[rows], buf.at[pl.ds(0, 2)])
    copies.start(group, conf.at[rows], buf.at[pl.ds(2, 2)])
    copies.start(group, shift.at[:, rows], buf.at[pl.ds(4, 6)].reshape(3, 2, *layer))
    rows = pl.ds(side * (dens.shape[1] - 3), 3)
    at = 2 * EARLY
    copies.start(group, dens.at[0, rows], buf.at[pl.ds(at, 3)])
    copies.start(group, mom.at[0, :, rows], buf.at[pl.ds(at + 3, 9)].reshape(3, 3, *layer))
    copies.start(group, ener.at[0, rows], buf.at[pl.ds(at + 12, 3)])
    copies.start(group, velo.at[0, 0, rows], buf.at[pl.ds(at + 15, 3)])
    copies.start(group, pres.at[0, rows], buf.at[pl.ds(at + 18, 3)])


def send_late(copies, group, side, mean, metric, curv, buf, at):
    layer = mean.shape[1:]
    rows = pl.ds(side * (mean.shape[0] - 2), 2)
    copies.start(group, metric.at[:, rows], buf.at[pl.ds(at, 12)].reshape(6, 2, *layer))
    copies.start(group, curv.at[:, rows], buf.at[pl.ds(at + 12, 12)].reshape(6, 2, *layer))
    copies.start(group, mean.at[rows], buf.at[pl.ds(at + 24, 2)])


def fill_spare(up, third, mean, buf):
    @pl.when(up)
    def _():
        for k in range(2):
            buf[SPARE + k] = mean(k)

    @pl.when(jnp.logical_not(up))
    def _():
        for n, row, count, layer, at in coarse_rows(buf.shape[1]):
            buf[SPARE + layer, pl.ds(at, count), :] = third(n, pl.ds(row, count))


def pack_kernel(lapse, conf, shift, mean, dens, mom, ener, velo, pres, buf, third, high, sems):
    copies = Copies(sems)
    side = slow_side()
    copies.start("s", lapse.at[2], third.at[0])
    copies.start("s", conf.at[2], third.at[1])
    copies.start("s", shift.at[0, 2], third.at[2])
    copies.start("s", mean.at[pl.ds(mean.shape[0] - 2, 2)], high)
    send_early(copies, 0, side, lapse, conf, shift, dens, mom, ener, velo, pres, buf)
    buf[EARLY_LAYERS - 1] = jnp.zeros(buf.shape[1:], F32)
    copies.wait("s")
    fill_spare(side == 1, lambda n, sl: third[n, sl, :], lambda k: high[k], buf)
    copies.wait_all()


def bssn_layer(state, source, out, at, out_at):
    ny, nz = state.shape[-2:]

    def value(field, off=0):
        return state[field, at + off]

    def rolled(v, axis):
        n = (ny, nz)[axis]
        return tuple(pltpu.roll(v, s % n, axis) for s in (2, 1, -1, -2))

    def first(taps):
        m2, m1, p1, p2 = taps
        return (m2 - p2) + 8.0 * (p1 - m1)

    def second(taps, mid):
        m2, m1, p1, p2 = taps
        return 16.0 * (m1 + p1) - (m2 + p2) - 30.0 * mid

    def xtaps(field):
        return tuple(value(field, o) for o in (-2, -1, 1, 2))

    twelfth = 1.0 / 12.0
    third = 1.0 / 3.0
    lapse = value(0)
    conf = value(1)
    mean = value(2)
    shift12 = [value(15 + n) * twelfth for n in range(3)]

    def gradient(field):
        v = value(field)
        return first(xtaps(field)), first(rolled(v, 0)), first(rolled(v, 1))

    def along_shift(field):
        gx, gy, gz = gradient(field)
        return shift12[0] * gx + shift12[1] * gy + shift12[2] * gz

    dshift = [[None] * 3 for _ in range(3)]
    for n in range(3):
        for k, g in enumerate(gradient(15 + n)):
            dshift[k][n] = g * twelfth
    div_shift = dshift[0][0] + dshift[1][1] + dshift[2][2]
    div23 = (2.0 / 3.0) * div_shift

    taps_x = xtaps(0)
    taps_y = rolled(lapse, 0)
    taps_z = rolled(lapse, 1)
    lx, ly, lz = first(taps_x), first(taps_y), first(taps_z)
    out[0, out_at] = (shift12[0] * lx + shift12[1] * ly + shift12[2] * lz) - 2.0 * lapse * mean
    sq = twelfth * twelfth
    hess = (
        second(taps_x, lapse) * twelfth,
        first(rolled(lx, 0)) * sq,
        first(rolled(lx, 1)) * sq,
        second(taps_y, lapse) * twelfth,
        first(rolled(lz, 0)) * sq,
        second(taps_z, lapse) * twelfth,
    )
    out[1, out_at] = along_shift(1) + conf * ((2.0 / 3.0) * (lapse * mean) - div23)

    a, b, c, d, e, f = g = [value(3 + n) for n in range(6)]
    cof = (d * f - e * e, c * e - b * f, b * e - c * d, a * f - c * c, b * c - a * e, a * d - b * b)
    scale = 1.0 / (a * cof[0] + b * cof[1] + c * cof[2])
    inv = [entry * scale for entry in cof]
    trace = (inv[0] * hess[0] + inv[3] * hess[3] + inv[5] * hess[5]) + 2.0 * (
        inv[1] * hess[1] + inv[2] * hess[2] + inv[4] * hess[4]
    )
    trace3 = trace * third
    curv = [value(9 + n) for n in range(6)]

    def pick(six, i, j):
        return six[pair_index[i][j]]

    def total(terms):
        return functools.reduce(lambda x, y: x + y, terms)

    mixed = [
        [total([pick(curv, i, l) * pick(inv, l, j) for l in range(3)]) for j in range(3)]
        for i in range(3)
    ]
    square = (mixed[0][0] * mixed[0][0] + mixed[1][1] * mixed[1][1] + mixed[2][2] * mixed[2][2]) + 2.0 * (
        mixed[0][1] * mixed[1][0] + mixed[0][2] * mixed[2][0] + mixed[1][2] * mixed[2][1]
    )
    out[2, out_at] = (
        along_shift(2)
        - conf * trace
        + lapse * (square + mean * mean * third + (4.0 * math.pi) * source)
    )
    lapse2 = 2.0 * lapse
    mean_lapse = lapse * mean

    def stretched(six, i, j):
        if i == j:
            return 2.0 * total([pick(six, i, k) * dshift[i][k] for k in range(3)])
        return total([pick(six, i, k) * dshift[j][k] + pick(six, j, k) * dshift[i][k] for k in range(3)])

    for p, (i, j) in enumerate(sym_pairs):
        product = total([mixed[i][k] * pick(curv, k, j) for k in range(3)])
        out[9 + p, out_at] = (
            along_shift(9 + p)
            + (mean_lapse - div23) * curv[p]
            - lapse2 * product
            + stretched(curv, i, j)
            - conf * (hess[p] - trace3 * g[p])
        )
    for p, (i, j) in enumerate(sym_pairs):
        out[3 + p, out_at] = along_shift(3 + p) - lapse2 * curv[p] + stretched(g, i, j) - div23 * g[p]


def lane_matrix(nz, weights):
    row = lax.broadcasted_iota(jnp.int32, (nz, nz), 0)
    col = lax.broadcasted_iota(jnp.int32, (nz, nz), 1)
    return weights(row, col)


def dot(x, y):
    return jnp.dot(x, y, precision=lax.Precision.HIGHEST, preferred_element_type=F32)


def restrict_planes(pairs, rows, outs):
    ny, nz = outs[0][0].shape[-2:]
    half = ny // 2
    quarter_y, quarter_z = ny // 4, nz // 4
    count = len(pairs)
    for n, plane in enumerate(pairs):
        for h in range(nz // LANES):
            rows[h, pl.ds(n * ny, ny), :] = plane()[:, h * LANES : (h + 1) * LANES]
    halves = [
        rows[h, pl.ds(0, count * half, stride=2), :] + rows[h, pl.ds(1, count * half, stride=2), :]
        for h in range(nz // LANES)
    ]
    matrix = lane_matrix(
        nz, lambda r, c: jnp.where(c == quarter_z + lax.shift_right_logical(r, 1), 0.125, 0.0).astype(F32)
    )
    level = dot(jnp.concatenate(halves, axis=1), matrix)
    for n, (out, at) in enumerate(outs):
        out[at] = jnp.zeros((ny, nz), F32)
        out[at, pl.ds(quarter_y, half), :] = level[n * half : (n + 1) * half]


def prolong_yz(planes, rows, out):
    ny, nz = out.shape[-2:]
    half = ny // 2
    start_y, start_z = ny // 4, nz // 4
    flat = [plane for field in planes for plane in field]
    for n, plane in enumerate(flat):
        mid = 0.75 * plane(pl.ds(start_y, half))
        even = mid + 0.25 * plane(pl.ds(start_y - 1, half))
        odd = mid + 0.25 * plane(pl.ds(start_y + 1, half))
        for h in range(nz // LANES):
            lanes = slice(h * LANES, (h + 1) * LANES)
            rows[h, pl.ds(n * ny, half, stride=2), :] = even[:, lanes]
            rows[h, pl.ds(n * ny + 1, half, stride=2), :] = odd[:, lanes]

    def weights(r, c):
        mid = start_z + lax.shift_right_logical(c, 1)
        side = mid - 1 + 2 * (c & 1)
        return jnp.where(r == mid, 0.75, jnp.where(r == side, 0.25, 0.0)).astype(F32)

    matrix = lane_matrix(nz, weights)
    wide = jnp.concatenate([rows[h, pl.ds(0, len(flat) * ny), :] for h in range(nz // LANES)], axis=1)
    fine = dot(wide, matrix)
    at = 0
    for field, layers in enumerate(planes):
        for n in range(len(layers)):
            out[field, n] = fine[at * ny : (at + 1) * ny]
            at += 1


def split_flux(fluid, lapse, shift, conf, out, out_at):
    root = lax.rsqrt(conf)
    transport = lapse * fluid(5) - shift
    weight = lapse * (root * root * root) * fluid(6)
    speed = lapse + jnp.abs(shift)
    for n in range(5):
        u = fluid(n)
        flux = u * transport
        if n == 1:
            flux = flux + weight
        if n == 4:
            flux = flux + weight * fluid(5)
        moved = speed * u
        plus, minus = flux + moved, flux - moved
        out[n, out_at] = plus
        out[5 + n, out_at] = minus


def weno_cells(flux, field, rows, base, count, emit):
    def differences(which, low, high):
        v = {j: flux[which, base + j, rows, :] for j in range(low, high + 1)}
        e = {j: v[j + 1] - v[j] for j in range(low, high)}
        d = {j: e[j] - e[j - 1] for j in range(low + 1, high)}
        t = {j: d[j + 1] - d[j] for j in range(low + 1, high - 1)}
        h = {j: 0.5 * d[j] for j in d}
        s = {j: (13.0 / 12.0) * (d[j] * d[j]) + 4.0 * weno_eps for j in d}
        return v, e, d, t, h, s

    faces = range(-1, count)
    v, e, _, t, h, s = differences(field, -3, count + 1)
    u, eu, _, tu, hu, su = differences(5 + field, -2, count + 2)

    def quotient(b0, b1, b2, t0, t2):
        w0, w1, w2 = b1 * b2, b0 * b2, b0 * b1
        w0, w1, w2 = w0 * w0, 6.0 * (w1 * w1), w2 * w2
        return (w0 * t0 + 1.5 * (w2 * t2)) / (w0 + w1 + 3.0 * w2)

    def square(x):
        return x * x

    previous = None
    for i in faces:
        left = quotient(
            s[i - 1] + square(h[i - 1] + e[i - 1]),
            s[i] + square(h[i] + e[i - 1]),
            s[i + 1] + square(h[i + 1] - e[i]),
            t[i - 1],
            t[i],
        )
        right = quotient(
            su[i + 2] + square(hu[i + 2] - eu[i + 1]),
            su[i + 1] + square(hu[i + 1] - eu[i + 1]),
            su[i] + square(hu[i] + eu[i]),
            tu[i + 1],
            tu[i],
        )
        face = (
            3.0 * (v[i] + u[i + 1])
            + 0.5 * (e[i - 1] - eu[i + 1])
            + (e[i] - eu[i])
            + (right - left)
        )
        if previous is not None:
            emit(i, (previous - face) * (1.0 / 3.0))
        previous = face


def local_kernel(
    packed, lapse, conf, mean, metric, curv, shift, dens, mom, ener, velo, pres,
    state, flux, sources, fluid, fast, late,
    coarse, rows, sems,
):
    nx, ny, nz = lapse.shape
    fx = dens.shape[1]
    copies = Copies(sems)
    inner = pl.ds(2, nx)
    copies.start("c", lapse, state.at[0, inner])
    copies.start("c", conf, state.at[1, inner])
    copies.start("c", shift, state.at[pl.ds(15, 3), inner])
    copies.start("f", dens.at[0], fluid.at[0])
    copies.start("f", mom.at[0], fluid.at[pl.ds(1, 3)])
    copies.start("f", ener.at[0], fluid.at[4])
    copies.start("f", velo.at[0, 0], fluid.at[5])
    copies.start("f", pres.at[0], fluid.at[6])
    copies.start("f", velo.at[0, pl.ds(1, 2)], fluid.at[pl.ds(7, 2)])
    side = slow_side()
    send_late(copies, "o", side, mean, metric, curv, late, 0)
    send_early(copies, "o", 1 - side, lapse, conf, shift, dens, mom, ener, velo, pres, fast)
    send_late(copies, "o", 1 - side, mean, metric, curv, fast, EARLY_LAYERS)
    copies.start("o", mean, state.at[2, inner])
    copies.start("o", metric, state.at[pl.ds(3, 6), inner])
    copies.start("o", curv, state.at[pl.ds(9, 6), inner])

    @pl.loop(2, 15)
    def _(n):
        for k in (0, 1, nx + 2, nx + 3):
            state[n, k] = jnp.zeros((ny, nz), F32)

    copies.wait("c")

    def coarse_plane(field, layer):
        return lambda sl: state[field, layer + 2, sl, :]

    prolong_yz([[coarse_plane(f, l) for l in range(nx)] for f in (0, 15, 1)], rows, coarse)
    copies.wait("f")

    @pl.loop(0, fx - 3)
    def _(i):
        mid = lax.shift_right_logical(i, 1) + 1
        side = mid - 1 + 2 * (i & 1)
        parts = [0.75 * coarse[n, mid] + 0.25 * coarse[n, side] for n in range(3)]
        split_flux(lambda n: fluid[n, i], *parts, flux, i + 3)

    def pair(layer):
        def one(x):
            return (
                fluid[4, x]
                + fluid[0, x]
                + (fluid[1, x] * fluid[5, x] + fluid[2, x] * fluid[7, x] + fluid[3, x] * fluid[8, x])
                + 3.0 * fluid[6, x]
            )

        return lambda: one(2 * layer) + one(2 * layer + 1)

    plane = EARLY_LAYERS + 2 * LATE
    restrict_planes(
        [pair(l) for l in range(nx)],
        rows,
        [(sources, l + 1) for l in range(nx - 1)] + [(fast, plane)],
    )
    sources[0] = jnp.zeros((ny, nz), F32)
    for k in range(2):
        fast[SPARE + k] = jnp.zeros((ny, nz), F32)
    for n, row, count, layer, at in coarse_rows(ny):
        fast[SPARE + layer, pl.ds(at, count), :] = state[(0, 1, 15)[n], 4, pl.ds(row, count), :]
    copies.wait_all()

    @pl.when(slow_side() == 1)
    def _():
        late[PLANE] = fast[plane]


def inner_kernel(state, flux, sources, rates, hydro, stage, hstage, sems):
    nx, ny, _ = sources.shape
    fx = hydro.shape[2]
    copies = Copies(sems)

    @pl.loop(0, 5)
    def _(n):
        for part in range(ny // 8):
            sl = pl.ds(part * 8, 8)

            def emit(i, value):
                hstage[n, i, sl, :] = value

            weno_cells(flux, n, sl, 9, fx - 12, emit)

    copies.start("o", hstage, hydro.at[0, :, pl.ds(6, fx - 12)])

    @pl.loop(0, nx - 4)
    def _(l):
        bssn_layer(state, sources[l + 2], stage, l + 4, l)

    copies.start("o", stage, rates.at[:, pl.ds(2, nx - 4)])
    copies.wait_all()


def side_work(copies, side, recv, complete, state, flux, sources, fluid, hydro, stage, six, coarse, rows, hstage):
    nx = sources.shape[0]
    ny, _ = sources.shape[-2:]
    fx = fluid.shape[1]
    halo = side * (nx + 2)
    for k in range(2):
        for n, field in enumerate((0, 1, 15, 16, 17)):
            state[field, halo + k] = recv[2 * n + k]
    for n, row, count, layer, at in coarse_rows(ny):
        state[(0, 1, 15)[n], nx + 4, pl.ds(row, count), :] = recv[SPARE + layer, pl.ds(at, count), :]
    if complete:

        @pl.loop(0, LATE)
        def _(n):
            for k in range(2):
                field = jnp.where(n == LATE - 1, 2, n + 3)
                state[field, halo + k] = recv[EARLY_LAYERS + 2 * n + k]

    place = lax.axis_index(RING[-1])
    outer = jnp.where(side == 0, place == 0, place == lax.axis_size(RING[-1]) - 1)
    inside = jnp.where(outer, 0.0, 1.0).astype(F32)
    for n in range(FLUID):
        for k in range(3):
            value = recv[2 * EARLY + 3 * n + k]
            six[n, 3 * side + k] = value if n == 5 else value * inside
            six[n, 3 - 3 * side + k] = fluid[n, side * (fx - 3) + k]

    def coarse_plane(field, layer):
        return lambda sl: state[field, side * nx + 1 + layer, sl, :]

    prolong_yz([[coarse_plane(f, l) for l in range(4)] for f in (0, 15, 1)], rows, coarse)

    @pl.loop(0, 6)
    def _(j):
        mid = lax.shift_right_logical(j + 1, 1)
        other = mid + 1 - 2 * (j & 1)
        parts = [0.75 * coarse[n, mid] + 0.25 * coarse[n, other] for n in range(3)]
        split_flux(lambda n: six[n, j], *parts, flux, side * fx + j)

    first = side * (fx - 6)

    @pl.loop(0, 5)
    def _(n):
        for part in range(ny // 8):
            sl = pl.ds(part * 8, 8)

            def emit(i, value):
                hstage[n, i, sl, :] = value

            weno_cells(flux, n, sl, first + 3, 6, emit)

    copies.start("o", hstage, hydro.at[0, :, pl.ds(first, 6)])

    @pl.loop(0, 2)
    def _(k):
        l = side * (nx - 2) + k
        source = sources[l]
        if complete:
            source = source + jnp.where(l == 0, 1.0, 0.0).astype(F32) * recv[EARLY_LAYERS + 2 * LATE]
        bssn_layer(state, source, stage, l + 2, k)


def fast_kernel(
    recv, rates_in, hydro_in, state_in, flux_in, sources, fluid,
    rates, hydro, state, flux,
    stage, six, coarse, rows, hstage, sems,
):
    copies = Copies(sems)
    side = 1 - slow_side()
    side_work(copies, side, recv, True, state, flux, sources, fluid, hydro, stage, six, coarse, rows, hstage)
    copies.start("o", stage, rates.at[:, pl.ds(side * (rates.shape[1] - 2), 2)])
    copies.wait_all()


def slow_kernel(
    recv, hydro_in, state_in, flux_in, sources, fluid,
    hydro, state, flux, stage,
    six, coarse, rows, hstage, sems,
):
    copies = Copies(sems)
    side_work(copies, slow_side(), recv, False, state, flux, sources, fluid, hydro, stage, six, coarse, rows, hstage)
    copies.wait_all()


def late_kernel(recv, early, stage_in, state, rates_in, rates, stage, sems):
    nx = rates.shape[1]
    copies = Copies(sems)
    side = slow_side()
    low = side == 0

    def pick(below, above):
        return jnp.where(low, below, above).astype(F32)

    taps = ((pick(1.0, -1.0), pick(-8.0, 0.0)), (pick(0.0, 8.0), pick(1.0, -1.0)))
    first = side * (nx - 2)
    layers = pl.ds(first, 2)
    copies.start("o", stage_in.at[pl.ds(0, 2)], rates.at[pl.ds(0, 2), layers])
    steps = [state[15, first + 2 + k] * (1.0 / 12.0) for k in range(2)]
    for begin, end in ((3, 7), (7, 11), (11, 15), (2, 3)):
        for field in range(begin, end):
            if field == 2:
                values = [jnp.where(low, early[SPARE + n], recv[PLANE + n]) for n in range(2)]
            else:
                values = [recv[2 * (field - 3) + n] for n in range(2)]
            for k in range(2):
                value = stage_in[field, k] + steps[k] * (taps[k][0] * values[0] + taps[k][1] * values[1])
                if field == 2 and k == 0:
                    value = value + pick(4.0 * math.pi, 0.0) * state[0, 2] * recv[PLANE]
                stage[field, k] = value
        group = pl.ds(begin, end - begin)
        copies.start("o", stage.at[group], rates.at[group, layers])
    copies.wait_all()


def substep(*fields):
    fields = [pltpu.with_memory_space_constraint(field, pltpu.HBM) for field in fields]
    lapse, conf, mean, _, _, shift, dens, mom, ener, velo, pres = fields
    nx, ny, nz = lapse.shape
    fx = dens.shape[1]
    layer = (ny, nz)

    def shape(*leading):
        return jax.ShapeDtypeStruct(leading + layer, F32)

    def vmem(*leading):
        return pltpu.VMEM(leading + layer, F32)

    def row_scratch(planes):
        return pltpu.VMEM((nz // LANES, planes * ny, LANES), F32)

    def sems(n):
        return pltpu.SemaphoreType.DMA((n,))

    count = lax.axis_size(RING)
    fast_pairs = [(i, i ^ 1) for i in range(count)]
    slow_pairs = [(i, (i + (1 if i % 2 else -1)) % count) for i in range(count)]
    params = pltpu.CompilerParams(vmem_limit_bytes=GRANT)

    def cost(flops):
        return pl.CostEstimate(flops=flops, transcendentals=0, bytes_accessed=6_000_000)

    early = pl.pallas_call(
        pack_kernel,
        out_shape=shape(EARLY_LAYERS),
        in_specs=[HBM] * 9,
        out_specs=VMEM,
        scratch_shapes=[vmem(3), vmem(2), sems(16)],
        compiler_params=params,
        name="pack",
    )(lapse, conf, shift, mean, dens, mom, ener, velo, pres)
    packed = early
    early = lax.ppermute(early, RING, slow_pairs)
    local = pl.pallas_call(
        local_kernel,
        out_shape=(
            shape(METRIC, nx + 5),
            shape(10, fx + 6),
            shape(nx),
            shape(9, fx),
            shape(EARLY_LAYERS + 2 * LATE + 1),
            shape(2 * LATE),
        ),
        in_specs=[VMEM] + [HBM] * 11,
        out_specs=[VMEM] * 6,
        scratch_shapes=[vmem(3, nx), row_scratch(3 * nx), sems(40)],
        cost_estimate=cost(200_000_000),
        compiler_params=params,
        name="local",
    )
    state, flux, sources, fluid, fast, late = local(packed, *fields)
    late = lax.ppermute(late, RING, slow_pairs)
    fast = lax.ppermute(fast, RING, fast_pairs)
    rates, hydro = pl.pallas_call(
        inner_kernel,
        out_shape=(shape(15, nx), shape(1, 5, fx)),
        in_specs=[VMEM] * 3,
        out_specs=[HBM] * 2,
        scratch_shapes=[vmem(15, nx - 4), vmem(5, fx - 12), sems(4)],
        cost_estimate=cost(400_000_000),
        compiler_params=params,
        name="inner",
    )(state, flux, sources)
    work = [vmem(FLUID, 6), vmem(3, 4), row_scratch(12), vmem(5, 6), sems(4)]
    rates, hydro, state, flux = pl.pallas_call(
        fast_kernel,
        out_shape=(shape(15, nx), shape(1, 5, fx), shape(METRIC, nx + 5), shape(10, fx + 6)),
        in_specs=[VMEM] + [HBM] * 2 + [VMEM] * 4,
        out_specs=[HBM] * 2 + [VMEM] * 2,
        input_output_aliases={1: 0, 2: 1, 3: 2, 4: 3},
        scratch_shapes=[vmem(15, 2)] + work,
        cost_estimate=cost(300_000_000),
        compiler_params=params,
        name="fast",
    )(fast, rates, hydro, state, flux, sources, fluid)
    hydro, state, _, stage = pl.pallas_call(
        slow_kernel,
        out_shape=(shape(1, 5, fx), shape(METRIC, nx + 5), shape(10, fx + 6), shape(15, 2)),
        in_specs=[VMEM, HBM] + [VMEM] * 4,
        out_specs=[HBM] + [VMEM] * 3,
        input_output_aliases={1: 0, 2: 1, 3: 2},
        scratch_shapes=work,
        cost_estimate=cost(300_000_000),
        compiler_params=params,
        name="slow",
    )(early, hydro, state, flux, sources, fluid)
    rates = pl.pallas_call(
        late_kernel,
        out_shape=shape(15, nx),
        in_specs=[VMEM] * 4 + [HBM],
        out_specs=HBM,
        input_output_aliases={4: 0},
        scratch_shapes=[vmem(15, 2), sems(8)],
        compiler_params=params,
        name="late",
    )(late, early, stage, state, rates)
    return rates, hydro


def solution(mesh):
    in_specs = (
        P(RING, None, None),
        P(RING, None, None),
        P(RING, None, None),
        P(None, RING, None, None),
        P(None, RING, None, None),
        P(None, RING, None, None),
        P("star", "blk", None, None),
        P("star", None, "blk", None, None),
        P("star", "blk", None, None),
        P("star", None, "blk", None, None),
        P("star", "blk", None, None),
    )
    out_specs = (P(None, RING, None, None), P("star", None, "blk", None, None))
    return jax.shard_map(substep, mesh=mesh, in_specs=in_specs, out_specs=out_specs, check_vma=False)
```
